256 devices in a mesh: seq: 64 (over x, z, core), head: 4 (over y).
Axes of the slice: x: 4, y: 4, z: 8, core: 2. Of those that a mesh axis runs over, the one named last changes fastest.
Arguments:
- queries: bfloat16 [32768, 4096], P('seq', 'head'), may hold values from -120 to 120
- keys: bfloat16 [32768, 1024], P('seq', 'head'), may hold values from -4 to 4
- values: bfloat16 [32768, 1024], P('seq', 'head'), may hold values from -6 to 6
- doc_start: int32 [32768], P('seq'), may hold values from 0 to 32767, as said below
- hop_counts: int32 [64], P('seq'), may hold values from 0 to 4, as said below
- loss_mask: int32 [32768], P('seq'), may hold values from 0 to 1, as said below
Outputs:
- attention: bfloat16 [32768, 4096], P('seq', 'head')
- objective: float32 [], replicated
The draws below stay inside these ranges and needn't reach their ends.
Inputs may be any that keep to these rules, and one draw needn't show every extreme that they name: doc_start is nondecreasing; doc_start[doc_start[i]] = doc_start[i] <= i; a document holds at most 2048 tokens, and some document holds exactly that many in every draw. hop_counts[b] = b - floor(doc_start[b * 512] / 512); the most, 4, is reached in every draw. loss_mask[0] = 1.
All inputs are finite; a program needn't handle non-finite values.
Results may differ from the reference program's by a relative error of at most 0.0035.
Values may be sent and summed in bfloat16 or wider, within the bound.
No kernel may reach another device: no remote copies, remote signals or barrier semaphores. Data moves between devices by JAX's collectives and lax.ppermute only.
A program may use at most 128 MiB of HBM per device.

```python
import math
import jax
import jax.numpy as jnp
from jax import lax

QUERY_HEADS = 32
KEY_VALUE_HEADS = 8
HEAD_WIDTH = 128
BLOCK_TOKENS = 512
HOPS = 4
PACKED_TOKENS = 32768


def doc_layout(key):
    span = HOPS * BLOCK_TOKENS
    places = jnp.arange(PACKED_TOKENS, dtype=jnp.int32)
    windows = PACKED_TOKENS // span + 2
    rates = jax.random.randint(jax.random.fold_in(key, 11), (windows,), 0, 3)
    levels = jnp.array([2, 4, 8], dtype=jnp.int32)[rates]
    whole_window = jax.random.randint(jax.random.fold_in(key, 13), (), 0, max(PACKED_TOKENS // span - 1, 1))
    window_ids = jnp.arange(windows, dtype=jnp.int32)
    levels = jnp.where(window_ids == whole_window, 0, levels)
    ticket = jax.random.randint(jax.random.fold_in(key, 12), (PACKED_TOKENS,), 0, span)
    window_of = jnp.maximum(places - 1, 0) // span
    flagged = (places % span == 1) | (places == 0) | (places == PACKED_TOKENS - 1) | (ticket < levels[window_of])
    starts = lax.cummax(jnp.where(flagged, places, 0), axis=0)
    block_ids = jnp.arange(PACKED_TOKENS // BLOCK_TOKENS, dtype=jnp.int32)
    hops = block_ids - starts[block_ids * BLOCK_TOKENS] // BLOCK_TOKENS
    return (starts.astype(jnp.int32), hops.astype(jnp.int32))


def draw_doc_start(key, part):
    return doc_layout(key)[0]


def draw_hop_counts(key, part):
    return doc_layout(key)[1]


def draw_loss_mask(key, part):
    places = jnp.arange(PACKED_TOKENS, dtype=jnp.int32)
    ticket = jax.random.randint(jax.random.fold_in(key, 31), (PACKED_TOKENS,), 0, 1000)
    marks = (ticket < 200 + 500 * places // PACKED_TOKENS).astype(jnp.int32)
    return marks.at[0].set(1)


def query_keys(key):
    resident_keys = jnp.clip(jax.random.normal(jax.random.fold_in(key, 21), (PACKED_TOKENS, KEY_VALUE_HEADS * HEAD_WIDTH), jnp.float32), -4.0, 4.0)
    base_queries = jnp.clip(jax.random.normal(jax.random.fold_in(key, 22), (PACKED_TOKENS, QUERY_HEADS * HEAD_WIDTH), jnp.float32), -4.0, 4.0)
    return (base_queries, resident_keys)


def draw_queries(key, part):
    return query_keys(key)[0].astype(jnp.bfloat16)


def draw_keys(key, part):
    return query_keys(key)[1].astype(jnp.bfloat16)


def block_levels(rng, shape, pieces, low, top_value):
    level = 1.0
    for dim, shards_of in pieces:
        steps = jax.random.uniform(jax.random.fold_in(jax.random.fold_in(rng, 6), dim), (shards_of,), jnp.float32, low / len(pieces), top_value / len(pieces))
        level = level * jnp.repeat(jnp.exp(steps), shape[dim] // shards_of).reshape((-1,) + (1,) * (len(shape) - 1 - dim))
    return level


def centred(stream_key, extent, scale, reach, pieces=(), kind=jnp.bfloat16):
    level = block_levels(stream_key, extent, pieces, -0.22, 0.18) if pieces else 1.0
    result = jax.random.normal(stream_key, extent, jnp.float32) * scale * level
    return jnp.minimum(jnp.maximum(result, -reach), reach).astype(kind)


def setup_inputs(seed: int = 0) -> dict:
    arg_keys = jax.random.split(jax.random.key(seed), 7)
    queries = draw_queries(jax.random.fold_in(arg_keys[6], 71), 0)
    keys = draw_keys(jax.random.fold_in(arg_keys[6], 71), 0)
    values = centred(arg_keys[2], (PACKED_TOKENS, KEY_VALUE_HEADS * HEAD_WIDTH), 1.0, 6.0, ((0, 64), (1, 4)))
    doc_start = draw_doc_start(jax.random.fold_in(arg_keys[6], 71), 0)
    hop_counts = draw_hop_counts(jax.random.fold_in(arg_keys[6], 71), 0)
    loss_mask = draw_loss_mask(jax.random.fold_in(arg_keys[6], 71), 0)
    return {"queries": queries, "keys": keys, "values": values, "doc_start": doc_start, "hop_counts": hop_counts, "loss_mask": loss_mask}


def reference(queries, keys, values, doc_start, hop_counts, loss_mask):
    group_size = QUERY_HEADS // KEY_VALUE_HEADS
    blocks = PACKED_TOKENS // BLOCK_TOKENS
    border_width = HOPS * BLOCK_TOKENS
    reach_extent = (HOPS + 1) * BLOCK_TOKENS
    key_padding = jnp.concatenate([jnp.zeros((border_width, KEY_VALUE_HEADS * HEAD_WIDTH), keys.dtype), keys], axis=0)
    value_padding = jnp.concatenate([jnp.zeros((border_width, KEY_VALUE_HEADS * HEAD_WIDTH), values.dtype), values], axis=0)

    def one_block(block):
        block_offset = (block * BLOCK_TOKENS).astype(jnp.int32)
        query_row_block = lax.dynamic_slice_in_dim(queries, block_offset, BLOCK_TOKENS, 0).reshape(BLOCK_TOKENS, KEY_VALUE_HEADS, group_size, HEAD_WIDTH).astype(jnp.float32)
        key_row_block = lax.dynamic_slice_in_dim(key_padding, block_offset, reach_extent, 0).reshape(reach_extent, KEY_VALUE_HEADS, HEAD_WIDTH).astype(jnp.float32)
        value_row_block = lax.dynamic_slice_in_dim(value_padding, block_offset, reach_extent, 0).reshape(reach_extent, KEY_VALUE_HEADS, HEAD_WIDTH).astype(jnp.float32)
        scores = jnp.einsum('tgqd,sgd->tgqs', query_row_block, key_row_block) / math.sqrt(HEAD_WIDTH)
        key_place = block_offset - border_width + jnp.arange(reach_extent, dtype=jnp.int32)
        query_place = block_offset + jnp.arange(BLOCK_TOKENS, dtype=jnp.int32)
        firsts = lax.dynamic_slice_in_dim(doc_start, block_offset, BLOCK_TOKENS, 0)
        hop_limit = lax.dynamic_index_in_dim(hop_counts, block, 0, keepdims=False)
        distance = block - jnp.floor_divide(key_place, BLOCK_TOKENS)
        seen = (key_place[None, :] >= firsts[:, None]) & (key_place[None, :] <= query_place[:, None]) & (distance <= hop_limit)[None, :]
        seen = seen[:, None, None, :]
        masked = jnp.where(seen, scores, jnp.float32(-1e+30))
        top = lax.optimization_barrier(jnp.max(masked, axis=-1, keepdims=True))
        weights = jnp.where(seen, jnp.exp(masked - top), jnp.float32(0.0))
        total = lax.optimization_barrier(jnp.sum(weights, axis=-1))
        rounded = lax.optimization_barrier(weights.astype(jnp.bfloat16))
        numer = jnp.einsum('tgqs,sgd->tgqd', rounded.astype(jnp.float32), value_row_block)
        attended = (numer / total[..., None]).reshape(BLOCK_TOKENS, QUERY_HEADS * HEAD_WIDTH)
        marks = lax.dynamic_slice_in_dim(loss_mask, block_offset, BLOCK_TOKENS, 0).astype(jnp.float32)
        squares = jnp.sum(marks[:, None] * attended * attended)
        return (attended.astype(jnp.bfloat16), squares)
    outputs, squares = lax.map(one_block, jnp.arange(blocks, dtype=jnp.int32))
    attention = outputs.reshape(PACKED_TOKENS, QUERY_HEADS * HEAD_WIDTH)
    counted = jnp.sum(loss_mask.astype(jnp.float32))
    objective = jnp.sum(squares) / (QUERY_HEADS * counted)
    return (attention, objective)
```

```python
import math

import jax
import jax.numpy as jnp
from jax import lax
from jax.experimental import pallas as pl
from jax.experimental.pallas import tpu as pltpu
from jax.sharding import Mesh
from jax.sharding import PartitionSpec as P

QUERY_HEADS = 32
KEY_VALUE_HEADS = 8
HEAD_WIDTH = 128
GROUP = QUERY_HEADS // KEY_VALUE_HEADS
SEQ = ("seq_0", "seq_1", "seq_2")
SEQ_HEAD = ("seq_0", "seq_1", "seq_2", "head")
ROWS = 512
TILE = 128
TILES = ROWS // TILE
LOCAL_KV = 2
WIDE = GROUP * HEAD_WIDTH
LOWEST = -1e30
EXP2_SCALE = math.log2(math.e) / math.sqrt(HEAD_WIDTH)
TOP, TOTAL, FIRST, MARK = 0, GROUP, 2 * GROUP, 2 * GROUP + 1


def ds(start, size):
    return pl.ds(start if isinstance(start, int) else pl.multiple_of(start, size), size)


def dot(a, b, contract_b):
    return lax.dot_general(
        a, b, (((1,), (contract_b,)), ((), ())), preferred_element_type=jnp.float32
    )


def grouped_queries(q_ref, kv, tile):
    parts = [
        q_ref[ds(tile * TILE, TILE), ds(kv * WIDE + g * HEAD_WIDTH, HEAD_WIDTH)]
        for g in range(GROUP)
    ]
    return jnp.concatenate(parts, axis=0)


def with_lanes(base, columns):
    lane = lax.broadcasted_iota(jnp.int32, base.shape, 1)
    for at, column in columns:
        base = jnp.where(lane == at, column, base)
    return base


def absorb_own(q_ref, block_ref, acc_ref, stat_ref, kv, tile, first, mark):
    seen_keys = (tile + 1) * TILE
    k = block_ref[0:seen_keys, ds(kv * HEAD_WIDTH, HEAD_WIDTH)]
    v = block_ref[0:seen_keys, ds((LOCAL_KV + kv) * HEAD_WIDTH, HEAD_WIDTH)]
    scores = dot(grouped_queries(q_ref, kv, tile), k, 1)
    place = lax.broadcasted_iota(jnp.int32, (TILE, seen_keys), 1).astype(jnp.float32)
    row = lax.broadcasted_iota(jnp.int32, (TILE, seen_keys), 0).astype(jnp.float32) + tile * TILE
    seen = (place >= first[:, 0:1]) & (place <= row)
    rounded, columns = [], [(FIRST, first), (MARK, mark)]
    for g in range(GROUP):
        part = jnp.where(seen, scores[g * TILE : (g + 1) * TILE], LOWEST)
        top = jnp.max(part, axis=1, keepdims=True)
        weights = jnp.exp2((part - top) * EXP2_SCALE)
        columns += [(TOP + g, top), (TOTAL + g, jnp.sum(weights, axis=1, keepdims=True))]
        rounded.append(weights.astype(jnp.bfloat16))
    update = dot(jnp.concatenate(rounded, axis=0), v, 0)
    for g in range(GROUP):
        acc_ref[tile * TILE : (tile + 1) * TILE, ds(kv * WIDE + g * HEAD_WIDTH, HEAD_WIDTH)] = (
            update[g * TILE : (g + 1) * TILE]
        )
    stat_ref[kv, tile * TILE : (tile + 1) * TILE, :] = with_lanes(
        jnp.zeros((TILE, 128), jnp.float32), columns
    )


def absorb_earlier(q_ref, block_ref, acc_ref, stat_ref, kv, tile, offset):
    rows = ds(tile * TILE, TILE)
    stats = stat_ref[kv, rows, :]
    k = block_ref[:, ds(kv * HEAD_WIDTH, HEAD_WIDTH)]
    v = block_ref[:, ds((LOCAL_KV + kv) * HEAD_WIDTH, HEAD_WIDTH)]
    scores = dot(grouped_queries(q_ref, kv, tile), k, 1)
    place = (lax.broadcasted_iota(jnp.int32, (TILE, ROWS), 1) + offset).astype(jnp.float32)
    seen = place >= stats[:, FIRST : FIRST + 1]
    rounded, columns, ratios = [], [], []
    for g in range(GROUP):
        part = jnp.where(seen, scores[g * TILE : (g + 1) * TILE], LOWEST)
        top_old = stats[:, TOP + g : TOP + g + 1]
        top = jnp.maximum(top_old, jnp.max(part, axis=1, keepdims=True))
        ratio = jnp.exp2((top_old - top) * EXP2_SCALE)
        weights = jnp.exp2((part - top) * EXP2_SCALE)
        total = stats[:, TOTAL + g : TOTAL + g + 1] * ratio
        columns += [
            (TOP + g, top),
            (TOTAL + g, total + jnp.sum(weights, axis=1, keepdims=True)),
        ]
        ratios.append(ratio)
        rounded.append(weights.astype(jnp.bfloat16))
    update = dot(jnp.concatenate(rounded, axis=0), v, 0)
    for g in range(GROUP):
        cols = ds(kv * WIDE + g * HEAD_WIDTH, HEAD_WIDTH)
        acc_ref[rows, cols] = acc_ref[rows, cols] * ratios[g] + update[g * TILE : (g + 1) * TILE]
    stat_ref[kv, rows, :] = with_lanes(stats, columns)


def reaches(doc_ref, spot_ref, tile, offset):
    earliest = jnp.maximum(doc_ref[tile * TILE], spot_ref[1]) - spot_ref[0]
    return (offset < 0) & (offset + ROWS > earliest)


def first_kernel(
    spot_ref, doc_ref, rows_ref, q_ref, own_ref, side_ref, acc_ref, stat_ref
):
    def turned(at):
        row = jnp.broadcast_to(rows_ref[at : at + 1, :], (TILE, 128))
        return row.T

    def head(kv, carry):
        for tile in range(TILES):
            absorb_own(
                q_ref, own_ref, acc_ref, stat_ref, kv, tile, turned(tile), turned(TILES + tile)
            )
        return carry

    lax.fori_loop(0, LOCAL_KV, head, 0)
    sweep(spot_ref, doc_ref, q_ref, (side_ref,), acc_ref, stat_ref, lambda kv, tile: None)


def sweep(spot_ref, doc_ref, q_ref, block_refs, acc_ref, stat_ref, before):
    def step(index, carry):
        kv, tile = index // TILES, index % TILES
        before(kv, tile)
        for slot, block_ref in enumerate(block_refs):
            offset = spot_ref[2 + slot]

            @pl.when(reaches(doc_ref, spot_ref, tile, offset))
            def _():
                absorb_earlier(q_ref, block_ref, acc_ref, stat_ref, kv, tile, offset)

        return carry

    lax.fori_loop(0, LOCAL_KV * TILES, step, 0)


def middle_kernel(
    spot_ref, doc_ref, q_ref, far_ref, side_ref, acc_in, stat_in, acc_ref, stat_ref
):
    def before(kv, tile):
        rows, cols = ds(tile * TILE, TILE), ds(kv * WIDE, WIDE)
        acc_ref[rows, cols] = acc_in[rows, cols]
        stat_ref[kv, rows, :] = stat_in[kv, rows, :]

    sweep(spot_ref, doc_ref, q_ref, (far_ref, side_ref), acc_ref, stat_ref, before)


def last_kernel(
    spot_ref, doc_ref, q_ref, far_ref, side_ref, acc_in, stat_in, out_ref, share_ref,
    acc_ref, stat_ref, squares_ref, count_ref
):
    squares_ref[...] = jnp.zeros_like(squares_ref)
    count_ref[...] = jnp.zeros_like(count_ref)

    def finish(acc, stat, kv, tile):
        rows = ds(tile * TILE, TILE)
        stats = stat[kv, rows, :]
        marks = stats[:, MARK : MARK + 1]
        squares = jnp.zeros((TILE, HEAD_WIDTH), jnp.float32)
        for g in range(GROUP):
            cols = ds(kv * WIDE + g * HEAD_WIDTH, HEAD_WIDTH)
            attended = acc[rows, cols] / stats[:, TOTAL + g : TOTAL + g + 1]
            out_ref[rows, cols] = attended.astype(jnp.bfloat16)
            squares += attended * attended
        squares *= marks
        squares_ref[...] += jnp.sum(squares.reshape(TILE // 8, 8, HEAD_WIDTH), axis=0)
        count_ref[...] += jnp.sum(stats.reshape(TILE // 8, 8, 128), axis=0)

    def step(index, carry):
        kv, tile = index // TILES, index % TILES
        rows, cols = ds(tile * TILE, TILE), ds(kv * WIDE, WIDE)
        needs = [
            reaches(doc_ref, spot_ref, tile, spot_ref[2]),
            reaches(doc_ref, spot_ref, tile, spot_ref[3]),
        ]

        @pl.when(needs[0] | needs[1])
        def _():
            acc_ref[rows, cols] = acc_in[rows, cols]
            stat_ref[kv, rows, :] = stat_in[kv, rows, :]
            for slot, block_ref in enumerate((far_ref, side_ref)):

                @pl.when(needs[slot])
                def _():
                    absorb_earlier(
                        q_ref, block_ref, acc_ref, stat_ref, kv, tile, spot_ref[2 + slot]
                    )

            finish(acc_ref, stat_ref, kv, tile)

        @pl.when(jnp.logical_not(needs[0] | needs[1]))
        def _():
            finish(acc_in, stat_in, kv, tile)

        return carry

    lax.fori_loop(0, LOCAL_KV * TILES, step, 0)
    lane = lax.broadcasted_iota(jnp.int32, (8, 128), 1)
    squares = jnp.sum(squares_ref[...])
    count = jnp.sum(jnp.where(lane == MARK, count_ref[...], 0.0)) * (1.0 / LOCAL_KV)
    full = lax.broadcasted_iota(jnp.int32, share_ref.shape, 1)
    share_ref[...] = jnp.where(full == 0, squares, jnp.where(full == 1, count, 0.0))


def call(kernel, out_shapes, operands, flops, scratch=()):
    smem = pl.BlockSpec(memory_space=pltpu.SMEM)
    vmem = pl.BlockSpec(memory_space=pltpu.VMEM)
    return pl.pallas_call(
        kernel,
        out_shape=out_shapes,
        in_specs=[smem, smem] + [vmem] * (len(operands) - 2),
        out_specs=[vmem] * len(out_shapes),
        scratch_shapes=list(scratch),
        compiler_params=pltpu.CompilerParams(vmem_limit_bytes=24 * 1024 * 1024),
        cost_estimate=pl.CostEstimate(flops=flops, bytes_accessed=2**20, transcendentals=2**21),
    )(*operands)


def on_device(queries, keys, values, doc_start, hop_counts, loss_mask):
    core = lax.axis_index("seq_2")
    block = lax.axis_index(SEQ)
    here = block * ROWS
    floor = (block - hop_counts[0]) * ROWS
    nowhere = jnp.int32(ROWS)

    def spot(*offsets):
        return jnp.stack([here, floor] + [jnp.int32(o) for o in offsets])

    own = jnp.concatenate([keys, values], axis=1)

    def onward(shard):
        devices = lax.axis_size(SEQ)
        return lax.ppermute(shard, SEQ, [(i, i + 2) for i in range(devices - 2)])

    def across(shard, pairs):
        return lax.ppermute(shard, "seq_2", pairs)

    far_2 = onward(own)
    side_a = across(own, [(0, 1)])

    first_key = (jnp.maximum(doc_start, floor) - here).astype(jnp.float32)
    rows = jnp.concatenate(
        [first_key.reshape(TILES, TILE), loss_mask.astype(jnp.float32).reshape(TILES, TILE)]
    )
    acc_shape = jax.ShapeDtypeStruct((ROWS, LOCAL_KV * WIDE), jnp.float32)
    stat_shape = jax.ShapeDtypeStruct((LOCAL_KV, ROWS, 128), jnp.float32)
    acc, stat = call(
        first_kernel,
        [acc_shape, stat_shape],
        [spot(jnp.where(core == 1, -ROWS, nowhere)), doc_start, rows, queries, own, side_a],
        2 * 10**9,
    )
    far_4 = onward(far_2)
    side_b = across(far_2, [(0, 1), (1, 0)])
    acc, stat = call(
        middle_kernel,
        [acc_shape, stat_shape],
        [
            spot(-2 * ROWS, jnp.where(core == 1, -3 * ROWS, -ROWS)),
            doc_start, queries, far_2, side_b, acc, stat,
        ],
        2 * 10**9,
    )
    side_c = across(far_4, [(1, 0)])
    devices = lax.axis_size(SEQ_HEAD)
    attention, share = call(
        last_kernel,
        [
            jax.ShapeDtypeStruct((ROWS, LOCAL_KV * WIDE), jnp.bfloat16),
            jax.ShapeDtypeStruct((devices, 128), jnp.float32),
        ],
        [
            spot(-4 * ROWS, jnp.where(core == 1, nowhere, -3 * ROWS)),
            doc_start, queries, far_4, side_c, acc, stat,
        ],
        10**9,
        scratch=[
            pltpu.VMEM(acc_shape.shape, jnp.float32),
            pltpu.VMEM(stat_shape.shape, jnp.float32),
            pltpu.VMEM((8, 128), jnp.float32),
            pltpu.VMEM((8, 128), jnp.float32),
        ],
    )
    shares = lax.all_to_all(share, SEQ_HEAD, 0, 0, tiled=True)
    sums = jnp.sum(shares, axis=0)
    objective = sums[0] / (QUERY_HEADS * (sums[1] / lax.axis_size("head")))
    return (attention, objective)


def solution(mesh):
    torus = Mesh(
        mesh.devices.reshape(4, 8, 2, mesh.shape["head"]), ("seq_0", "seq_1", "seq_2", "head")
    )
    placed = (P(SEQ, "head"), P(SEQ, "head"), P(SEQ, "head"), P(SEQ), P(SEQ), P(SEQ))

    return jax.shard_map(
        on_device, mesh=torus, in_specs=placed, out_specs=(P(SEQ, "head"), P()), check_vma=False
    )
```

```python
import math

import jax
import jax.numpy as jnp
from jax import lax
from jax.experimental import pallas as pl
from jax.experimental.pallas import tpu as pltpu
from jax.sharding import Mesh
from jax.sharding import PartitionSpec as P

QUERY_HEADS = 32
KEY_VALUE_HEADS = 8
HEAD_WIDTH = 128
GROUP = QUERY_HEADS // KEY_VALUE_HEADS
SEQ = ("seq_0", "seq_1", "seq_2")
SEQ_HEAD = ("seq_0", "seq_1", "seq_2", "head")
ROWS = 512
TILE = 128
TILES = ROWS // TILE
LOCAL_KV = 2
HEADS = LOCAL_KV * GROUP
LOWEST = -1e30
EXP2_SCALE = math.log2(math.e) / math.sqrt(HEAD_WIDTH)
NOWHERE = ROWS


def aligned(start, size):
    return pl.ds(start if isinstance(start, int) else pl.multiple_of(start, size), size)


def tile_rows(tile):
    return aligned(tile * TILE, TILE)


def columns(head):
    return slice(head * HEAD_WIDTH, (head + 1) * HEAD_WIDTH)


def dot(a, b, contract_b):
    return lax.dot_general(
        a, b, (((1,), (contract_b,)), ((), ())), preferred_element_type=jnp.float32
    )


def lane_groups(x):
    return [x[:, i : i + 128] for i in range(0, x.shape[1], 128)]


def folded(op, parts):
    while len(parts) > 1:
        parts = [op(*parts[i : i + 2]) if i + 1 < len(parts) else parts[i] for i in range(0, len(parts), 2)]
    return parts[0]


def widened(x, width):
    return jnp.concatenate([x] * (width // 128), axis=1)


def attend(q_ref, block_ref, tile, width, seen, old, new):
    rows = tile_rows(tile)
    for kv in range(LOCAL_KV):
        k = block_ref[0, 0:width, columns(kv)]
        v = block_ref[1, 0:width, columns(kv)]
        heads = [kv * GROUP + g for g in range(GROUP)]
        q = jnp.concatenate([q_ref[rows, columns(h)] for h in heads], axis=0)
        scores = dot(q, k, 1)
        rounded, states = [], []
        for g, head in enumerate(heads):
            part = jnp.where(seen, scores[g * TILE : (g + 1) * TILE], LOWEST)
            top = jnp.max(folded(jnp.maximum, lane_groups(part)), axis=1, keepdims=True)
            top = jnp.broadcast_to(top, (TILE, 128))
            before = old(head)
            ratio = None
            if before is not None:
                top = jnp.maximum(before[0], top)
                ratio = jnp.exp2((before[0] - top) * EXP2_SCALE)
            weights = jnp.exp2((part - widened(top, width)) * EXP2_SCALE)
            total = folded(jnp.add, lane_groups(weights))
            if before is not None:
                total = before[1] * ratio + total
            states.append((top, total, ratio))
            rounded.append(weights.astype(jnp.bfloat16))
        update = dot(jnp.concatenate(rounded, axis=0), v, 0)
        for g, head in enumerate(heads):
            top, total, ratio = states[g]
            sums = update[g * TILE : (g + 1) * TILE]
            if ratio is not None:
                sums = old(head)[2]() * ratio + sums
            new(head, top, total, sums)


def reader(state, rows):
    acc_ref, top_ref, tot_ref = state
    return lambda head: (
        top_ref[head, rows, :],
        tot_ref[head, rows, :],
        lambda: acc_ref[rows, columns(head)],
    )


def writer(state, rows):
    acc_ref, top_ref, tot_ref = state

    def store(head, top, total, sums):
        top_ref[head, rows, :] = top
        tot_ref[head, rows, :] = total
        acc_ref[rows, columns(head)] = sums

    return store


def attend_earlier(q_ref, block_ref, first_ref, tile, offset, old, new):
    place = (lax.broadcasted_iota(jnp.int32, (TILE, ROWS), 1) + offset).astype(jnp.float32)
    seen = place >= widened(first_ref[tile_rows(tile), :], ROWS)
    attend(q_ref, block_ref, tile, ROWS, seen, old, new)


def reaches(spot_ref, hop_ref, doc_ref, tile, offset):
    floor = spot_ref[0] - hop_ref[0] * ROWS
    earliest = jnp.maximum(doc_ref[tile * TILE], floor) - spot_ref[0]
    return (offset < 0) & (offset + ROWS > earliest)


def pack_kernel(keys_ref, values_ref, out_ref, sems):
    copies = [
        pltpu.make_async_copy(ref, out_ref.at[i], sems.at[i])
        for i, ref in enumerate((keys_ref, values_ref))
    ]
    for copy in copies:
        copy.start()
    for copy in copies:
        copy.wait()


def first_kernel(
    spot_ref, hop_ref, doc_ref, starts_ref, marks_ref, q_ref, own_ref, side_ref,
    acc_ref, top_ref, tot_ref, first_ref, mark_ref,
):
    floor = spot_ref[0] - hop_ref[0] * ROWS
    state = (acc_ref, top_ref, tot_ref)
    for tile in range(TILES):
        width = (tile + 1) * TILE
        rows = tile_rows(tile)
        starts = jnp.maximum(starts_ref[tile : tile + 1, :], floor) - spot_ref[0]
        first = jnp.broadcast_to(starts.astype(jnp.float32), (TILE, 128)).T
        first_ref[rows, :] = first
        marks = marks_ref[tile : tile + 1, :].astype(jnp.float32)
        mark_ref[rows, :] = jnp.broadcast_to(marks, (TILE, 128)).T
        place = lax.broadcasted_iota(jnp.int32, (TILE, width), 1)
        row = lax.broadcasted_iota(jnp.int32, (TILE, width), 0) + tile * TILE
        seen = (place.astype(jnp.float32) >= widened(first, width)) & (place <= row)
        attend(q_ref, own_ref, tile, width, seen, lambda head: None, writer(state, rows))
    offset = jnp.where(spot_ref[1] == 1, -ROWS, NOWHERE)

    def step(tile, carry):
        @pl.when(reaches(spot_ref, hop_ref, doc_ref, tile, offset))
        def _():
            rows = tile_rows(tile)
            attend_earlier(
                q_ref, side_ref, first_ref, tile, offset, reader(state, rows), writer(state, rows)
            )

        return carry

    lax.fori_loop(0, TILES, step, 0)


def copy_tile(source, target, rows, target_rows):
    for head in range(HEADS):
        top, total, sums = reader(source, rows)(head)
        writer(target, target_rows)(head, top, total, sums())


def middle_kernel(
    spot_ref, hop_ref, doc_ref, q_ref, far_ref, side_ref, first_ref, acc_in, top_in, tot_in,
    acc_ref, top_ref, tot_ref,
):
    source, state = (acc_in, top_in, tot_in), (acc_ref, top_ref, tot_ref)
    offsets = (-2 * ROWS, jnp.where(spot_ref[1] == 1, -3 * ROWS, -ROWS))

    def step(tile, carry):
        rows = tile_rows(tile)
        far = reaches(spot_ref, hop_ref, doc_ref, tile, offsets[0])
        side = reaches(spot_ref, hop_ref, doc_ref, tile, offsets[1])

        @pl.when(far)
        def _():
            attend_earlier(
                q_ref, far_ref, first_ref, tile, offsets[0],
                reader(source, rows), writer(state, rows),
            )

        @pl.when(jnp.logical_not(far))
        def _():
            copy_tile(source, state, rows, rows)

        @pl.when(side)
        def _():
            attend_earlier(
                q_ref, side_ref, first_ref, tile, offsets[1],
                reader(state, rows), writer(state, rows),
            )

        return carry

    lax.fori_loop(0, TILES, step, 0)


def last_kernel(
    spot_ref, hop_ref, doc_ref, q_ref, far_ref, side_ref, first_ref, mark_ref, acc_in, top_in,
    tot_in, out_ref, share_ref, acc_ref, top_ref, tot_ref, squares_ref, count_ref,
):
    source, state = (acc_in, top_in, tot_in), (acc_ref, top_ref, tot_ref)
    offsets = (-4 * ROWS, jnp.where(spot_ref[1] == 1, NOWHERE, -3 * ROWS))
    squares_ref[...] = jnp.zeros_like(squares_ref)
    count_ref[...] = jnp.zeros_like(count_ref)
    here = slice(0, TILE)

    def finish(final, rows, tile):
        marks = mark_ref[tile_rows(tile), :]
        squares = jnp.zeros((TILE, HEAD_WIDTH), jnp.float32)
        for head in range(HEADS):
            _, total, sums = reader(final, rows)(head)
            attended = sums() * (1.0 / jnp.sum(total, axis=1, keepdims=True))
            out_ref[tile_rows(tile), columns(head)] = attended.astype(jnp.bfloat16)
            squares += attended * attended
        squares *= marks
        squares_ref[...] += jnp.sum(squares.reshape(TILE // 8, 8, HEAD_WIDTH), axis=0)
        count_ref[...] += jnp.sum(marks.reshape(TILE // 8, 8, 128), axis=0)

    def step(tile, carry):
        rows = tile_rows(tile)
        far = reaches(spot_ref, hop_ref, doc_ref, tile, offsets[0])
        side = reaches(spot_ref, hop_ref, doc_ref, tile, offsets[1])

        @pl.when(far | side)
        def _():
            copy_tile(source, state, rows, here)
            for needed, block_ref, offset in (
                (far, far_ref, offsets[0]),
                (side, side_ref, offsets[1]),
            ):

                @pl.when(needed)
                def _():
                    attend_earlier(
                        q_ref, block_ref, first_ref, tile, offset,
                        reader(state, here), writer(state, here),
                    )

            finish(state, here, tile)

        @pl.when(jnp.logical_not(far | side))
        def _():
            finish(source, rows, tile)

        return carry

    lax.fori_loop(0, TILES, step, 0)
    squares = jnp.sum(squares_ref[...])
    count = jnp.sum(count_ref[...]) * (1.0 / 128)
    lane = lax.broadcasted_iota(jnp.int32, share_ref.shape, 1)
    share_ref[...] = jnp.where(lane == 0, squares, jnp.where(lane == 1, count, 0.0))


def call(kernel, scalars, arrays, out_shapes, flops, scratch=()):
    smem = pl.BlockSpec(memory_space=pltpu.SMEM)
    vmem = pl.BlockSpec(memory_space=pltpu.VMEM)
    return pl.pallas_call(
        kernel,
        out_shape=out_shapes,
        in_specs=[smem] * len(scalars) + [vmem] * len(arrays),
        out_specs=[vmem] * len(out_shapes),
        scratch_shapes=list(scratch),
        compiler_params=pltpu.CompilerParams(vmem_limit_bytes=8 * 1024 * 1024),
        cost_estimate=pl.CostEstimate(flops=flops, bytes_accessed=2**20, transcendentals=2**21),
    )(*scalars, *arrays)


def packed(keys, values):
    return pl.pallas_call(
        pack_kernel,
        out_shape=jax.ShapeDtypeStruct((2, *keys.shape), keys.dtype),
        in_specs=[pl.BlockSpec(memory_space=pltpu.HBM)] * 2,
        out_specs=pl.BlockSpec(memory_space=pltpu.VMEM),
        scratch_shapes=[pltpu.SemaphoreType.DMA((2,))],
        compiler_params=pltpu.CompilerParams(vmem_limit_bytes=4 * 1024 * 1024),
    )(keys, values)


def onward(shard):
    devices = lax.axis_size(SEQ)
    return lax.ppermute(shard, SEQ, [(i, i + 2) for i in range(devices - 2)])


def across(shard, pairs):
    return lax.ppermute(shard, "seq_2", pairs)


def f32(*shape):
    return jax.ShapeDtypeStruct(shape, jnp.float32)


def on_device(queries, keys, values, doc_start, hop_counts, loss_mask):
    spot = jnp.stack([lax.axis_index(SEQ) * ROWS, lax.axis_index("seq_2")])
    scalars = [spot, hop_counts, doc_start]
    own = packed(keys, values)
    far_2 = onward(own)
    side_1 = across(own, [(0, 1)])
    state_shapes = [f32(ROWS, HEADS * HEAD_WIDTH), f32(HEADS, ROWS, 128), f32(HEADS, ROWS, 128)]
    *state, first, mark = call(
        first_kernel,
        scalars,
        [doc_start.reshape(TILES, TILE), loss_mask.reshape(TILES, TILE), queries, own, side_1],
        state_shapes + [f32(ROWS, 128)] * 2,
        2 * 10**9,
    )
    far_4 = onward(far_2)
    side_2 = across(far_2, [(0, 1), (1, 0)])
    state = call(
        middle_kernel, scalars, [queries, far_2, side_2, first, *state], state_shapes, 2 * 10**9
    )
    side_3 = across(far_4, [(1, 0)])
    devices = lax.axis_size(SEQ_HEAD)
    attention, share = call(
        last_kernel,
        scalars,
        [queries, far_4, side_3, first, mark, *state],
        [jax.ShapeDtypeStruct((ROWS, HEADS * HEAD_WIDTH), jnp.bfloat16), f32(devices, 128)],
        10**9,
        scratch=[
            pltpu.VMEM((TILE, HEADS * HEAD_WIDTH), jnp.float32),
            pltpu.VMEM((HEADS, TILE, 128), jnp.float32),
            pltpu.VMEM((HEADS, TILE, 128), jnp.float32),
            pltpu.VMEM((8, 128), jnp.float32),
            pltpu.VMEM((8, 128), jnp.float32),
        ],
    )
    shares = lax.all_to_all(share, SEQ_HEAD, 0, 0, tiled=True)
    sums = jnp.sum(shares, axis=0)
    objective = sums[0] / (QUERY_HEADS * (sums[1] / lax.axis_size("head")))
    return (attention, objective)


def solution(mesh):
    torus = Mesh(
        mesh.devices.reshape(4, 8, 2, mesh.shape["head"]), ("seq_0", "seq_1", "seq_2", "head")
    )
    placed = (P(SEQ, "head"), P(SEQ, "head"), P(SEQ, "head"), P(SEQ), P(SEQ), P(SEQ))

    return jax.shard_map(
        on_device, mesh=torus, in_specs=placed, out_specs=(P(SEQ, "head"), P()), check_vma=False
    )
```

```python
import functools
import math

import jax
import jax.numpy as jnp
from jax import lax
from jax.experimental import pallas as pl
from jax.experimental.pallas import tpu as pltpu
from jax.sharding import Mesh
from jax.sharding import PartitionSpec as P

QUERY_HEADS = 32
KEY_VALUE_HEADS = 8
HEAD_WIDTH = 128
GROUP = QUERY_HEADS // KEY_VALUE_HEADS
SEQ = ("seq_0", "seq_1", "seq_2")
SEQ_HEAD = ("seq_0", "seq_1", "seq_2", "head")
ROWS = 512
TILE = 128
TILES = ROWS // TILE
LOCAL_KV = 2
HEADS = LOCAL_KV * GROUP
LOWEST = -1e30
EXP2_SCALE = math.log2(math.e) / math.sqrt(HEAD_WIDTH)
NOWHERE = ROWS


def aligned(start, size):
    return pl.ds(start if isinstance(start, int) else pl.multiple_of(start, size), size)


def tile_rows(tile):
    return aligned(tile * TILE, TILE)


def columns(head):
    return slice(head * HEAD_WIDTH, (head + 1) * HEAD_WIDTH)


def dot(a, b, contract_b):
    return lax.dot_general(
        a, b, (((1,), (contract_b,)), ((), ())), preferred_element_type=jnp.float32
    )


def lane_groups(x):
    return [x[:, i : i + 128] for i in range(0, x.shape[1], 128)]


def folded(op, parts):
    while len(parts) > 1:
        parts = [op(*parts[i : i + 2]) if i + 1 < len(parts) else parts[i] for i in range(0, len(parts), 2)]
    return parts[0]


def widened(x, width):
    return jnp.concatenate([x] * (width // 128), axis=1)


def attend(q_ref, block_ref, tile, width, seen, old, new):
    rows = tile_rows(tile)
    for kv in range(LOCAL_KV):
        k = block_ref[0, 0:width, columns(kv)]
        v = block_ref[1, 0:width, columns(kv)]
        heads = [kv * GROUP + g for g in range(GROUP)]
        q = jnp.concatenate([q_ref[rows, columns(h)] for h in heads], axis=0)
        scores = dot(q, k, 1)
        rounded, states = [], []
        for g, head in enumerate(heads):
            part = jnp.where(seen, scores[g * TILE : (g + 1) * TILE], LOWEST)
            top = jnp.max(folded(jnp.maximum, lane_groups(part)), axis=1, keepdims=True)
            top = jnp.broadcast_to(top, (TILE, 128))
            before = old(head)
            ratio = None
            if before is not None:
                top = jnp.maximum(before[0], top)
                ratio = jnp.exp2((before[0] - top) * EXP2_SCALE)
            weights = jnp.exp2((part - widened(top, width)) * EXP2_SCALE)
            total = folded(jnp.add, lane_groups(weights))
            if before is not None:
                total = before[1] * ratio + total
            states.append((top, total, ratio))
            rounded.append(weights.astype(jnp.bfloat16))
        update = dot(jnp.concatenate(rounded, axis=0), v, 0)
        for g, head in enumerate(heads):
            top, total, ratio = states[g]
            sums = update[g * TILE : (g + 1) * TILE]
            if ratio is not None:
                sums = old(head)[2]() * ratio + sums
            new(head, top, total, sums)


def reader(state, rows):
    acc_ref, top_ref, tot_ref = state
    return lambda head: (
        top_ref[head, rows, :],
        tot_ref[head, rows, :],
        lambda: acc_ref[rows, columns(head)],
    )


def writer(state, rows):
    acc_ref, top_ref, tot_ref = state

    def store(head, top, total, sums):
        top_ref[head, rows, :] = top
        tot_ref[head, rows, :] = total
        acc_ref[rows, columns(head)] = sums

    return store


def attend_earlier(q_ref, block_ref, first_ref, tile, offset, old, new):
    place = (lax.broadcasted_iota(jnp.int32, (TILE, ROWS), 1) + offset).astype(jnp.float32)
    seen = place >= widened(first_ref[tile_rows(tile), :], ROWS)
    attend(q_ref, block_ref, tile, ROWS, seen, old, new)


def reaches(spot_ref, hop_ref, doc_ref, tile, offset):
    floor = spot_ref[0] - hop_ref[0] * ROWS
    earliest = jnp.maximum(doc_ref[tile * TILE], floor) - spot_ref[0]
    return (offset < 0) & (offset + ROWS > earliest)


def pack_kernel(keys_ref, values_ref, out_ref, sems):
    copies = [
        pltpu.make_async_copy(ref, out_ref.at[i], sems.at[i])
        for i, ref in enumerate((keys_ref, values_ref))
    ]
    for copy in copies:
        copy.start()
    for copy in copies:
        copy.wait()


def first_kernel(
    spot_ref, hop_ref, doc_ref, starts_ref, marks_ref, q_ref, own_ref,
    acc_ref, top_ref, tot_ref, first_ref, mark_ref,
):
    floor = spot_ref[0] - hop_ref[0] * ROWS
    state = (acc_ref, top_ref, tot_ref)
    for tile in range(TILES):
        width = (tile + 1) * TILE
        rows = tile_rows(tile)
        starts = jnp.maximum(starts_ref[tile : tile + 1, :], floor) - spot_ref[0]
        first = jnp.broadcast_to(starts.astype(jnp.float32), (TILE, 128)).T
        first_ref[rows, :] = first
        marks = marks_ref[tile : tile + 1, :].astype(jnp.float32)
        mark_ref[rows, :] = jnp.broadcast_to(marks, (TILE, 128)).T
        place = lax.broadcasted_iota(jnp.int32, (TILE, width), 1)
        row = lax.broadcasted_iota(jnp.int32, (TILE, width), 0) + tile * TILE
        seen = (place.astype(jnp.float32) >= widened(first, width)) & (place <= row)
        attend(q_ref, own_ref, tile, width, seen, lambda head: None, writer(state, rows))


def copy_tile(source, target, rows, target_rows):
    for head in range(HEADS):
        top, total, sums = reader(source, rows)(head)
        writer(target, target_rows)(head, top, total, sums())


def finish(state, rows, mark_ref, out_ref, squares_ref, tile):
    marks = mark_ref[tile_rows(tile), :]
    squares = jnp.zeros((TILE, HEAD_WIDTH), jnp.float32)
    for head in range(HEADS):
        _, total, sums = reader(state, rows)(head)
        attended = sums() * (1.0 / jnp.sum(total, axis=1, keepdims=True))
        out_ref[tile_rows(tile), columns(head)] = attended.astype(jnp.bfloat16)
        squares += attended * attended
    squares *= marks
    squares_ref[...] += jnp.sum(squares.reshape(TILE // 8, 8, HEAD_WIDTH), axis=0)


def last_offsets(spot_ref):
    return (-4 * ROWS, jnp.where(spot_ref[1] == 1, NOWHERE, -3 * ROWS))


def middle_kernel(
    spot_ref, hop_ref, doc_ref, q_ref, near_ref, far_ref, side_ref, first_ref, mark_ref,
    acc_in, top_in, tot_in, acc_ref, top_ref, tot_ref, out_ref, squares_ref,
):
    source, state = (acc_in, top_in, tot_in), (acc_ref, top_ref, tot_ref)
    odd = spot_ref[1] == 1
    slots = (
        (near_ref, jnp.where(odd, -ROWS, NOWHERE)),
        (far_ref, -2 * ROWS),
        (side_ref, jnp.where(odd, -3 * ROWS, -ROWS)),
    )
    squares_ref[...] = jnp.zeros_like(squares_ref)

    def step(tile, carry):
        rows = tile_rows(tile)
        copy_tile(source, state, rows, rows)
        for block_ref, offset in slots:

            @pl.when(reaches(spot_ref, hop_ref, doc_ref, tile, offset))
            def _():
                attend_earlier(
                    q_ref, block_ref, first_ref, tile, offset,
                    reader(state, rows), writer(state, rows),
                )

        late = [reaches(spot_ref, hop_ref, doc_ref, tile, o) for o in last_offsets(spot_ref)]

        @pl.when(jnp.logical_not(late[0] | late[1]))
        def _():
            finish(state, rows, mark_ref, out_ref, squares_ref, tile)

        return carry

    lax.fori_loop(0, TILES, step, 0)


def last_kernel(
    spot_ref, hop_ref, doc_ref, q_ref, far_ref, side_ref, first_ref, mark_ref, acc_in, top_in,
    tot_in, done_ref, squares_in, out_ref, share_ref, acc_ref, top_ref, tot_ref, squares_ref,
):
    source, state = (acc_in, top_in, tot_in), (acc_ref, top_ref, tot_ref)
    offsets = last_offsets(spot_ref)
    squares_ref[...] = squares_in[...]
    here = slice(0, TILE)

    def step(tile, carry):
        rows = tile_rows(tile)
        late = [reaches(spot_ref, hop_ref, doc_ref, tile, offset) for offset in offsets]

        @pl.when(late[0] | late[1])
        def _():
            copy_tile(source, state, rows, here)
            for needed, block_ref, offset in zip(late, (far_ref, side_ref), offsets):

                @pl.when(needed)
                def _():
                    attend_earlier(
                        q_ref, block_ref, first_ref, tile, offset,
                        reader(state, here), writer(state, here),
                    )

            finish(state, here, mark_ref, out_ref, squares_ref, tile)

        @pl.when(jnp.logical_not(late[0] | late[1]))
        def _():
            out_ref[rows, :] = done_ref[rows, :]

        return carry

    lax.fori_loop(0, TILES, step, 0)
    squares = jnp.sum(squares_ref[...])
    count = jnp.sum(jnp.sum(mark_ref[...].reshape(ROWS // 8, 8, 128), axis=0)) * (1.0 / 128)
    lane = lax.broadcasted_iota(jnp.int32, share_ref.shape, 1)
    share_ref[...] = jnp.where(lane == 0, squares, jnp.where(lane == 1, count, 0.0))


def call(kernel, scalars, arrays, out_shapes, flops, scratch=()):
    smem = pl.BlockSpec(memory_space=pltpu.SMEM)
    vmem = pl.BlockSpec(memory_space=pltpu.VMEM)
    return pl.pallas_call(
        kernel,
        out_shape=out_shapes,
        in_specs=[smem] * len(scalars) + [vmem] * len(arrays),
        out_specs=[vmem] * len(out_shapes),
        scratch_shapes=list(scratch),
        compiler_params=pltpu.CompilerParams(vmem_limit_bytes=8 * 1024 * 1024),
        cost_estimate=pl.CostEstimate(flops=flops, bytes_accessed=2**20, transcendentals=2**21),
    )(*scalars, *arrays)


def packed(keys, values):
    return pl.pallas_call(
        pack_kernel,
        out_shape=jax.ShapeDtypeStruct((2, *keys.shape), keys.dtype),
        in_specs=[pl.BlockSpec(memory_space=pltpu.HBM)] * 2,
        out_specs=pl.BlockSpec(memory_space=pltpu.VMEM),
        scratch_shapes=[pltpu.SemaphoreType.DMA((2,))],
        compiler_params=pltpu.CompilerParams(vmem_limit_bytes=4 * 1024 * 1024),
    )(keys, values)


def objective_kernel(copies, shares_ref, out_ref):
    sums = jnp.sum(shares_ref[...], axis=0, keepdims=True)
    lane = lax.broadcasted_iota(jnp.int32, sums.shape, 1)
    squares = jnp.sum(jnp.where(lane == 0, sums, 0.0))
    count = jnp.sum(jnp.where(lane == 1, sums, 0.0)) * (1.0 / copies)
    out_ref[0] = squares / (QUERY_HEADS * count)


def objective_of(shares, copies):
    return pl.pallas_call(
        functools.partial(objective_kernel, copies),
        out_shape=f32(1),
        in_specs=[pl.BlockSpec(memory_space=pltpu.VMEM)],
        out_specs=pl.BlockSpec(memory_space=pltpu.SMEM),
        compiler_params=pltpu.CompilerParams(vmem_limit_bytes=4 * 1024 * 1024),
    )(shares).reshape(())


def onward(shard):
    devices = lax.axis_size(SEQ)
    return lax.ppermute(shard, SEQ, [(i, i + 2) for i in range(devices - 2)])


def across(shard, pairs):
    return lax.ppermute(shard, "seq_2", pairs)


def f32(*shape):
    return jax.ShapeDtypeStruct(shape, jnp.float32)


def on_device(queries, keys, values, doc_start, hop_counts, loss_mask):
    spot = jnp.stack([lax.axis_index(SEQ) * ROWS, lax.axis_index("seq_2")])
    scalars = [spot, hop_counts, doc_start]
    own = packed(keys, values)
    far_2 = onward(own)
    side_1 = across(own, [(0, 1)])
    state_shapes = [f32(ROWS, HEADS * HEAD_WIDTH), f32(HEADS, ROWS, 128), f32(HEADS, ROWS, 128)]
    *state, first, mark = call(
        first_kernel,
        scalars,
        [doc_start.reshape(TILES, TILE), loss_mask.reshape(TILES, TILE), queries, own],
        state_shapes + [f32(ROWS, 128)] * 2,
        2 * 10**9,
    )
    far_4 = onward(far_2)
    side_2 = across(far_2, [(0, 1), (1, 0)])
    out_shape = jax.ShapeDtypeStruct((ROWS, HEADS * HEAD_WIDTH), jnp.bfloat16)
    *state, done, squares = call(
        middle_kernel,
        scalars,
        [queries, side_1, far_2, side_2, first, mark, *state],
        state_shapes + [out_shape, f32(8, 128)],
        2 * 10**9,
    )
    side_3 = across(far_4, [(1, 0)])
    devices = lax.axis_size(SEQ_HEAD)
    attention, share = call(
        last_kernel,
        scalars,
        [queries, far_4, side_3, first, mark, *state, done, squares],
        [out_shape, f32(devices, 128)],
        10**9,
        scratch=[
            pltpu.VMEM((TILE, HEADS * HEAD_WIDTH), jnp.float32),
            pltpu.VMEM((HEADS, TILE, 128), jnp.float32),
            pltpu.VMEM((HEADS, TILE, 128), jnp.float32),
            pltpu.VMEM((8, 128), jnp.float32),
        ],
    )
    shares = lax.all_to_all(share, SEQ_HEAD, 0, 0, tiled=True)
    return (attention, objective_of(shares, lax.axis_size("head")))


def solution(mesh):
    torus = Mesh(
        mesh.devices.reshape(4, 8, 2, mesh.shape["head"]), ("seq_0", "seq_1", "seq_2", "head")
    )
    placed = (P(SEQ, "head"), P(SEQ, "head"), P(SEQ, "head"), P(SEQ), P(SEQ), P(SEQ))

    return jax.shard_map(
        on_device, mesh=torus, in_specs=placed, out_specs=(P(SEQ, "head"), P()), check_vma=False
    )
```

```python
import functools
import math

import jax
import jax.numpy as jnp
from jax import lax
from jax.experimental import pallas as pl
from jax.experimental.pallas import tpu as pltpu
from jax.sharding import Mesh
from jax.sharding import PartitionSpec as P

QUERY_HEADS = 32
KEY_VALUE_HEADS = 8
HEAD_WIDTH = 128
GROUP = QUERY_HEADS // KEY_VALUE_HEADS
SEQ = ("seq_0", "seq_1", "seq_2")
SEQ_HEAD = ("seq_0", "seq_1", "seq_2", "head")
ROWS = 512
TILE = 128
TILES = ROWS // TILE
LOCAL_KV = 2
HEADS = LOCAL_KV * GROUP
LOWEST = -1e30
EXP2_SCALE = math.log2(math.e) / math.sqrt(HEAD_WIDTH)
NOWHERE = ROWS


def aligned(start, size):
    return pl.ds(start if isinstance(start, int) else pl.multiple_of(start, size), size)


def tile_rows(tile):
    return aligned(tile * TILE, TILE)


def columns(head):
    return slice(head * HEAD_WIDTH, (head + 1) * HEAD_WIDTH)


def dot(a, b, contract_b):
    return lax.dot_general(
        a, b, (((1,), (contract_b,)), ((), ())), preferred_element_type=jnp.float32
    )


def heads_of(kv):
    return range(kv * GROUP, (kv + 1) * GROUP)


def lane_groups(x):
    return [x[:, i : i + 128] for i in range(0, x.shape[1], 128)]


def folded(op, parts):
    while len(parts) > 1:
        parts = [op(*parts[i : i + 2]) if i + 1 < len(parts) else parts[i] for i in range(0, len(parts), 2)]
    return parts[0]


def widened(x, width):
    return jnp.concatenate([x] * (width // 128), axis=1)


def attend(q_ref, block_ref, tile, width, seen, old, new):
    rows = tile_rows(tile)

    def score(kv):
        q = jnp.concatenate([q_ref[rows, columns(h)] for h in heads_of(kv)], axis=0)
        return dot(q, block_ref[0, 0:width, columns(kv)], 1)

    def weigh(kv, scores):
        rounded, states = [], []
        for g, head in enumerate(heads_of(kv)):
            part = jnp.where(seen, scores[g * TILE : (g + 1) * TILE], LOWEST)
            top = jnp.max(folded(jnp.maximum, lane_groups(part)), axis=1, keepdims=True)
            top = jnp.broadcast_to(top, (TILE, 128))
            before = old(head)
            ratio = None
            if before is not None:
                top = jnp.maximum(before[0], top)
                ratio = jnp.exp2((before[0] - top) * EXP2_SCALE)
            weights = jnp.exp2((part - widened(top, width)) * EXP2_SCALE)
            states.append((top, ratio))
            rounded.append(weights.astype(jnp.bfloat16))
        return jnp.concatenate(rounded, axis=0), states

    def add(kv, rounded, states):
        v = block_ref[1, 0:width, columns(kv)]
        update = dot(rounded, jnp.concatenate([v, jnp.ones_like(v)], axis=1), 0)
        for g, head in enumerate(heads_of(kv)):
            top, ratio = states[g]
            part = update[g * TILE : (g + 1) * TILE]
            sums, total = part[:, 0:HEAD_WIDTH], part[:, HEAD_WIDTH:]
            if ratio is not None:
                _, total_old, sums_old = old(head)
                sums, total = sums_old() * ratio + sums, total_old * ratio + total
            new(head, top, total, sums)

    scores = score(0)
    pending = None
    for kv in range(LOCAL_KV):
        ahead = score(kv + 1) if kv + 1 < LOCAL_KV else None
        weighed = weigh(kv, scores)
        if pending is not None:
            add(*pending)
        scores, pending = ahead, (kv, *weighed)
    add(*pending)


def reader(state, rows):
    acc_ref, top_ref, tot_ref = state
    return lambda head: (
        top_ref[head, rows, :],
        tot_ref[head, rows, :],
        lambda: acc_ref[rows, columns(head)],
    )


def writer(state, rows):
    acc_ref, top_ref, tot_ref = state

    def store(head, top, total, sums):
        top_ref[head, rows, :] = top
        tot_ref[head, rows, :] = total
        acc_ref[rows, columns(head)] = sums

    return store


def attend_earlier(q_ref, block_ref, first_ref, tile, offset, old, new):
    place = (lax.broadcasted_iota(jnp.int32, (TILE, ROWS), 1) + offset).astype(jnp.float32)
    seen = place >= widened(first_ref[tile_rows(tile), :], ROWS)
    attend(q_ref, block_ref, tile, ROWS, seen, old, new)


def reaches(spot_ref, hop_ref, doc_ref, tile, offset):
    floor = spot_ref[0] - hop_ref[0] * ROWS
    earliest = jnp.maximum(doc_ref[tile * TILE], floor) - spot_ref[0]
    return (offset < 0) & (offset + ROWS > earliest)


def pack_kernel(keys_ref, values_ref, out_ref, sems):
    copies = [
        pltpu.make_async_copy(ref, out_ref.at[i], sems.at[i])
        for i, ref in enumerate((keys_ref, values_ref))
    ]
    for copy in copies:
        copy.start()
    for copy in copies:
        copy.wait()


def first_kernel(
    spot_ref, hop_ref, doc_ref, starts_ref, marks_ref, q_ref, own_ref,
    acc_ref, top_ref, tot_ref, first_ref, mark_ref,
):
    floor = spot_ref[0] - hop_ref[0] * ROWS
    state = (acc_ref, top_ref, tot_ref)
    for tile in range(TILES):
        width = (tile + 1) * TILE
        rows = tile_rows(tile)
        starts = jnp.maximum(starts_ref[tile : tile + 1, :], floor) - spot_ref[0]
        first = jnp.broadcast_to(starts.astype(jnp.float32), (TILE, 128)).T
        first_ref[rows, :] = first
        marks = marks_ref[tile : tile + 1, :].astype(jnp.float32)
        mark_ref[rows, :] = jnp.broadcast_to(marks, (TILE, 128)).T
        place = lax.broadcasted_iota(jnp.int32, (TILE, width), 1)
        row = lax.broadcasted_iota(jnp.int32, (TILE, width), 0) + tile * TILE
        seen = (place.astype(jnp.float32) >= widened(first, width)) & (place <= row)
        attend(q_ref, own_ref, tile, width, seen, lambda head: None, writer(state, rows))


def copy_tile(source, target, rows, target_rows):
    for head in range(HEADS):
        top, total, sums = reader(source, rows)(head)
        writer(target, target_rows)(head, top, total, sums())


def finish(state, rows, mark_ref, out_ref, squares_ref, tile):
    marks = mark_ref[tile_rows(tile), :]
    squares = jnp.zeros((TILE, HEAD_WIDTH), jnp.float32)
    for head in range(HEADS):
        _, total, sums = reader(state, rows)(head)
        attended = sums() * (1.0 / total)
        out_ref[tile_rows(tile), columns(head)] = attended.astype(jnp.bfloat16)
        squares += attended * attended
    squares *= marks
    squares_ref[...] += jnp.sum(squares.reshape(TILE // 8, 8, HEAD_WIDTH), axis=0)


def last_offsets(spot_ref):
    return (-4 * ROWS, jnp.where(spot_ref[1] == 1, NOWHERE, -3 * ROWS))


def near_kernel(
    spot_ref, hop_ref, doc_ref, q_ref, near_ref, first_ref, acc_in, top_in, tot_in,
    acc_ref, top_ref, tot_ref,
):
    source, state = (acc_in, top_in, tot_in), (acc_ref, top_ref, tot_ref)
    offset = jnp.where(spot_ref[1] == 1, -ROWS, NOWHERE)

    def step(tile, carry):
        rows = tile_rows(tile)
        needed = reaches(spot_ref, hop_ref, doc_ref, tile, offset)

        @pl.when(needed)
        def _():
            attend_earlier(
                q_ref, near_ref, first_ref, tile, offset,
                reader(source, rows), writer(state, rows),
            )

        @pl.when(jnp.logical_not(needed))
        def _():
            copy_tile(source, state, rows, rows)

        return carry

    lax.fori_loop(0, TILES, step, 0)


def middle_kernel(
    spot_ref, hop_ref, doc_ref, q_ref, far_ref, side_ref, first_ref, mark_ref,
    acc_in, top_in, tot_in, acc_ref, top_ref, tot_ref, out_ref, squares_ref,
):
    source, state = (acc_in, top_in, tot_in), (acc_ref, top_ref, tot_ref)
    odd = spot_ref[1] == 1
    slots = (
        (far_ref, -2 * ROWS),
        (side_ref, jnp.where(odd, -3 * ROWS, -ROWS)),
    )
    squares_ref[...] = jnp.zeros_like(squares_ref)

    def step(tile, carry):
        rows = tile_rows(tile)
        copy_tile(source, state, rows, rows)
        for block_ref, offset in slots:

            @pl.when(reaches(spot_ref, hop_ref, doc_ref, tile, offset))
            def _():
                attend_earlier(
                    q_ref, block_ref, first_ref, tile, offset,
                    reader(state, rows), writer(state, rows),
                )

        late = [reaches(spot_ref, hop_ref, doc_ref, tile, o) for o in last_offsets(spot_ref)]

        @pl.when(jnp.logical_not(late[0] | late[1]))
        def _():
            finish(state, rows, mark_ref, out_ref, squares_ref, tile)

        return carry

    lax.fori_loop(0, TILES, step, 0)


def last_kernel(
    spot_ref, hop_ref, doc_ref, q_ref, far_ref, side_ref, first_ref, mark_ref, acc_in, top_in,
    tot_in, done_ref, squares_in, out_ref, share_ref, acc_ref, top_ref, tot_ref, squares_ref,
):
    source, state = (acc_in, top_in, tot_in), (acc_ref, top_ref, tot_ref)
    offsets = last_offsets(spot_ref)
    squares_ref[...] = squares_in[...]
    here = slice(0, TILE)

    def step(tile, carry):
        rows = tile_rows(tile)
        late = [reaches(spot_ref, hop_ref, doc_ref, tile, offset) for offset in offsets]

        @pl.when(late[0] | late[1])
        def _():
            copy_tile(source, state, rows, here)
            for needed, block_ref, offset in zip(late, (far_ref, side_ref), offsets):

                @pl.when(needed)
                def _():
                    attend_earlier(
                        q_ref, block_ref, first_ref, tile, offset,
                        reader(state, here), writer(state, here),
                    )

            finish(state, here, mark_ref, out_ref, squares_ref, tile)

        @pl.when(jnp.logical_not(late[0] | late[1]))
        def _():
            out_ref[rows, :] = done_ref[rows, :]

        return carry

    lax.fori_loop(0, TILES, step, 0)
    squares = jnp.sum(squares_ref[...])
    count = jnp.sum(jnp.sum(mark_ref[...].reshape(ROWS // 8, 8, 128), axis=0)) * (1.0 / 128)
    lane = lax.broadcasted_iota(jnp.int32, share_ref.shape, 1)
    share_ref[...] = jnp.where(lane == 0, squares, jnp.where(lane == 1, count, 0.0))


def call(kernel, scalars, arrays, out_shapes, flops, scratch=()):
    smem = pl.BlockSpec(memory_space=pltpu.SMEM)
    vmem = pl.BlockSpec(memory_space=pltpu.VMEM)
    return pl.pallas_call(
        kernel,
        out_shape=out_shapes,
        in_specs=[smem] * len(scalars) + [vmem] * len(arrays),
        out_specs=[vmem] * len(out_shapes),
        scratch_shapes=list(scratch),
        compiler_params=pltpu.CompilerParams(vmem_limit_bytes=8 * 1024 * 1024),
        cost_estimate=pl.CostEstimate(flops=flops, bytes_accessed=2**20, transcendentals=2**21),
    )(*scalars, *arrays)


def packed(keys, values):
    return pl.pallas_call(
        pack_kernel,
        out_shape=jax.ShapeDtypeStruct((2, *keys.shape), keys.dtype),
        in_specs=[pl.BlockSpec(memory_space=pltpu.HBM)] * 2,
        out_specs=pl.BlockSpec(memory_space=pltpu.VMEM),
        scratch_shapes=[pltpu.SemaphoreType.DMA((2,))],
        compiler_params=pltpu.CompilerParams(vmem_limit_bytes=4 * 1024 * 1024),
    )(keys, values)


def objective_kernel(copies, shares_ref, out_ref):
    sums = jnp.sum(shares_ref[...], axis=0, keepdims=True)
    lane = lax.broadcasted_iota(jnp.int32, sums.shape, 1)
    squares = jnp.sum(jnp.where(lane == 0, sums, 0.0))
    count = jnp.sum(jnp.where(lane == 1, sums, 0.0)) * (1.0 / copies)
    out_ref[0] = squares / (QUERY_HEADS * count)


def objective_of(shares, copies):
    return pl.pallas_call(
        functools.partial(objective_kernel, copies),
        out_shape=f32(1),
        in_specs=[pl.BlockSpec(memory_space=pltpu.VMEM)],
        out_specs=pl.BlockSpec(memory_space=pltpu.SMEM),
        compiler_params=pltpu.CompilerParams(vmem_limit_bytes=4 * 1024 * 1024),
    )(shares).reshape(())


def onward(shard):
    devices = lax.axis_size(SEQ)
    return lax.ppermute(shard, SEQ, [(i, i + 2) for i in range(devices - 2)])


def across(shard, pairs):
    return lax.ppermute(shard, "seq_2", pairs)


def f32(*shape):
    return jax.ShapeDtypeStruct(shape, jnp.float32)


def on_device(queries, keys, values, doc_start, hop_counts, loss_mask):
    spot = jnp.stack([lax.axis_index(SEQ) * ROWS, lax.axis_index("seq_2")])
    scalars = [spot, hop_counts, doc_start]
    own = packed(keys, values)
    far_2 = onward(own)
    side_1 = across(own, [(0, 1)])
    state_shapes = [f32(ROWS, HEADS * HEAD_WIDTH), f32(HEADS, ROWS, 128), f32(HEADS, ROWS, 128)]
    *state, first, mark = call(
        first_kernel,
        scalars,
        [doc_start.reshape(TILES, TILE), loss_mask.reshape(TILES, TILE), queries, own],
        state_shapes + [f32(ROWS, 128)] * 2,
        2 * 10**9,
    )
    state = call(near_kernel, scalars, [queries, side_1, first, *state], state_shapes, 10**9)
    far_4 = onward(far_2)
    side_2 = across(far_2, [(0, 1), (1, 0)])
    out_shape = jax.ShapeDtypeStruct((ROWS, HEADS * HEAD_WIDTH), jnp.bfloat16)
    *state, done, squares = call(
        middle_kernel,
        scalars,
        [queries, far_2, side_2, first, mark, *state],
        state_shapes + [out_shape, f32(8, 128)],
        2 * 10**9,
    )
    side_3 = across(far_4, [(1, 0)])
    devices = lax.axis_size(SEQ_HEAD)
    attention, share = call(
        last_kernel,
        scalars,
        [queries, far_4, side_3, first, mark, *state, done, squares],
        [out_shape, f32(devices, 128)],
        10**9,
        scratch=[
            pltpu.VMEM((TILE, HEADS * HEAD_WIDTH), jnp.float32),
            pltpu.VMEM((HEADS, TILE, 128), jnp.float32),
            pltpu.VMEM((HEADS, TILE, 128), jnp.float32),
            pltpu.VMEM((8, 128), jnp.float32),
        ],
    )
    shares = lax.all_to_all(share, SEQ_HEAD, 0, 0, tiled=True)
    return (attention, objective_of(shares, lax.axis_size("head")))


def solution(mesh):
    torus = Mesh(
        mesh.devices.reshape(4, 8, 2, mesh.shape["head"]), ("seq_0", "seq_1", "seq_2", "head")
    )
    placed = (P(SEQ, "head"), P(SEQ, "head"), P(SEQ, "head"), P(SEQ), P(SEQ), P(SEQ))

    return jax.shard_map(
        on_device, mesh=torus, in_specs=placed, out_specs=(P(SEQ, "head"), P()), check_vma=False
    )
```

```python
import functools
import math

import jax
import jax.numpy as jnp
from jax import lax
from jax.experimental import pallas as pl
from jax.experimental.pallas import tpu as pltpu
from jax.sharding import Mesh
from jax.sharding import PartitionSpec as P

QUERY_HEADS = 32
KEY_VALUE_HEADS = 8
HEAD_WIDTH = 128
GROUP = QUERY_HEADS // KEY_VALUE_HEADS
SEQ = ("seq_0", "seq_1", "seq_2")
SEQ_HEAD = ("seq_0", "seq_1", "seq_2", "head")
ROWS = 512
TILE = 128
TILES = ROWS // TILE
PART = 32
LOCAL_KV = 2
HEADS = LOCAL_KV * GROUP
LOWEST = -1e30
EXP2_SCALE = math.log2(math.e) / math.sqrt(HEAD_WIDTH)
NOWHERE = ROWS


def aligned(start, by, size=None):
    return pl.ds(start if isinstance(start, int) else pl.multiple_of(start, by), size or by)


def tile_rows(tile):
    return aligned(tile * TILE, TILE)


def columns(head):
    return slice(head * HEAD_WIDTH, (head + 1) * HEAD_WIDTH)


def dot(a, b, contract_b):
    return lax.dot_general(
        a, b, (((1,), (contract_b,)), ((), ())), preferred_element_type=jnp.float32
    )


def heads_of(kv):
    return range(kv * GROUP, (kv + 1) * GROUP)


def lane_groups(x):
    return [x[:, i : i + 128] for i in range(0, x.shape[1], 128)]


def folded(op, parts):
    while len(parts) > 1:
        parts = [op(*parts[i : i + 2]) if i + 1 < len(parts) else parts[i] for i in range(0, len(parts), 2)]
    return parts[0]


def widened(x, width):
    return jnp.concatenate([x] * (width // 128), axis=1)


def attend(q_ref, block_ref, rows, size, width, seen, old, new):
    def score(kv):
        q = jnp.concatenate([q_ref[rows, columns(h)] for h in heads_of(kv)], axis=0)
        return dot(q, block_ref[0, 0:width, columns(kv)], 1)

    def weigh(kv, scores):
        rounded, states = [], []
        for g, head in enumerate(heads_of(kv)):
            part = jnp.where(seen, scores[g * size : (g + 1) * size], LOWEST)
            top = jnp.max(folded(jnp.maximum, lane_groups(part)), axis=1, keepdims=True)
            top = jnp.broadcast_to(top, (size, 128))
            before = old(head)
            ratio = None
            if before is not None:
                top = jnp.maximum(before[0], top)
                ratio = jnp.exp2((before[0] - top) * EXP2_SCALE)
            weights = jnp.exp2((part - widened(top, width)) * EXP2_SCALE)
            states.append((top, ratio))
            rounded.append(weights.astype(jnp.bfloat16))
        return jnp.concatenate(rounded, axis=0), states

    def add(kv, rounded, states):
        v = block_ref[1, 0:width, columns(kv)]
        update = dot(rounded, jnp.concatenate([v, jnp.ones_like(v)], axis=1), 0)
        for g, head in enumerate(heads_of(kv)):
            top, ratio = states[g]
            part = update[g * size : (g + 1) * size]
            sums, total = part[:, 0:HEAD_WIDTH], part[:, HEAD_WIDTH:]
            if ratio is not None:
                _, total_old, sums_old = old(head)
                sums, total = sums_old() * ratio + sums, total_old * ratio + total
            new(head, top, total, sums)

    scores = score(0)
    pending = None
    for kv in range(LOCAL_KV):
        ahead = score(kv + 1) if kv + 1 < LOCAL_KV else None
        weighed = weigh(kv, scores)
        if pending is not None:
            add(*pending)
        scores, pending = ahead, (kv, *weighed)
    add(*pending)


def reader(state, rows):
    acc_ref, top_ref, tot_ref = state
    return lambda head: (
        top_ref[head, rows, :],
        tot_ref[head, rows, :],
        lambda: acc_ref[rows, columns(head)],
    )


def writer(state, rows):
    acc_ref, top_ref, tot_ref = state

    def store(head, top, total, sums):
        top_ref[head, rows, :] = top
        tot_ref[head, rows, :] = total
        acc_ref[rows, columns(head)] = sums

    return store


def attend_earlier(q_ref, block_ref, first_ref, rows, size, offset, old, new):
    place = (lax.broadcasted_iota(jnp.int32, (size, ROWS), 1) + offset).astype(jnp.float32)
    seen = place >= widened(first_ref[rows, :], ROWS)
    attend(q_ref, block_ref, rows, size, ROWS, seen, old, new)


def reaches(spot_ref, hop_ref, doc_ref, row, offset):
    floor = spot_ref[0] - hop_ref[0] * ROWS
    earliest = jnp.maximum(doc_ref[row], floor) - spot_ref[0]
    return (offset < 0) & (offset + ROWS > earliest)


def first_kernel(
    spot_ref, hop_ref, doc_ref, starts_ref, marks_ref, q_ref, own_ref,
    acc_ref, top_ref, tot_ref, first_ref, mark_ref,
):
    floor = spot_ref[0] - hop_ref[0] * ROWS
    state = (acc_ref, top_ref, tot_ref)
    for tile in range(TILES):
        width = (tile + 1) * TILE
        rows = tile_rows(tile)
        starts = jnp.maximum(starts_ref[tile : tile + 1, :], floor) - spot_ref[0]
        first = jnp.broadcast_to(starts.astype(jnp.float32), (TILE, 128)).T
        first_ref[rows, :] = first
        marks = marks_ref[tile : tile + 1, :].astype(jnp.float32)
        mark_ref[rows, :] = jnp.broadcast_to(marks, (TILE, 128)).T
        place = lax.broadcasted_iota(jnp.int32, (TILE, width), 1)
        row = lax.broadcasted_iota(jnp.int32, (TILE, width), 0) + tile * TILE
        seen = (place.astype(jnp.float32) >= widened(first, width)) & (place <= row)
        attend(q_ref, own_ref, rows, TILE, width, seen, lambda head: None, writer(state, rows))


def copy_tile(source, target, rows, target_rows):
    for head in range(HEADS):
        top, total, sums = reader(source, rows)(head)
        writer(target, target_rows)(head, top, total, sums())


def finish(state, rows, size, mark_ref, out_ref, squares_ref, places):
    squares = jnp.zeros((size, HEAD_WIDTH), jnp.float32)
    for head in range(HEADS):
        _, total, sums = reader(state, rows)(head)
        attended = sums() * (1.0 / total)
        out_ref[places, columns(head)] = attended.astype(jnp.bfloat16)
        squares += attended * attended
    squares *= mark_ref[places, :]
    squares_ref[...] += jnp.sum(squares.reshape(size // 8, 8, HEAD_WIDTH), axis=0)


def out_copy(from_ref, out_ref, sems, tile):
    rows = tile_rows(tile)
    return pltpu.make_async_copy(from_ref.at[rows, :], out_ref.at[rows, :], sems.at[tile])


def last_offsets(spot_ref):
    return (-4 * ROWS, jnp.where(spot_ref[1] == 1, NOWHERE, -3 * ROWS))


def near_kernel(
    spot_ref, hop_ref, doc_ref, q_ref, near_ref, first_ref, acc_in, top_in, tot_in,
    acc_ref, top_ref, tot_ref,
):
    source, state = (acc_in, top_in, tot_in), (acc_ref, top_ref, tot_ref)
    offset = jnp.where(spot_ref[1] == 1, -ROWS, NOWHERE)

    def step(tile, carry):
        rows = tile_rows(tile)
        needed = reaches(spot_ref, hop_ref, doc_ref, tile * TILE, offset)

        @pl.when(needed)
        def _():
            attend_earlier(
                q_ref, near_ref, first_ref, rows, TILE, offset,
                reader(source, rows), writer(state, rows),
            )

        @pl.when(jnp.logical_not(needed))
        def _():
            copy_tile(source, state, rows, rows)

        return carry

    lax.fori_loop(0, TILES, step, 0)


def middle_kernel(
    spot_ref, hop_ref, doc_ref, q_ref, far_ref, side_ref, first_ref, mark_ref,
    acc_in, top_in, tot_in, acc_ref, top_ref, tot_ref, out_ref, squares_ref, done_ref, sems,
):
    source, state = (acc_in, top_in, tot_in), (acc_ref, top_ref, tot_ref)
    slots = (
        (far_ref, -2 * ROWS),
        (side_ref, jnp.where(spot_ref[1] == 1, -3 * ROWS, -ROWS)),
    )
    squares_ref[...] = jnp.zeros_like(squares_ref)

    def is_late(tile):
        a, b = [
            reaches(spot_ref, hop_ref, doc_ref, tile * TILE, offset)
            for offset in last_offsets(spot_ref)
        ]
        return a | b

    def step(tile, carry):
        rows = tile_rows(tile)
        copy_tile(source, state, rows, rows)
        for block_ref, offset in slots:

            @pl.when(reaches(spot_ref, hop_ref, doc_ref, tile * TILE, offset))
            def _():
                attend_earlier(
                    q_ref, block_ref, first_ref, rows, TILE, offset,
                    reader(state, rows), writer(state, rows),
                )

        @pl.when(jnp.logical_not(is_late(tile)))
        def _():
            finish(state, rows, TILE, mark_ref, done_ref, squares_ref, rows)

        @pl.when(tile > 0)
        def _():
            send(tile - 1)

        return carry

    def send(tile):
        @pl.when(jnp.logical_not(is_late(tile)))
        def _():
            out_copy(done_ref, out_ref, sems, tile).start()

    lax.fori_loop(0, TILES, step, 0)
    send(TILES - 1)
    for tile in range(TILES):

        @pl.when(jnp.logical_not(is_late(tile)))
        def _():
            out_copy(done_ref, out_ref, sems, tile).wait()


def last_offsets(spot_ref):
    return (-4 * ROWS, jnp.where(spot_ref[1] == 1, NOWHERE, -3 * ROWS))


def last_kernel(
    spot_ref, hop_ref, doc_ref, q_ref, far_ref, side_ref, first_ref, mark_ref, acc_in, top_in,
    tot_in, squares_in, out_in, out_ref, share_ref, acc_ref, top_ref, tot_ref, squares_ref,
    done_ref, sems,
):
    source, state = (acc_in, top_in, tot_in), (acc_ref, top_ref, tot_ref)
    slots = list(zip((far_ref, side_ref), last_offsets(spot_ref)))
    squares_ref[...] = squares_in[...]

    def late_from(row):
        a, b = [reaches(spot_ref, hop_ref, doc_ref, row, offset) for _, offset in slots]
        return a | b

    def absorb(places, size, row):
        here = slice(0, size)
        copy_tile(source, state, places, here)
        for block_ref, offset in slots:

            @pl.when(reaches(spot_ref, hop_ref, doc_ref, row, offset))
            def _():
                attend_earlier(
                    q_ref, block_ref, first_ref, places, size, offset,
                    reader(state, here), writer(state, here),
                )

        finish(state, here, size, mark_ref, done_ref, squares_ref, places)

    def step(tile, carry):
        @pl.when(late_from(tile * TILE))
        def _():
            whole = late_from(tile * TILE + PART)

            @pl.when(whole)
            def _():
                absorb(tile_rows(tile), TILE, tile * TILE)

            @pl.when(jnp.logical_not(whole))
            def _():
                absorb(aligned(tile * TILE, PART), PART, tile * TILE)
                rest = aligned(tile * TILE + PART, PART, TILE - PART)
                finish(source, rest, TILE - PART, mark_ref, done_ref, squares_ref, rest)

        return carry

    lax.fori_loop(0, TILES, step, 0)
    squares = jnp.sum(squares_ref[...])
    count = jnp.sum(jnp.sum(mark_ref[...].reshape(ROWS // 8, 8, 128), axis=0)) * (1.0 / 128)
    lane = lax.broadcasted_iota(jnp.int32, share_ref.shape, 1)
    share_ref[...] = jnp.where(lane == 0, squares, jnp.where(lane == 1, count, 0.0))
    for ended in (False, True):
        for tile in range(TILES):

            @pl.when(late_from(tile * TILE))
            def _():
                copy = out_copy(done_ref, out_ref, sems, tile)
                copy.wait() if ended else copy.start()


def call(
    kernel, scalars, arrays, out_shapes, flops, scratch=(), in_hbm=0, out_hbm=None, alias=None
):
    smem, vmem, hbm = [
        pl.BlockSpec(memory_space=space) for space in (pltpu.SMEM, pltpu.VMEM, pltpu.HBM)
    ]
    return pl.pallas_call(
        kernel,
        out_shape=out_shapes,
        in_specs=[smem] * len(scalars) + [vmem] * (len(arrays) - in_hbm) + [hbm] * in_hbm,
        out_specs=[hbm if i == out_hbm else vmem for i in range(len(out_shapes))],
        scratch_shapes=list(scratch),
        input_output_aliases=alias or {},
        compiler_params=pltpu.CompilerParams(vmem_limit_bytes=8 * 1024 * 1024),
        cost_estimate=pl.CostEstimate(flops=flops, bytes_accessed=2**20, transcendentals=2**21),
    )(*scalars, *arrays)


def packed(keys, values):
    pads = ((0, 0), (0, 0))
    return jnp.pad(keys[None], ((0, 1), *pads)) + jnp.pad(values[None], ((1, 0), *pads))


def objective_kernel(copies, shares_ref, out_ref):
    sums = jnp.sum(shares_ref[...], axis=0, keepdims=True)
    lane = lax.broadcasted_iota(jnp.int32, sums.shape, 1)
    squares = jnp.sum(jnp.where(lane == 0, sums, 0.0))
    count = jnp.sum(jnp.where(lane == 1, sums, 0.0)) * (1.0 / copies)
    out_ref[0] = squares / (QUERY_HEADS * count)


def objective_of(shares, copies):
    return pl.pallas_call(
        functools.partial(objective_kernel, copies),
        out_shape=f32(1),
        in_specs=[pl.BlockSpec(memory_space=pltpu.VMEM)],
        out_specs=pl.BlockSpec(memory_space=pltpu.SMEM),
        compiler_params=pltpu.CompilerParams(vmem_limit_bytes=4 * 1024 * 1024),
    )(shares).reshape(())


def onward(shard):
    devices = lax.axis_size(SEQ)
    return lax.ppermute(shard, SEQ, [(i, i + 2) for i in range(devices - 2)])


def across(shard, pairs):
    return lax.ppermute(shard, "seq_2", pairs)


def f32(*shape):
    return jax.ShapeDtypeStruct(shape, jnp.float32)


def on_device(queries, keys, values, doc_start, hop_counts, loss_mask):
    spot = jnp.stack([lax.axis_index(SEQ) * ROWS, lax.axis_index("seq_2")])
    scalars = [spot, hop_counts, doc_start]
    own = packed(keys, values)
    far_2 = onward(own)
    side_1 = across(own, [(0, 1)])
    state_shapes = [f32(ROWS, HEADS * HEAD_WIDTH), f32(HEADS, ROWS, 128), f32(HEADS, ROWS, 128)]
    *state, first, mark = call(
        first_kernel,
        scalars,
        [doc_start.reshape(TILES, TILE), loss_mask.reshape(TILES, TILE), queries, own],
        state_shapes + [f32(ROWS, 128)] * 2,
        2 * 10**9,
    )
    state = call(near_kernel, scalars, [queries, side_1, first, *state], state_shapes, 10**9)
    far_4 = onward(far_2)
    side_2 = across(far_2, [(0, 1), (1, 0)])
    out_shape = jax.ShapeDtypeStruct((ROWS, HEADS * HEAD_WIDTH), jnp.bfloat16)
    copy_scratch = [pltpu.VMEM(out_shape.shape, jnp.bfloat16), pltpu.SemaphoreType.DMA((TILES,))]
    *state, done, squares = call(
        middle_kernel,
        scalars,
        [queries, far_2, side_2, first, mark, *state],
        state_shapes + [out_shape, f32(8, 128)],
        2 * 10**9,
        scratch=copy_scratch,
        out_hbm=3,
    )
    side_3 = across(far_4, [(1, 0)])
    devices = lax.axis_size(SEQ_HEAD)
    arrays = [queries, far_4, side_3, first, mark, *state, squares, done]
    attention, share = call(
        last_kernel,
        scalars,
        arrays,
        [out_shape, f32(devices, 128)],
        10**9,
        scratch=[
            pltpu.VMEM((TILE, HEADS * HEAD_WIDTH), jnp.float32),
            pltpu.VMEM((HEADS, TILE, 128), jnp.float32),
            pltpu.VMEM((HEADS, TILE, 128), jnp.float32),
            pltpu.VMEM((8, 128), jnp.float32),
            *copy_scratch,
        ],
        in_hbm=1,
        out_hbm=0,
        alias={len(scalars) + len(arrays) - 1: 0},
    )
    shares = lax.all_to_all(share, SEQ_HEAD, 0, 0, tiled=True)
    return (attention, objective_of(shares, lax.axis_size("head")))


def solution(mesh):
    torus = Mesh(
        mesh.devices.reshape(4, 8, 2, mesh.shape["head"]), ("seq_0", "seq_1", "seq_2", "head")
    )
    placed = (P(SEQ, "head"), P(SEQ, "head"), P(SEQ, "head"), P(SEQ), P(SEQ), P(SEQ))

    return jax.shard_map(
        on_device, mesh=torus, in_specs=placed, out_specs=(P(SEQ, "head"), P()), check_vma=False
    )
```

```python
import functools
import math

import jax
import jax.numpy as jnp
from jax import lax
from jax.experimental import pallas as pl
from jax.experimental.pallas import tpu as pltpu
from jax.sharding import Mesh
from jax.sharding import PartitionSpec as P

QUERY_HEADS = 32
KEY_VALUE_HEADS = 8
HEAD_WIDTH = 128
GROUP = QUERY_HEADS // KEY_VALUE_HEADS
SEQ = ("seq_0", "seq_1", "seq_2")
SEQ_HEAD = ("seq_0", "seq_1", "seq_2", "head")
ROWS = 512
TILE = 128
TILES = ROWS // TILE
PART = 32
LOCAL_KV = 2
HEADS = LOCAL_KV * GROUP
LOWEST = -1e30
EXP2_SCALE = math.log2(math.e) / math.sqrt(HEAD_WIDTH)
NOWHERE = ROWS


def aligned(start, by, size=None):
    return pl.ds(start if isinstance(start, int) else pl.multiple_of(start, by), size or by)


def tile_rows(tile):
    return aligned(tile * TILE, TILE)


def columns(head):
    return slice(head * HEAD_WIDTH, (head + 1) * HEAD_WIDTH)


def dot(a, b, contract_b):
    return lax.dot_general(
        a, b, (((1,), (contract_b,)), ((), ())), preferred_element_type=jnp.float32
    )


def heads_of(kv):
    return range(kv * GROUP, (kv + 1) * GROUP)


def lane_groups(x):
    return [x[:, i : i + 128] for i in range(0, x.shape[1], 128)]


def folded(op, parts):
    while len(parts) > 1:
        parts = [op(*parts[i : i + 2]) if i + 1 < len(parts) else parts[i] for i in range(0, len(parts), 2)]
    return parts[0]


def widened(x, width):
    return jnp.concatenate([x] * (width // 128), axis=1)


def attend(q_ref, block_ref, rows, size, width, seen, old, new):
    def score(kv):
        q = jnp.concatenate([q_ref[rows, columns(h)] for h in heads_of(kv)], axis=0)
        return dot(q, block_ref[0, 0:width, columns(kv)], 1)

    def weigh(kv, scores):
        rounded, states = [], []
        for g, head in enumerate(heads_of(kv)):
            part = jnp.where(seen, scores[g * size : (g + 1) * size], LOWEST)
            top = jnp.max(folded(jnp.maximum, lane_groups(part)), axis=1, keepdims=True)
            top = jnp.broadcast_to(top, (size, 128))
            before = old(head)
            ratio = None
            if before is not None:
                top = jnp.maximum(before[0], top)
                ratio = jnp.exp2((before[0] - top) * EXP2_SCALE)
            weights = jnp.exp2((part - widened(top, width)) * EXP2_SCALE)
            states.append((top, ratio))
            rounded.append(weights.astype(jnp.bfloat16))
        return jnp.concatenate(rounded, axis=0), states

    def add(kv, rounded, states):
        v = block_ref[1, 0:width, columns(kv)]
        update = dot(rounded, jnp.concatenate([v, jnp.ones_like(v)], axis=1), 0)
        for g, head in enumerate(heads_of(kv)):
            top, ratio = states[g]
            part = update[g * size : (g + 1) * size]
            sums, total = part[:, 0:HEAD_WIDTH], part[:, HEAD_WIDTH:]
            if ratio is not None:
                _, total_old, sums_old = old(head)
                sums, total = sums_old() * ratio + sums, total_old * ratio + total
            new(head, top, total, sums)

    scores = score(0)
    pending = None
    for kv in range(LOCAL_KV):
        ahead = score(kv + 1) if kv + 1 < LOCAL_KV else None
        weighed = weigh(kv, scores)
        if pending is not None:
            add(*pending)
        scores, pending = ahead, (kv, *weighed)
    add(*pending)


def reader(state, rows):
    acc_ref, top_ref, tot_ref = state
    return lambda head: (
        top_ref[head, rows, :],
        tot_ref[head, rows, :],
        lambda: acc_ref[rows, columns(head)],
    )


def writer(state, rows):
    acc_ref, top_ref, tot_ref = state

    def store(head, top, total, sums):
        top_ref[head, rows, :] = top
        tot_ref[head, rows, :] = total
        acc_ref[rows, columns(head)] = sums

    return store


def attend_earlier(q_ref, block_ref, first_ref, rows, size, offset, old, new):
    place = (lax.broadcasted_iota(jnp.int32, (size, ROWS), 1) + offset).astype(jnp.float32)
    seen = place >= widened(first_ref[rows, :], ROWS)
    attend(q_ref, block_ref, rows, size, ROWS, seen, old, new)


def reaches(spot_ref, hop_ref, doc_ref, row, offset):
    floor = spot_ref[0] - hop_ref[0] * ROWS
    earliest = jnp.maximum(doc_ref[row], floor) - spot_ref[0]
    return (offset < 0) & (offset + ROWS > earliest)


def first_kernel(
    spot_ref, hop_ref, doc_ref, starts_ref, marks_ref, q_ref, own_ref,
    acc_ref, top_ref, tot_ref, first_ref, mark_ref,
):
    floor = spot_ref[0] - hop_ref[0] * ROWS
    state = (acc_ref, top_ref, tot_ref)
    for tile in range(TILES):
        width = (tile + 1) * TILE
        rows = tile_rows(tile)
        starts = jnp.maximum(starts_ref[tile : tile + 1, :], floor) - spot_ref[0]
        first = jnp.broadcast_to(starts.astype(jnp.float32), (TILE, 128)).T
        first_ref[rows, :] = first
        marks = marks_ref[tile : tile + 1, :].astype(jnp.float32)
        mark_ref[rows, :] = jnp.broadcast_to(marks, (TILE, 128)).T
        place = lax.broadcasted_iota(jnp.int32, (TILE, width), 1)
        row = lax.broadcasted_iota(jnp.int32, (TILE, width), 0) + tile * TILE
        seen = (place.astype(jnp.float32) >= widened(first, width)) & (place <= row)
        attend(q_ref, own_ref, rows, TILE, width, seen, lambda head: None, writer(state, rows))


def copy_tile(source, target, rows, target_rows):
    for head in range(HEADS):
        top, total, sums = reader(source, rows)(head)
        writer(target, target_rows)(head, top, total, sums())


def finish(state, rows, size, mark_ref, out_ref, squares_ref, places):
    squares = jnp.zeros((size, HEAD_WIDTH), jnp.float32)
    for head in range(HEADS):
        _, total, sums = reader(state, rows)(head)
        attended = sums() * (1.0 / total)
        out_ref[places, columns(head)] = attended.astype(jnp.bfloat16)
        squares += attended * attended
    squares *= mark_ref[places, :]
    squares_ref[...] += jnp.sum(squares.reshape(size // 8, 8, HEAD_WIDTH), axis=0)


def out_copy(from_ref, out_ref, sems, tile):
    rows = tile_rows(tile)
    return pltpu.make_async_copy(from_ref.at[rows, :], out_ref.at[rows, :], sems.at[tile])


def on_core(spot_ref, core, distance):
    return jnp.where(spot_ref[1] == core, -distance * ROWS, NOWHERE)


def near_kernel(
    spot_ref, hop_ref, doc_ref, q_ref, near_ref, far_ref, first_ref, acc_in, top_in, tot_in,
    acc_ref, top_ref, tot_ref,
):
    source, state = (acc_in, top_in, tot_in), (acc_ref, top_ref, tot_ref)
    slots = ((near_ref, on_core(spot_ref, 1, 1)), (far_ref, on_core(spot_ref, 1, 2)))

    def step(tile, carry):
        rows = tile_rows(tile)
        copy_tile(source, state, rows, rows)
        for block_ref, offset in slots:

            @pl.when(reaches(spot_ref, hop_ref, doc_ref, tile * TILE, offset))
            def _():
                attend_earlier(
                    q_ref, block_ref, first_ref, rows, TILE, offset,
                    reader(state, rows), writer(state, rows),
                )

        return carry

    lax.fori_loop(0, TILES, step, 0)


def middle_kernel(
    spot_ref, hop_ref, doc_ref, q_ref, near_ref, far_ref, side_ref, first_ref, mark_ref,
    acc_in, top_in, tot_in, acc_ref, top_ref, tot_ref, out_ref, squares_ref, done_ref, sems,
):
    source, state = (acc_in, top_in, tot_in), (acc_ref, top_ref, tot_ref)
    slots = (
        (near_ref, on_core(spot_ref, 0, 1)),
        (far_ref, on_core(spot_ref, 0, 2)),
        (side_ref, on_core(spot_ref, 1, 3)),
    )
    squares_ref[...] = jnp.zeros_like(squares_ref)

    def is_late(tile):
        return late_from(spot_ref, hop_ref, doc_ref, tile * TILE)

    def step(tile, carry):
        rows = tile_rows(tile)
        copy_tile(source, state, rows, rows)
        for block_ref, offset in slots:

            @pl.when(reaches(spot_ref, hop_ref, doc_ref, tile * TILE, offset))
            def _():
                attend_earlier(
                    q_ref, block_ref, first_ref, rows, TILE, offset,
                    reader(state, rows), writer(state, rows),
                )

        @pl.when(jnp.logical_not(is_late(tile)))
        def _():
            finish(state, rows, TILE, mark_ref, done_ref, squares_ref, rows)

        @pl.when(tile > 0)
        def _():
            send(tile - 1)

        return carry

    def send(tile):
        @pl.when(jnp.logical_not(is_late(tile)))
        def _():
            out_copy(done_ref, out_ref, sems, tile).start()

    lax.fori_loop(0, TILES, step, 0)
    send(TILES - 1)
    for tile in range(TILES):

        @pl.when(jnp.logical_not(is_late(tile)))
        def _():
            out_copy(done_ref, out_ref, sems, tile).wait()


def late_from(spot_ref, hop_ref, doc_ref, row):
    offset = jnp.where(spot_ref[1] == 1, -4 * ROWS, -3 * ROWS)
    return reaches(spot_ref, hop_ref, doc_ref, row, offset)


def last_kernel(
    spot_ref, hop_ref, doc_ref, q_ref, odd_ref, even_ref, side_ref, first_ref, mark_ref, acc_in,
    top_in, tot_in, squares_in, out_in, out_ref, share_ref, acc_ref, top_ref, tot_ref, squares_ref,
    done_ref, sems,
):
    source, state = (acc_in, top_in, tot_in), (acc_ref, top_ref, tot_ref)
    slots = (
        (odd_ref, on_core(spot_ref, 1, 4)),
        (side_ref, on_core(spot_ref, 0, 3)),
        (even_ref, on_core(spot_ref, 0, 4)),
    )
    late = functools.partial(late_from, spot_ref, hop_ref, doc_ref)
    squares_ref[...] = squares_in[...]

    def absorb(places, size, row):
        here = slice(0, size)
        copy_tile(source, state, places, here)
        for block_ref, offset in slots:

            @pl.when(reaches(spot_ref, hop_ref, doc_ref, row, offset))
            def _():
                attend_earlier(
                    q_ref, block_ref, first_ref, places, size, offset,
                    reader(state, here), writer(state, here),
                )

        finish(state, here, size, mark_ref, done_ref, squares_ref, places)

    def step(tile, carry):
        @pl.when(late(tile * TILE))
        def _():
            whole = late(tile * TILE + PART)

            @pl.when(whole)
            def _():
                absorb(tile_rows(tile), TILE, tile * TILE)

            @pl.when(jnp.logical_not(whole))
            def _():
                absorb(aligned(tile * TILE, PART), PART, tile * TILE)
                rest = aligned(tile * TILE + PART, PART, TILE - PART)
                finish(source, rest, TILE - PART, mark_ref, done_ref, squares_ref, rest)

        return carry

    lax.fori_loop(0, TILES, step, 0)
    squares = jnp.sum(squares_ref[...])
    count = jnp.sum(jnp.sum(mark_ref[...].reshape(ROWS // 8, 8, 128), axis=0)) * (1.0 / 128)
    lane = lax.broadcasted_iota(jnp.int32, share_ref.shape, 1)
    share_ref[...] = jnp.where(lane == 0, squares, jnp.where(lane == 1, count, 0.0))
    for ended in (False, True):
        for tile in range(TILES):

            @pl.when(late(tile * TILE))
            def _():
                copy = out_copy(done_ref, out_ref, sems, tile)
                copy.wait() if ended else copy.start()


def call(
    kernel, scalars, arrays, out_shapes, flops, scratch=(), in_hbm=0, out_hbm=None, alias=None
):
    smem, vmem, hbm = [
        pl.BlockSpec(memory_space=space) for space in (pltpu.SMEM, pltpu.VMEM, pltpu.HBM)
    ]
    return pl.pallas_call(
        kernel,
        out_shape=out_shapes,
        in_specs=[smem] * len(scalars) + [vmem] * (len(arrays) - in_hbm) + [hbm] * in_hbm,
        out_specs=[hbm if i == out_hbm else vmem for i in range(len(out_shapes))],
        scratch_shapes=list(scratch),
        input_output_aliases=alias or {},
        compiler_params=pltpu.CompilerParams(vmem_limit_bytes=8 * 1024 * 1024),
        cost_estimate=pl.CostEstimate(flops=flops, bytes_accessed=2**20, transcendentals=2**21),
    )(*scalars, *arrays)


def packed(keys, values):
    pads = ((0, 0), (0, 0))
    return jnp.pad(keys[None], ((0, 1), *pads)) + jnp.pad(values[None], ((1, 0), *pads))


def objective_kernel(copies, shares_ref, out_ref):
    sums = jnp.sum(shares_ref[...], axis=0, keepdims=True)
    lane = lax.broadcasted_iota(jnp.int32, sums.shape, 1)
    squares = jnp.sum(jnp.where(lane == 0, sums, 0.0))
    count = jnp.sum(jnp.where(lane == 1, sums, 0.0)) * (1.0 / copies)
    out_ref[0] = squares / (QUERY_HEADS * count)


def objective_of(shares, copies):
    return pl.pallas_call(
        functools.partial(objective_kernel, copies),
        out_shape=f32(1),
        in_specs=[pl.BlockSpec(memory_space=pltpu.VMEM)],
        out_specs=pl.BlockSpec(memory_space=pltpu.SMEM),
        compiler_params=pltpu.CompilerParams(vmem_limit_bytes=4 * 1024 * 1024),
    )(shares).reshape(())


def onward(shard, core):
    return lax.ppermute(shard, SEQ, [(i, i + 2) for i in range(core, lax.axis_size(SEQ) - 2, 2)])


def across(shard, core):
    return lax.ppermute(shard, "seq_2", [(core, 1 - core)])


def f32(*shape):
    return jax.ShapeDtypeStruct(shape, jnp.float32)


def on_device(queries, keys, values, doc_start, hop_counts, loss_mask):
    spot = jnp.stack([lax.axis_index(SEQ) * ROWS, lax.axis_index("seq_2")])
    scalars = [spot, hop_counts, doc_start]
    own = packed(keys, values)
    odd_2 = onward(own, 1)
    side_1 = across(own, 0)
    even_2 = onward(own, 0)
    state_shapes = [f32(ROWS, HEADS * HEAD_WIDTH), f32(HEADS, ROWS, 128), f32(HEADS, ROWS, 128)]
    *state, first, mark = call(
        first_kernel,
        scalars,
        [doc_start.reshape(TILES, TILE), loss_mask.reshape(TILES, TILE), queries, own],
        state_shapes + [f32(ROWS, 128)] * 2,
        2 * 10**9,
    )
    odd_4 = onward(odd_2, 1)
    side_2 = across(odd_2, 1)
    state = call(
        near_kernel, scalars, [queries, side_1, odd_2, first, *state], state_shapes, 2 * 10**9
    )
    even_4 = onward(even_2, 0)
    side_3 = across(even_2, 0)
    out_shape = jax.ShapeDtypeStruct((ROWS, HEADS * HEAD_WIDTH), jnp.bfloat16)
    copy_scratch = [pltpu.VMEM(out_shape.shape, jnp.bfloat16), pltpu.SemaphoreType.DMA((TILES,))]
    *state, done, squares = call(
        middle_kernel,
        scalars,
        [queries, side_2, even_2, side_3, first, mark, *state],
        state_shapes + [out_shape, f32(8, 128)],
        2 * 10**9,
        scratch=copy_scratch,
        out_hbm=3,
    )
    side_4 = across(odd_4, 1)
    devices = lax.axis_size(SEQ_HEAD)
    arrays = [queries, odd_4, even_4, side_4, first, mark, *state, squares, done]
    attention, share = call(
        last_kernel,
        scalars,
        arrays,
        [out_shape, f32(devices, 128)],
        10**9,
        scratch=[
            pltpu.VMEM((TILE, HEADS * HEAD_WIDTH), jnp.float32),
            pltpu.VMEM((HEADS, TILE, 128), jnp.float32),
            pltpu.VMEM((HEADS, TILE, 128), jnp.float32),
            pltpu.VMEM((8, 128), jnp.float32),
            *copy_scratch,
        ],
        in_hbm=1,
        out_hbm=0,
        alias={len(scalars) + len(arrays) - 1: 0},
    )
    shares = lax.all_to_all(share, SEQ_HEAD, 0, 0, tiled=True)
    return (attention, objective_of(shares, lax.axis_size("head")))


def solution(mesh):
    torus = Mesh(
        mesh.devices.reshape(4, 8, 2, mesh.shape["head"]), ("seq_0", "seq_1", "seq_2", "head")
    )
    placed = (P(SEQ, "head"), P(SEQ, "head"), P(SEQ, "head"), P(SEQ), P(SEQ), P(SEQ))

    return jax.shard_map(
        on_device, mesh=torus, in_specs=placed, out_specs=(P(SEQ, "head"), P()), check_vma=False
    )
```

```python
import functools
import math

import jax
import jax.numpy as jnp
from jax import lax
from jax.experimental import pallas as pl
from jax.experimental.pallas import tpu as pltpu
from jax.sharding import Mesh
from jax.sharding import PartitionSpec as P

QUERY_HEADS = 32
KEY_VALUE_HEADS = 8
HEAD_WIDTH = 128
GROUP = QUERY_HEADS // KEY_VALUE_HEADS
SEQ = ("seq_0", "seq_1", "seq_2")
SEQ_HEAD = ("seq_0", "seq_1", "seq_2", "head")
ROWS = 512
TILE = 128
TILES = ROWS // TILE
PART = 32
PAIR = 2 * TILE
LOCAL_KV = 2
HEADS = LOCAL_KV * GROUP
LOWEST = -1e30
EXP2_SCALE = math.log2(math.e) / math.sqrt(HEAD_WIDTH)
NOWHERE = ROWS


def aligned(start, by, size=None):
    return pl.ds(start if isinstance(start, int) else pl.multiple_of(start, by), size or by)


def tile_rows(tile):
    return aligned(tile * TILE, TILE)


def columns(head):
    return slice(head * HEAD_WIDTH, (head + 1) * HEAD_WIDTH)


def dot(a, b, contract_b):
    return lax.dot_general(
        a, b, (((1,), (contract_b,)), ((), ())), preferred_element_type=jnp.float32
    )


def heads_of(kv):
    return range(kv * GROUP, (kv + 1) * GROUP)


def lane_groups(x):
    return [x[:, i : i + 128] for i in range(0, x.shape[1], 128)]


def folded(op, parts):
    while len(parts) > 1:
        parts = [op(*parts[i : i + 2]) if i + 1 < len(parts) else parts[i] for i in range(0, len(parts), 2)]
    return parts[0]


def widened(x, width):
    return jnp.concatenate([x] * (width // 128), axis=1)


def attend(q_ref, block_ref, parts, size):
    steps = [(part, kv) for part in parts for kv in range(LOCAL_KV)]

    def score(step):
        (rows, width, *_), kv = step
        q = jnp.concatenate([q_ref[rows, columns(h)] for h in heads_of(kv)], axis=0)
        return dot(q, block_ref[0, 0:width, columns(kv)], 1)

    def weigh(step, scores):
        (_, width, seen, old, _), kv = step
        rounded, states = [], []
        for g, head in enumerate(heads_of(kv)):
            part = jnp.where(seen, scores[g * size : (g + 1) * size], LOWEST)
            top = jnp.max(folded(jnp.maximum, lane_groups(part)), axis=1, keepdims=True)
            top = jnp.broadcast_to(top, (size, 128))
            before = old(head)
            ratio = None
            if before is not None:
                top = jnp.maximum(before[0], top)
                ratio = jnp.exp2((before[0] - top) * EXP2_SCALE)
            weights = jnp.exp2((part - widened(top, width)) * EXP2_SCALE)
            states.append((top, ratio))
            rounded.append(weights.astype(jnp.bfloat16))
        return jnp.concatenate(rounded, axis=0), states

    def add(step, rounded, states):
        (_, width, _, old, new), kv = step
        v = block_ref[1, 0:width, columns(kv)]
        update = dot(rounded, jnp.concatenate([v, jnp.ones_like(v)], axis=1), 0)
        for g, head in enumerate(heads_of(kv)):
            top, ratio = states[g]
            part = update[g * size : (g + 1) * size]
            sums, total = part[:, 0:HEAD_WIDTH], part[:, HEAD_WIDTH:]
            if ratio is not None:
                _, total_old, sums_old = old(head)
                sums, total = sums_old() * ratio + sums, total_old * ratio + total
            new(head, top, total, sums)

    scores, pending = score(steps[0]), None
    for at, step in enumerate(steps):
        ahead = score(steps[at + 1]) if at + 1 < len(steps) else None
        weighed = weigh(step, scores)
        if pending is not None:
            add(*pending)
        scores, pending = ahead, (step, *weighed)
    add(*pending)


def reader(state, rows):
    acc_ref, top_ref, tot_ref = state
    return lambda head: (
        top_ref[head, rows, :],
        tot_ref[head, rows, :],
        lambda: acc_ref[rows, columns(head)],
    )


def writer(state, rows):
    acc_ref, top_ref, tot_ref = state

    def store(head, top, total, sums):
        top_ref[head, rows, :] = top
        tot_ref[head, rows, :] = total
        acc_ref[rows, columns(head)] = sums

    return store


def attend_earlier(q_ref, block_ref, first_ref, places, size, offset, source, state):
    parts = []
    for rows, rows_in, rows_out in places:
        place = (lax.broadcasted_iota(jnp.int32, (size, ROWS), 1) + offset).astype(jnp.float32)
        seen = place >= widened(first_ref[rows, :], ROWS)
        parts.append((rows, ROWS, seen, reader(source, rows_in), writer(state, rows_out)))
    attend(q_ref, block_ref, parts, size)


def pair_rows(pair):
    return [aligned(pair * PAIR + i, TILE) for i in range(0, PAIR, TILE)]


def same(rows):
    return [(r, r, r) for r in rows]


def reaches(spot_ref, hop_ref, doc_ref, row, offset):
    floor = spot_ref[0] - hop_ref[0] * ROWS
    earliest = jnp.maximum(doc_ref[row], floor) - spot_ref[0]
    return (offset < 0) & (offset + ROWS > earliest)


def first_kernel(
    spot_ref, hop_ref, doc_ref, starts_ref, marks_ref, q_ref, own_ref,
    acc_ref, top_ref, tot_ref, first_ref, mark_ref,
):
    floor = spot_ref[0] - hop_ref[0] * ROWS
    state = (acc_ref, top_ref, tot_ref)
    parts = []
    for tile in range(TILES):
        width = (tile + 1) * TILE
        rows = tile_rows(tile)
        starts = jnp.maximum(starts_ref[tile : tile + 1, :], floor) - spot_ref[0]
        first = jnp.broadcast_to(starts.astype(jnp.float32), (TILE, 128)).T
        first_ref[rows, :] = first
        marks = marks_ref[tile : tile + 1, :].astype(jnp.float32)
        mark_ref[rows, :] = jnp.broadcast_to(marks, (TILE, 128)).T
        place = lax.broadcasted_iota(jnp.int32, (TILE, width), 1)
        row = lax.broadcasted_iota(jnp.int32, (TILE, width), 0) + tile * TILE
        seen = (place.astype(jnp.float32) >= widened(first, width)) & (place <= row)
        parts.append((rows, width, seen, lambda head: None, writer(state, rows)))
    attend(q_ref, own_ref, parts, TILE)


def copy_tile(source, target, rows, target_rows):
    for head in range(HEADS):
        top, total, sums = reader(source, rows)(head)
        writer(target, target_rows)(head, top, total, sums())


def finish(state, rows, size, mark_ref, out_ref, squares_ref, places):
    squares = jnp.zeros((size, HEAD_WIDTH), jnp.float32)
    for head in range(HEADS):
        _, total, sums = reader(state, rows)(head)
        attended = sums() * (1.0 / total)
        out_ref[places, columns(head)] = attended.astype(jnp.bfloat16)
        squares += attended * attended
    squares *= mark_ref[places, :]
    squares_ref[...] += jnp.sum(squares.reshape(size // 8, 8, HEAD_WIDTH), axis=0)


def out_copy(from_ref, out_ref, sems, tile):
    rows = tile_rows(tile)
    return pltpu.make_async_copy(from_ref.at[rows, :], out_ref.at[rows, :], sems.at[tile])


def near_kernel(
    spot_ref, hop_ref, doc_ref, q_ref, near_ref, first_ref, acc_in, top_in, tot_in,
    acc_ref, top_ref, tot_ref,
):
    source, state = (acc_in, top_in, tot_in), (acc_ref, top_ref, tot_ref)
    offset = on_core(spot_ref, 1, 1)

    def step(pair, carry):
        rows = pair_rows(pair)
        needed = reaches(spot_ref, hop_ref, doc_ref, pair * PAIR, offset)

        @pl.when(needed)
        def _():
            attend_earlier(q_ref, near_ref, first_ref, same(rows), TILE, offset, source, state)

        @pl.when(jnp.logical_not(needed))
        def _():
            for part in rows:
                copy_tile(source, state, part, part)

        return carry

    lax.fori_loop(0, ROWS // PAIR, step, 0)


def on_core(spot_ref, core, distance):
    return jnp.where(spot_ref[1] == core, -distance * ROWS, NOWHERE)


def middle_kernel(
    spot_ref, hop_ref, doc_ref, q_ref, far_ref, side_ref, first_ref, mark_ref,
    acc_in, top_in, tot_in, acc_ref, top_ref, tot_ref, out_ref, squares_ref, done_ref, sems,
):
    source, state = (acc_in, top_in, tot_in), (acc_ref, top_ref, tot_ref)
    offsets = (-2 * ROWS, jnp.where(spot_ref[1] == 1, -3 * ROWS, -ROWS))
    squares_ref[...] = jnp.zeros_like(squares_ref)

    def is_late(tile):
        return late_from(spot_ref, hop_ref, doc_ref, tile * TILE)

    def step(pair, carry):
        rows = pair_rows(pair)
        far, side = [reaches(spot_ref, hop_ref, doc_ref, pair * PAIR, offset) for offset in offsets]

        @pl.when(far)
        def _():
            attend_earlier(q_ref, far_ref, first_ref, same(rows), TILE, offsets[0], source, state)

        @pl.when(jnp.logical_not(far))
        def _():
            for part in rows:
                copy_tile(source, state, part, part)

        @pl.when(side)
        def _():
            attend_earlier(q_ref, side_ref, first_ref, same(rows), TILE, offsets[1], state, state)

        for i, part in enumerate(rows):

            @pl.when(jnp.logical_not(is_late(pair * len(rows) + i)))
            def _():
                finish(state, part, TILE, mark_ref, done_ref, squares_ref, part)

        @pl.when(pair > 0)
        def _():
            for i in range(len(rows)):
                send((pair - 1) * len(rows) + i)

        return carry

    def send(tile):
        @pl.when(jnp.logical_not(is_late(tile)))
        def _():
            out_copy(done_ref, out_ref, sems, tile).start()

    lax.fori_loop(0, ROWS // PAIR, step, 0)
    for tile in range(TILES - PAIR // TILE, TILES):
        send(tile)
    for tile in range(TILES):

        @pl.when(jnp.logical_not(is_late(tile)))
        def _():
            out_copy(done_ref, out_ref, sems, tile).wait()


def late_from(spot_ref, hop_ref, doc_ref, row):
    offset = jnp.where(spot_ref[1] == 1, -4 * ROWS, -3 * ROWS)
    return reaches(spot_ref, hop_ref, doc_ref, row, offset)


def last_kernel(
    spot_ref, hop_ref, doc_ref, q_ref, odd_ref, even_ref, side_ref, first_ref, mark_ref, acc_in,
    top_in, tot_in, squares_in, out_in, out_ref, share_ref, acc_ref, top_ref, tot_ref, squares_ref,
    done_ref, sems,
):
    source, state = (acc_in, top_in, tot_in), (acc_ref, top_ref, tot_ref)
    slots = (
        (odd_ref, on_core(spot_ref, 1, 4)),
        (side_ref, on_core(spot_ref, 0, 3)),
        (even_ref, on_core(spot_ref, 0, 4)),
    )
    late = functools.partial(late_from, spot_ref, hop_ref, doc_ref)
    squares_ref[...] = squares_in[...]

    def absorb(places, size, row):
        here = slice(0, size)
        copy_tile(source, state, places, here)
        for block_ref, offset in slots:

            @pl.when(reaches(spot_ref, hop_ref, doc_ref, row, offset))
            def _():
                attend_earlier(
                    q_ref, block_ref, first_ref, [(places, here, here)], size, offset, state, state
                )

        finish(state, here, size, mark_ref, done_ref, squares_ref, places)

    def step(tile, carry):
        @pl.when(late(tile * TILE))
        def _():
            whole = late(tile * TILE + PART)

            @pl.when(whole)
            def _():
                absorb(tile_rows(tile), TILE, tile * TILE)

            @pl.when(jnp.logical_not(whole))
            def _():
                absorb(aligned(tile * TILE, PART), PART, tile * TILE)
                rest = aligned(tile * TILE + PART, PART, TILE - PART)
                finish(source, rest, TILE - PART, mark_ref, done_ref, squares_ref, rest)

        return carry

    lax.fori_loop(0, TILES, step, 0)
    squares = jnp.sum(squares_ref[...])
    count = jnp.sum(jnp.sum(mark_ref[...].reshape(ROWS // 8, 8, 128), axis=0)) * (1.0 / 128)
    lane = lax.broadcasted_iota(jnp.int32, share_ref.shape, 1)
    share_ref[...] = jnp.where(lane == 0, squares, jnp.where(lane == 1, count, 0.0))
    for ended in (False, True):
        for tile in range(TILES):

            @pl.when(late(tile * TILE))
            def _():
                copy = out_copy(done_ref, out_ref, sems, tile)
                copy.wait() if ended else copy.start()


def call(
    kernel, scalars, arrays, out_shapes, flops, scratch=(), in_hbm=0, out_hbm=None, alias=None
):
    smem, vmem, hbm = [
        pl.BlockSpec(memory_space=space) for space in (pltpu.SMEM, pltpu.VMEM, pltpu.HBM)
    ]
    return pl.pallas_call(
        kernel,
        out_shape=out_shapes,
        in_specs=[smem] * len(scalars) + [vmem] * (len(arrays) - in_hbm) + [hbm] * in_hbm,
        out_specs=[hbm if i == out_hbm else vmem for i in range(len(out_shapes))],
        scratch_shapes=list(scratch),
        input_output_aliases=alias or {},
        compiler_params=pltpu.CompilerParams(vmem_limit_bytes=8 * 1024 * 1024),
        cost_estimate=pl.CostEstimate(flops=flops, bytes_accessed=2**20, transcendentals=2**21),
    )(*scalars, *arrays)


def packed(keys, values):
    pads = ((0, 0), (0, 0))
    return jnp.pad(keys[None], ((0, 1), *pads)) + jnp.pad(values[None], ((1, 0), *pads))


def objective_kernel(copies, shares_ref, out_ref):
    sums = jnp.sum(shares_ref[...], axis=0, keepdims=True)
    lane = lax.broadcasted_iota(jnp.int32, sums.shape, 1)
    squares = jnp.sum(jnp.where(lane == 0, sums, 0.0))
    count = jnp.sum(jnp.where(lane == 1, sums, 0.0)) * (1.0 / copies)
    out_ref[0] = squares / (QUERY_HEADS * count)


def objective_of(shares, copies):
    return pl.pallas_call(
        functools.partial(objective_kernel, copies),
        out_shape=f32(1),
        in_specs=[pl.BlockSpec(memory_space=pltpu.VMEM)],
        out_specs=pl.BlockSpec(memory_space=pltpu.SMEM),
        compiler_params=pltpu.CompilerParams(vmem_limit_bytes=4 * 1024 * 1024),
    )(shares).reshape(())


def onward(shard, cores):
    blocks = range(lax.axis_size(SEQ) - 2)
    return lax.ppermute(shard, SEQ, [(i, i + 2) for i in blocks if i % 2 in cores])


def across(shard, pairs):
    return lax.ppermute(shard, "seq_2", pairs)


def f32(*shape):
    return jax.ShapeDtypeStruct(shape, jnp.float32)


def on_device(queries, keys, values, doc_start, hop_counts, loss_mask):
    spot = jnp.stack([lax.axis_index(SEQ) * ROWS, lax.axis_index("seq_2")])
    scalars = [spot, hop_counts, doc_start]
    own = packed(keys, values)
    far_2 = onward(own, (0, 1))
    side_1 = across(own, [(0, 1)])
    state_shapes = [f32(ROWS, HEADS * HEAD_WIDTH), f32(HEADS, ROWS, 128), f32(HEADS, ROWS, 128)]
    *state, first, mark = call(
        first_kernel,
        scalars,
        [doc_start.reshape(TILES, TILE), loss_mask.reshape(TILES, TILE), queries, own],
        state_shapes + [f32(ROWS, 128)] * 2,
        2 * 10**9,
    )
    state = call(near_kernel, scalars, [queries, side_1, first, *state], state_shapes, 10**9)
    odd_4 = onward(far_2, (1,))
    side_2 = across(far_2, [(0, 1), (1, 0)])
    even_4 = onward(far_2, (0,))
    out_shape = jax.ShapeDtypeStruct((ROWS, HEADS * HEAD_WIDTH), jnp.bfloat16)
    copy_scratch = [pltpu.VMEM(out_shape.shape, jnp.bfloat16), pltpu.SemaphoreType.DMA((TILES,))]
    *state, done, squares = call(
        middle_kernel,
        scalars,
        [queries, far_2, side_2, first, mark, *state],
        state_shapes + [out_shape, f32(8, 128)],
        2 * 10**9,
        scratch=copy_scratch,
        out_hbm=3,
    )
    side_3 = across(odd_4, [(1, 0)])
    devices = lax.axis_size(SEQ_HEAD)
    arrays = [queries, odd_4, even_4, side_3, first, mark, *state, squares, done]
    attention, share = call(
        last_kernel,
        scalars,
        arrays,
        [out_shape, f32(devices, 128)],
        10**9,
        scratch=[
            pltpu.VMEM((TILE, HEADS * HEAD_WIDTH), jnp.float32),
            pltpu.VMEM((HEADS, TILE, 128), jnp.float32),
            pltpu.VMEM((HEADS, TILE, 128), jnp.float32),
            pltpu.VMEM((8, 128), jnp.float32),
            *copy_scratch,
        ],
        in_hbm=1,
        out_hbm=0,
        alias={len(scalars) + len(arrays) - 1: 0},
    )
    shares = lax.all_to_all(share, SEQ_HEAD, 0, 0, tiled=True)
    return (attention, objective_of(shares, lax.axis_size("head")))


def solution(mesh):
    torus = Mesh(
        mesh.devices.reshape(4, 8, 2, mesh.shape["head"]), ("seq_0", "seq_1", "seq_2", "head")
    )
    placed = (P(SEQ, "head"), P(SEQ, "head"), P(SEQ, "head"), P(SEQ), P(SEQ), P(SEQ))

    return jax.shard_map(
        on_device, mesh=torus, in_specs=placed, out_specs=(P(SEQ, "head"), P()), check_vma=False
    )
```

```python
import functools
import math

import jax
import jax.numpy as jnp
from jax import lax
from jax.experimental import pallas as pl
from jax.experimental.pallas import tpu as pltpu
from jax.sharding import Mesh
from jax.sharding import PartitionSpec as P

QUERY_HEADS = 32
KEY_VALUE_HEADS = 8
HEAD_WIDTH = 128
GROUP = QUERY_HEADS // KEY_VALUE_HEADS
SEQ = ("seq_0", "seq_1", "seq_2")
SEQ_HEAD = ("seq_0", "seq_1", "seq_2", "head")
ROWS = 512
TILE = 128
TILES = ROWS // TILE
PART = 32
PAIR = 2 * TILE
LOCAL_KV = 2
HEADS = LOCAL_KV * GROUP
LOWEST = -1e30
EXP2_SCALE = math.log2(math.e) / math.sqrt(HEAD_WIDTH)
NOWHERE = ROWS


def aligned(start, by, size=None):
    return pl.ds(start if isinstance(start, int) else pl.multiple_of(start, by), size or by)


def tile_rows(tile):
    return aligned(tile * TILE, TILE)


def columns(head):
    return slice(head * HEAD_WIDTH, (head + 1) * HEAD_WIDTH)


def dot(a, b, contract_b):
    return lax.dot_general(
        a, b, (((1,), (contract_b,)), ((), ())), preferred_element_type=jnp.float32
    )


def heads_of(kv):
    return range(kv * GROUP, (kv + 1) * GROUP)


def lane_groups(x):
    return [x[:, i : i + 128] for i in range(0, x.shape[1], 128)]


def folded(op, parts):
    while len(parts) > 1:
        parts = [op(*parts[i : i + 2]) if i + 1 < len(parts) else parts[i] for i in range(0, len(parts), 2)]
    return parts[0]


def widened(x, width):
    return jnp.concatenate([x] * (width // 128), axis=1)


def attend(q_ref, block_ref, parts, size):
    steps = [(part, kv) for part in parts for kv in range(LOCAL_KV)]

    def score(step):
        (rows, width, *_), kv = step
        q = jnp.concatenate([q_ref[rows, columns(h)] for h in heads_of(kv)], axis=0)
        return dot(q, block_ref[0, 0:width, columns(kv)], 1)

    def weigh(step, scores):
        (_, width, seen, old, _), kv = step
        rounded, states = [], []
        for g, head in enumerate(heads_of(kv)):
            part = jnp.where(seen, scores[g * size : (g + 1) * size], LOWEST)
            top = jnp.max(folded(jnp.maximum, lane_groups(part)), axis=1, keepdims=True)
            top = jnp.broadcast_to(top, (size, 128))
            before = old(head)
            ratio = None
            if before is not None:
                top = jnp.maximum(before[0], top)
                ratio = jnp.exp2((before[0] - top) * EXP2_SCALE)
            weights = jnp.exp2((part - widened(top, width)) * EXP2_SCALE)
            states.append((top, ratio))
            rounded.append(weights.astype(jnp.bfloat16))
        return jnp.concatenate(rounded, axis=0), states

    def add(step, rounded, states):
        (_, width, _, old, new), kv = step
        v = block_ref[1, 0:width, columns(kv)]
        update = dot(rounded, jnp.concatenate([v, jnp.ones_like(v)], axis=1), 0)
        for g, head in enumerate(heads_of(kv)):
            top, ratio = states[g]
            part = update[g * size : (g + 1) * size]
            sums, total = part[:, 0:HEAD_WIDTH], part[:, HEAD_WIDTH:]
            if ratio is not None:
                _, total_old, sums_old = old(head)
                sums, total = sums_old() * ratio + sums, total_old * ratio + total
            new(head, top, total, sums)

    scores, pending = score(steps[0]), None
    for at, step in enumerate(steps):
        ahead = score(steps[at + 1]) if at + 1 < len(steps) else None
        weighed = weigh(step, scores)
        if pending is not None:
            add(*pending)
        scores, pending = ahead, (step, *weighed)
    add(*pending)


def reader(state, rows):
    acc_ref, top_ref, tot_ref = state
    return lambda head: (
        top_ref[head, rows, :],
        tot_ref[head, rows, :],
        lambda: acc_ref[rows, columns(head)],
    )


def writer(state, rows):
    acc_ref, top_ref, tot_ref = state

    def store(head, top, total, sums):
        top_ref[head, rows, :] = top
        tot_ref[head, rows, :] = total
        acc_ref[rows, columns(head)] = sums

    return store


def attend_earlier(q_ref, block_ref, first_ref, places, size, offset, source, state):
    parts = []
    for rows, rows_in, rows_out in places:
        place = (lax.broadcasted_iota(jnp.int32, (size, ROWS), 1) + offset).astype(jnp.float32)
        seen = place >= widened(first_ref[rows, :], ROWS)
        parts.append((rows, ROWS, seen, reader(source, rows_in), writer(state, rows_out)))
    attend(q_ref, block_ref, parts, size)


def pair_rows(pair):
    return [aligned(pair * PAIR + i, TILE) for i in range(0, PAIR, TILE)]


def same(rows):
    return [(r, r, r) for r in rows]


def reaches(spot_ref, hop_ref, doc_ref, row, offset):
    floor = spot_ref[0] - hop_ref[0] * ROWS
    earliest = jnp.maximum(doc_ref[row], floor) - spot_ref[0]
    return (offset < 0) & (offset + ROWS > earliest)


def first_kernel(
    spot_ref, hop_ref, doc_ref, starts_ref, marks_ref, q_ref, own_ref,
    acc_ref, top_ref, tot_ref, first_ref, mark_ref,
):
    floor = spot_ref[0] - hop_ref[0] * ROWS
    state = (acc_ref, top_ref, tot_ref)
    parts = []
    for tile in range(TILES):
        width = (tile + 1) * TILE
        rows = tile_rows(tile)
        starts = jnp.maximum(starts_ref[tile : tile + 1, :], floor) - spot_ref[0]
        first = jnp.broadcast_to(starts.astype(jnp.float32), (TILE, 128)).T
        first_ref[rows, :] = first
        marks = marks_ref[tile : tile + 1, :].astype(jnp.float32)
        mark_ref[rows, :] = jnp.broadcast_to(marks, (TILE, 128)).T
        place = lax.broadcasted_iota(jnp.int32, (TILE, width), 1)
        row = lax.broadcasted_iota(jnp.int32, (TILE, width), 0) + tile * TILE
        seen = (place.astype(jnp.float32) >= widened(first, width)) & (place <= row)
        parts.append((rows, width, seen, lambda head: None, writer(state, rows)))
    attend(q_ref, own_ref, parts, TILE)


def copy_tile(source, target, rows, target_rows):
    for head in range(HEADS):
        top, total, sums = reader(source, rows)(head)
        writer(target, target_rows)(head, top, total, sums())


def finish(state, rows, size, mark_ref, out_ref, squares_ref, places):
    squares = jnp.zeros((size, HEAD_WIDTH), jnp.float32)
    for head in range(HEADS):
        _, total, sums = reader(state, rows)(head)
        attended = sums() * (1.0 / total)
        out_ref[places, columns(head)] = attended.astype(jnp.bfloat16)
        squares += attended * attended
    squares *= mark_ref[places, :]
    squares_ref[...] += jnp.sum(squares.reshape(size // 8, 8, HEAD_WIDTH), axis=0)


def out_copy(from_ref, out_ref, sems, tile):
    rows = tile_rows(tile)
    return pltpu.make_async_copy(from_ref.at[rows, :], out_ref.at[rows, :], sems.at[tile])


def near_kernel(
    spot_ref, hop_ref, doc_ref, q_ref, near_ref, first_ref, acc_in, top_in, tot_in,
    acc_ref, top_ref, tot_ref,
):
    source, state = (acc_in, top_in, tot_in), (acc_ref, top_ref, tot_ref)
    offset = on_core(spot_ref, 1, 1)

    def step(pair, carry):
        rows = pair_rows(pair)
        needed = reaches(spot_ref, hop_ref, doc_ref, pair * PAIR, offset)

        @pl.when(needed)
        def _():
            attend_earlier(q_ref, near_ref, first_ref, same(rows), TILE, offset, source, state)

        @pl.when(jnp.logical_not(needed))
        def _():
            for part in rows:
                copy_tile(source, state, part, part)

        return carry

    lax.fori_loop(0, ROWS // PAIR, step, 0)


def on_core(spot_ref, core, distance):
    return jnp.where(spot_ref[1] == core, -distance * ROWS, NOWHERE)


def side_offset(spot_ref):
    return jnp.where(spot_ref[1] == 1, -3 * ROWS, -ROWS)


def far_kernel(
    spot_ref, hop_ref, doc_ref, q_ref, far_ref, side_ref, first_ref, mark_ref,
    acc_in, top_in, tot_in, acc_ref, top_ref, tot_ref, done_ref, squares_ref,
):
    source, state = (acc_in, top_in, tot_in), (acc_ref, top_ref, tot_ref)
    far, side = -2 * ROWS, side_offset(spot_ref)
    squares_ref[...] = jnp.zeros_like(squares_ref)

    def step(pair, carry):
        rows = pair_rows(pair)
        needed = reaches(spot_ref, hop_ref, doc_ref, pair * PAIR, far)

        @pl.when(needed)
        def _():
            attend_earlier(q_ref, far_ref, first_ref, same(rows), TILE, far, source, state)

        @pl.when(jnp.logical_not(needed))
        def _():
            for part in rows:
                copy_tile(source, state, part, part)

        return carry

    lax.fori_loop(0, ROWS // PAIR, step, 0)

    @pl.when(reaches(spot_ref, hop_ref, doc_ref, 0, side))
    def _():
        attend_earlier(q_ref, side_ref, first_ref, same(pair_rows(0)), TILE, side, state, state)

    for tile in range(PAIR // TILE):

        @pl.when(jnp.logical_not(late_from(spot_ref, hop_ref, doc_ref, tile * TILE)))
        def _():
            rows = tile_rows(tile)
            finish(state, rows, TILE, mark_ref, done_ref, squares_ref, rows)


def side_kernel(
    spot_ref, hop_ref, doc_ref, q_ref, side_ref, first_ref, mark_ref, acc_in, top_in, tot_in,
    done_in, squares_in, acc_ref, top_ref, tot_ref, out_ref, squares_ref, done_ref, sems,
):
    source, state = (acc_in, top_in, tot_in), (acc_ref, top_ref, tot_ref)
    side = side_offset(spot_ref)
    early, after = range(PAIR // TILE), range(PAIR // TILE, TILES)
    squares_ref[...] = squares_in[...]

    def if_done(tile, act):
        pl.when(jnp.logical_not(late_from(spot_ref, hop_ref, doc_ref, tile * TILE)))(act)

    def moved(tile, act):
        copy = out_copy(done_in if tile in early else done_ref, out_ref, sems, tile)
        if_done(tile, getattr(copy, act))

    for tile in early:
        moved(tile, "start")

        @pl.when(late_from(spot_ref, hop_ref, doc_ref, tile * TILE))
        def _():
            copy_tile(source, state, tile_rows(tile), tile_rows(tile))

    rows = pair_rows(1)
    needed = reaches(spot_ref, hop_ref, doc_ref, PAIR, side)

    @pl.when(needed)
    def _():
        attend_earlier(q_ref, side_ref, first_ref, same(rows), TILE, side, source, state)

    @pl.when(jnp.logical_not(needed))
    def _():
        for part in rows:
            copy_tile(source, state, part, part)

    for tile in after:

        def act():
            part = tile_rows(tile)
            finish(state, part, TILE, mark_ref, done_ref, squares_ref, part)

        if_done(tile, act)
    for tile in after:
        moved(tile, "start")
    for tile in range(TILES):
        moved(tile, "wait")


def late_from(spot_ref, hop_ref, doc_ref, row):
    offset = jnp.where(spot_ref[1] == 1, -4 * ROWS, -3 * ROWS)
    return reaches(spot_ref, hop_ref, doc_ref, row, offset)


def last_kernel(
    spot_ref, hop_ref, doc_ref, q_ref, odd_ref, even_ref, side_ref, first_ref, mark_ref, acc_in,
    top_in, tot_in, squares_in, out_in, out_ref, share_ref, acc_ref, top_ref, tot_ref, squares_ref,
    done_ref, sems,
):
    source, state = (acc_in, top_in, tot_in), (acc_ref, top_ref, tot_ref)
    slots = (
        (odd_ref, on_core(spot_ref, 1, 4)),
        (side_ref, on_core(spot_ref, 0, 3)),
        (even_ref, on_core(spot_ref, 0, 4)),
    )
    late = functools.partial(late_from, spot_ref, hop_ref, doc_ref)
    squares_ref[...] = squares_in[...]

    def absorb(places, size, row):
        here = slice(0, size)
        copy_tile(source, state, places, here)
        for block_ref, offset in slots:

            @pl.when(reaches(spot_ref, hop_ref, doc_ref, row, offset))
            def _():
                attend_earlier(
                    q_ref, block_ref, first_ref, [(places, here, here)], size, offset, state, state
                )

        finish(state, here, size, mark_ref, done_ref, squares_ref, places)

    def step(tile, carry):
        @pl.when(late(tile * TILE))
        def _():
            whole = late(tile * TILE + PART)

            @pl.when(whole)
            def _():
                absorb(tile_rows(tile), TILE, tile * TILE)

            @pl.when(jnp.logical_not(whole))
            def _():
                absorb(aligned(tile * TILE, PART), PART, tile * TILE)
                rest = aligned(tile * TILE + PART, PART, TILE - PART)
                finish(source, rest, TILE - PART, mark_ref, done_ref, squares_ref, rest)

        return carry

    lax.fori_loop(0, TILES, step, 0)
    squares = jnp.sum(squares_ref[...])
    count = jnp.sum(jnp.sum(mark_ref[...].reshape(ROWS // 8, 8, 128), axis=0)) * (1.0 / 128)
    lane = lax.broadcasted_iota(jnp.int32, share_ref.shape, 1)
    share_ref[...] = jnp.where(lane == 0, squares, jnp.where(lane == 1, count, 0.0))
    for ended in (False, True):
        for tile in range(TILES):

            @pl.when(late(tile * TILE))
            def _():
                copy = out_copy(done_ref, out_ref, sems, tile)
                copy.wait() if ended else copy.start()


def call(
    kernel, scalars, arrays, out_shapes, flops, scratch=(), in_hbm=0, out_hbm=None, alias=None
):
    smem, vmem, hbm = [
        pl.BlockSpec(memory_space=space) for space in (pltpu.SMEM, pltpu.VMEM, pltpu.HBM)
    ]
    return pl.pallas_call(
        kernel,
        out_shape=out_shapes,
        in_specs=[smem] * len(scalars) + [vmem] * (len(arrays) - in_hbm) + [hbm] * in_hbm,
        out_specs=[hbm if i == out_hbm else vmem for i in range(len(out_shapes))],
        scratch_shapes=list(scratch),
        input_output_aliases=alias or {},
        compiler_params=pltpu.CompilerParams(vmem_limit_bytes=8 * 1024 * 1024),
        cost_estimate=pl.CostEstimate(flops=flops, bytes_accessed=2**20, transcendentals=2**21),
    )(*scalars, *arrays)


def packed(keys, values):
    pads = ((0, 0), (0, 0))
    return jnp.pad(keys[None], ((0, 1), *pads)) + jnp.pad(values[None], ((1, 0), *pads))


def objective_kernel(copies, shares_ref, out_ref):
    sums = jnp.sum(shares_ref[...], axis=0, keepdims=True)
    lane = lax.broadcasted_iota(jnp.int32, sums.shape, 1)
    squares = jnp.sum(jnp.where(lane == 0, sums, 0.0))
    count = jnp.sum(jnp.where(lane == 1, sums, 0.0)) * (1.0 / copies)
    out_ref[0] = squares / (QUERY_HEADS * count)


def objective_of(shares, copies):
    return pl.pallas_call(
        functools.partial(objective_kernel, copies),
        out_shape=f32(1),
        in_specs=[pl.BlockSpec(memory_space=pltpu.VMEM)],
        out_specs=pl.BlockSpec(memory_space=pltpu.SMEM),
        compiler_params=pltpu.CompilerParams(vmem_limit_bytes=4 * 1024 * 1024),
    )(shares).reshape(())


def onward(shard, cores):
    blocks = range(lax.axis_size(SEQ) - 2)
    return lax.ppermute(shard, SEQ, [(i, i + 2) for i in blocks if i % 2 in cores])


def across(shard, pairs):
    return lax.ppermute(shard, "seq_2", pairs)


def f32(*shape):
    return jax.ShapeDtypeStruct(shape, jnp.float32)


def on_device(queries, keys, values, doc_start, hop_counts, loss_mask):
    spot = jnp.stack([lax.axis_index(SEQ) * ROWS, lax.axis_index("seq_2")])
    scalars = [spot, hop_counts, doc_start]
    own = packed(keys, values)
    far_2 = onward(own, (0, 1))
    side_1 = across(own, [(0, 1)])
    state_shapes = [f32(ROWS, HEADS * HEAD_WIDTH), f32(HEADS, ROWS, 128), f32(HEADS, ROWS, 128)]
    *state, first, mark = call(
        first_kernel,
        scalars,
        [doc_start.reshape(TILES, TILE), loss_mask.reshape(TILES, TILE), queries, own],
        state_shapes + [f32(ROWS, 128)] * 2,
        2 * 10**9,
    )
    state = call(near_kernel, scalars, [queries, side_1, first, *state], state_shapes, 10**9)
    odd_4 = onward(far_2, (1,))
    side_2 = across(far_2, [(0, 1), (1, 0)])
    even_4 = onward(far_2, (0,))
    out_shape = jax.ShapeDtypeStruct((ROWS, HEADS * HEAD_WIDTH), jnp.bfloat16)
    copy_scratch = [pltpu.VMEM(out_shape.shape, jnp.bfloat16), pltpu.SemaphoreType.DMA((TILES,))]
    *state, done, squares = call(
        far_kernel,
        scalars,
        [queries, far_2, side_2, first, mark, *state],
        state_shapes + [out_shape, f32(8, 128)],
        2 * 10**9,
    )
    side_3 = across(odd_4, [(1, 0)])
    *state, done, squares = call(
        side_kernel,
        scalars,
        [queries, side_2, first, mark, *state, done, squares],
        state_shapes + [out_shape, f32(8, 128)],
        10**9,
        scratch=copy_scratch,
        out_hbm=3,
    )
    devices = lax.axis_size(SEQ_HEAD)
    arrays = [queries, odd_4, even_4, side_3, first, mark, *state, squares, done]
    attention, share = call(
        last_kernel,
        scalars,
        arrays,
        [out_shape, f32(devices, 128)],
        10**9,
        scratch=[
            pltpu.VMEM((TILE, HEADS * HEAD_WIDTH), jnp.float32),
            pltpu.VMEM((HEADS, TILE, 128), jnp.float32),
            pltpu.VMEM((HEADS, TILE, 128), jnp.float32),
            pltpu.VMEM((8, 128), jnp.float32),
            *copy_scratch,
        ],
        in_hbm=1,
        out_hbm=0,
        alias={len(scalars) + len(arrays) - 1: 0},
    )
    shares = lax.all_to_all(share, SEQ_HEAD, 0, 0, tiled=True)
    return (attention, objective_of(shares, lax.axis_size("head")))


def solution(mesh):
    torus = Mesh(
        mesh.devices.reshape(4, 8, 2, mesh.shape["head"]), ("seq_0", "seq_1", "seq_2", "head")
    )
    placed = (P(SEQ, "head"), P(SEQ, "head"), P(SEQ, "head"), P(SEQ), P(SEQ), P(SEQ))

    return jax.shard_map(
        on_device, mesh=torus, in_specs=placed, out_specs=(P(SEQ, "head"), P()), check_vma=False
    )
```

```python
import functools
import math

import jax
import jax.numpy as jnp
from jax import lax
from jax.experimental import pallas as pl
from jax.experimental.pallas import tpu as pltpu
from jax.sharding import Mesh
from jax.sharding import PartitionSpec as P

QUERY_HEADS = 32
KEY_VALUE_HEADS = 8
HEAD_WIDTH = 128
GROUP = QUERY_HEADS // KEY_VALUE_HEADS
SEQ = ("seq_0", "seq_1", "seq_2")
SEQ_HEAD = ("seq_0", "seq_1", "seq_2", "head")
ROWS = 512
TILE = 128
TILES = ROWS // TILE
PART = 32
PAIR = 2 * TILE
LOCAL_KV = 2
HEADS = LOCAL_KV * GROUP
LOWEST = -1e30
EXP2_SCALE = math.log2(math.e) / math.sqrt(HEAD_WIDTH)
NOWHERE = ROWS


def aligned(start, by, size=None):
    return pl.ds(start if isinstance(start, int) else pl.multiple_of(start, by), size or by)


def tile_rows(tile):
    return aligned(tile * TILE, TILE)


def columns(head):
    return slice(head * HEAD_WIDTH, (head + 1) * HEAD_WIDTH)


def dot(a, b, contract_b):
    return lax.dot_general(
        a, b, (((1,), (contract_b,)), ((), ())), preferred_element_type=jnp.float32
    )


def heads_of(kv):
    return range(kv * GROUP, (kv + 1) * GROUP)


def lane_groups(x):
    return [x[:, i : i + 128] for i in range(0, x.shape[1], 128)]


def folded(op, parts):
    while len(parts) > 1:
        parts = [op(*parts[i : i + 2]) if i + 1 < len(parts) else parts[i] for i in range(0, len(parts), 2)]
    return parts[0]


def widened(x, width):
    return jnp.concatenate([x] * (width // 128), axis=1)


def attend(q_ref, block_ref, parts, size):
    steps = [(part, kv) for part in parts for kv in range(LOCAL_KV)]

    def score(step):
        (rows, width, *_), kv = step
        q = jnp.concatenate([q_ref[rows, columns(h)] for h in heads_of(kv)], axis=0)
        return dot(q, block_ref[0, 0:width, columns(kv)], 1)

    def weigh(step, scores):
        (_, width, seen, old, _), kv = step
        rounded, states = [], []
        for g, head in enumerate(heads_of(kv)):
            part = jnp.where(seen, scores[g * size : (g + 1) * size], LOWEST)
            top = jnp.max(folded(jnp.maximum, lane_groups(part)), axis=1, keepdims=True)
            top = jnp.broadcast_to(top, (size, 128))
            before = old(head)
            ratio = None
            if before is not None:
                top = jnp.maximum(before[0], top)
                ratio = jnp.exp2((before[0] - top) * EXP2_SCALE)
            weights = jnp.exp2((part - widened(top, width)) * EXP2_SCALE)
            states.append((top, ratio))
            rounded.append(weights.astype(jnp.bfloat16))
        return jnp.concatenate(rounded, axis=0), states

    def add(step, rounded, states):
        (_, width, _, old, new), kv = step
        v = block_ref[1, 0:width, columns(kv)]
        update = dot(rounded, jnp.concatenate([v, jnp.ones_like(v)], axis=1), 0)
        for g, head in enumerate(heads_of(kv)):
            top, ratio = states[g]
            part = update[g * size : (g + 1) * size]
            sums, total = part[:, 0:HEAD_WIDTH], part[:, HEAD_WIDTH:]
            if ratio is not None:
                _, total_old, sums_old = old(head)
                sums, total = sums_old() * ratio + sums, total_old * ratio + total
            new(head, top, total, sums)

    scores, pending = score(steps[0]), None
    for at, step in enumerate(steps):
        ahead = score(steps[at + 1]) if at + 1 < len(steps) else None
        weighed = weigh(step, scores)
        if pending is not None:
            add(*pending)
        scores, pending = ahead, (step, *weighed)
    add(*pending)


def reader(state, rows):
    acc_ref, top_ref, tot_ref = state
    return lambda head: (
        top_ref[head, rows, :],
        tot_ref[head, rows, :],
        lambda: acc_ref[rows, columns(head)],
    )


def writer(state, rows):
    acc_ref, top_ref, tot_ref = state

    def store(head, top, total, sums):
        top_ref[head, rows, :] = top
        tot_ref[head, rows, :] = total
        acc_ref[rows, columns(head)] = sums

    return store


def attend_earlier(q_ref, block_ref, first_ref, places, size, offset, source, state):
    parts = []
    for rows, rows_in, rows_out in places:
        place = (lax.broadcasted_iota(jnp.int32, (size, ROWS), 1) + offset).astype(jnp.float32)
        seen = place >= widened(first_ref[rows, :], ROWS)
        parts.append((rows, ROWS, seen, reader(source, rows_in), writer(state, rows_out)))
    attend(q_ref, block_ref, parts, size)


def pair_rows(pair):
    return [aligned(pair * PAIR + i, TILE) for i in range(0, PAIR, TILE)]


def same(rows):
    return [(r, r, r) for r in rows]


def reaches(spot_ref, hop_ref, doc_ref, row, offset):
    floor = spot_ref[0] - hop_ref[0] * ROWS
    earliest = jnp.maximum(doc_ref[row], floor) - spot_ref[0]
    return (offset < 0) & (offset + ROWS > earliest)


def first_kernel(
    spot_ref, hop_ref, doc_ref, starts_ref, marks_ref, q_ref, own_ref,
    acc_ref, top_ref, tot_ref, first_ref, mark_ref,
):
    floor = spot_ref[0] - hop_ref[0] * ROWS
    state = (acc_ref, top_ref, tot_ref)
    parts = []
    for tile in range(TILES):
        width = (tile + 1) * TILE
        rows = tile_rows(tile)
        starts = jnp.maximum(starts_ref[tile : tile + 1, :], floor) - spot_ref[0]
        first = jnp.broadcast_to(starts.astype(jnp.float32), (TILE, 128)).T
        first_ref[rows, :] = first
        marks = marks_ref[tile : tile + 1, :].astype(jnp.float32)
        mark_ref[rows, :] = jnp.broadcast_to(marks, (TILE, 128)).T
        place = lax.broadcasted_iota(jnp.int32, (TILE, width), 1)
        row = lax.broadcasted_iota(jnp.int32, (TILE, width), 0) + tile * TILE
        seen = (place.astype(jnp.float32) >= widened(first, width)) & (place <= row)
        parts.append((rows, width, seen, lambda head: None, writer(state, rows)))
    attend(q_ref, own_ref, parts, TILE)


def copy_tile(source, target, rows, target_rows):
    for head in range(HEADS):
        top, total, sums = reader(source, rows)(head)
        writer(target, target_rows)(head, top, total, sums())


def finish(state, rows, size, mark_ref, out_ref, squares_ref, places):
    squares = jnp.zeros((size, HEAD_WIDTH), jnp.float32)
    for head in range(HEADS):
        _, total, sums = reader(state, rows)(head)
        attended = sums() * (1.0 / total)
        out_ref[places, columns(head)] = attended.astype(jnp.bfloat16)
        squares += attended * attended
    squares *= mark_ref[places, :]
    squares_ref[...] += jnp.sum(squares.reshape(size // 8, 8, HEAD_WIDTH), axis=0)


def out_copy(from_ref, out_ref, sems, tile):
    rows = tile_rows(tile)
    return pltpu.make_async_copy(from_ref.at[rows, :], out_ref.at[rows, :], sems.at[tile])


def near_kernel(
    spot_ref, hop_ref, doc_ref, q_ref, near_ref, first_ref, acc_in, top_in, tot_in,
    acc_ref, top_ref, tot_ref,
):
    source, state = (acc_in, top_in, tot_in), (acc_ref, top_ref, tot_ref)
    offset = on_core(spot_ref, 1, 1)

    def step(pair, carry):
        rows = pair_rows(pair)
        needed = reaches(spot_ref, hop_ref, doc_ref, pair * PAIR, offset)

        @pl.when(needed)
        def _():
            attend_earlier(q_ref, near_ref, first_ref, same(rows), TILE, offset, source, state)

        @pl.when(jnp.logical_not(needed))
        def _():
            for part in rows:
                copy_tile(source, state, part, part)

        return carry

    lax.fori_loop(0, ROWS // PAIR, step, 0)


def on_core(spot_ref, core, distance):
    return jnp.where(spot_ref[1] == core, -distance * ROWS, NOWHERE)


def side_offset(spot_ref):
    return jnp.where(spot_ref[1] == 1, -3 * ROWS, -ROWS)


def far_kernel(
    spot_ref, hop_ref, doc_ref, q_ref, far_ref, side_ref, first_ref, mark_ref,
    acc_in, top_in, tot_in, acc_ref, top_ref, tot_ref, done_ref, squares_ref,
):
    source, state = (acc_in, top_in, tot_in), (acc_ref, top_ref, tot_ref)
    far, side = -2 * ROWS, side_offset(spot_ref)
    squares_ref[...] = jnp.zeros_like(squares_ref)

    def step(pair, carry):
        rows = pair_rows(pair)
        needed = reaches(spot_ref, hop_ref, doc_ref, pair * PAIR, far)

        @pl.when(needed)
        def _():
            attend_earlier(q_ref, far_ref, first_ref, same(rows), TILE, far, source, state)

        @pl.when(jnp.logical_not(needed))
        def _():
            for part in rows:
                copy_tile(source, state, part, part)

        return carry

    lax.fori_loop(0, ROWS // PAIR, step, 0)

    @pl.when(reaches(spot_ref, hop_ref, doc_ref, 0, side))
    def _():
        attend_earlier(q_ref, side_ref, first_ref, same(pair_rows(0)), TILE, side, state, state)

    for tile in range(PAIR // TILE):

        @pl.when(jnp.logical_not(late_from(spot_ref, hop_ref, doc_ref, tile * TILE)))
        def _():
            rows = tile_rows(tile)
            finish(state, rows, TILE, mark_ref, done_ref, squares_ref, rows)


def side_kernel(
    spot_ref, hop_ref, doc_ref, q_ref, side_ref, first_ref, mark_ref, acc_in, top_in, tot_in,
    done_in, squares_in, acc_ref, top_ref, tot_ref, out_ref, squares_ref, done_ref, sems,
):
    source, state = (acc_in, top_in, tot_in), (acc_ref, top_ref, tot_ref)
    side = side_offset(spot_ref)
    early, after = range(PAIR // TILE), range(PAIR // TILE, TILES)
    squares_ref[...] = squares_in[...]

    def if_done(tile, act):
        pl.when(jnp.logical_not(late_from(spot_ref, hop_ref, doc_ref, tile * TILE)))(act)

    def moved(tile, act):
        copy = out_copy(done_in if tile in early else done_ref, out_ref, sems, tile)
        if_done(tile, getattr(copy, act))

    for tile in early:
        moved(tile, "start")

        @pl.when(late_from(spot_ref, hop_ref, doc_ref, tile * TILE))
        def _():
            copy_tile(source, state, tile_rows(tile), tile_rows(tile))

    rows = pair_rows(1)
    needed = reaches(spot_ref, hop_ref, doc_ref, PAIR, side)

    @pl.when(needed)
    def _():
        attend_earlier(q_ref, side_ref, first_ref, same(rows), TILE, side, source, state)

    @pl.when(jnp.logical_not(needed))
    def _():
        for part in rows:
            copy_tile(source, state, part, part)

    for tile in after:

        def act():
            part = tile_rows(tile)
            finish(state, part, TILE, mark_ref, done_ref, squares_ref, part)

        if_done(tile, act)
    for tile in after:
        moved(tile, "start")
    for tile in range(TILES):
        moved(tile, "wait")


def late_from(spot_ref, hop_ref, doc_ref, row):
    offset = jnp.where(spot_ref[1] == 1, -4 * ROWS, -3 * ROWS)
    return reaches(spot_ref, hop_ref, doc_ref, row, offset)


def last_kernel(
    spot_ref, hop_ref, doc_ref, q_ref, odd_ref, even_ref, side_ref, first_ref, mark_ref, acc_in,
    top_in, tot_in, squares_in, out_in, out_ref, share_ref, acc_ref, top_ref, tot_ref, squares_ref,
    done_ref, sems,
):
    source, state = (acc_in, top_in, tot_in), (acc_ref, top_ref, tot_ref)
    slots = (
        (odd_ref, on_core(spot_ref, 1, 4)),
        (side_ref, on_core(spot_ref, 0, 3)),
        (even_ref, on_core(spot_ref, 0, 4)),
    )
    late = functools.partial(late_from, spot_ref, hop_ref, doc_ref)
    squares_ref[...] = squares_in[...]

    def absorb(places, size, row):
        here = slice(0, size)
        copy_tile(source, state, places, here)
        for block_ref, offset in slots:

            @pl.when(reaches(spot_ref, hop_ref, doc_ref, row, offset))
            def _():
                attend_earlier(
                    q_ref, block_ref, first_ref, [(places, here, here)], size, offset, state, state
                )

        finish(state, here, size, mark_ref, done_ref, squares_ref, places)

    def step(tile, carry):
        @pl.when(late(tile * TILE))
        def _():
            whole = late(tile * TILE + PART)

            @pl.when(whole)
            def _():
                absorb(tile_rows(tile), TILE, tile * TILE)

            @pl.when(jnp.logical_not(whole))
            def _():
                absorb(aligned(tile * TILE, PART), PART, tile * TILE)
                rest = aligned(tile * TILE + PART, PART, TILE - PART)
                finish(source, rest, TILE - PART, mark_ref, done_ref, squares_ref, rest)

        return carry

    lax.fori_loop(0, TILES, step, 0)
    squares = jnp.sum(squares_ref[...])
    count = jnp.sum(jnp.sum(mark_ref[...].reshape(ROWS // 8, 8, 128), axis=0)) * (1.0 / 128)
    lane = lax.broadcasted_iota(jnp.int32, share_ref.shape, 1)
    share_ref[...] = jnp.where(lane == 0, squares, jnp.where(lane == 1, count, 0.0))
    for ended in (False, True):
        for tile in range(TILES):

            @pl.when(late(tile * TILE))
            def _():
                copy = out_copy(done_ref, out_ref, sems, tile)
                copy.wait() if ended else copy.start()


def call(
    kernel, scalars, arrays, out_shapes, flops, scratch=(), in_hbm=0, out_hbm=None, alias=None
):
    smem, vmem, hbm = [
        pl.BlockSpec(memory_space=space) for space in (pltpu.SMEM, pltpu.VMEM, pltpu.HBM)
    ]
    return pl.pallas_call(
        kernel,
        out_shape=out_shapes,
        in_specs=[smem] * len(scalars) + [vmem] * (len(arrays) - in_hbm) + [hbm] * in_hbm,
        out_specs=[hbm if i == out_hbm else vmem for i in range(len(out_shapes))],
        scratch_shapes=list(scratch),
        input_output_aliases=alias or {},
        compiler_params=pltpu.CompilerParams(vmem_limit_bytes=8 * 1024 * 1024),
        cost_estimate=pl.CostEstimate(flops=flops, bytes_accessed=2**20, transcendentals=2**21),
    )(*scalars, *arrays)


def packed(keys, values):
    pads = ((0, 0), (0, 0))
    return jnp.pad(keys[None], ((0, 1), *pads)) + jnp.pad(values[None], ((1, 0), *pads))


def objective_kernel(copies, shares_ref, out_ref):
    sums = jnp.sum(shares_ref[...], axis=0, keepdims=True)
    lane = lax.broadcasted_iota(jnp.int32, sums.shape, 1)
    squares = jnp.sum(jnp.where(lane == 0, sums, 0.0))
    count = jnp.sum(jnp.where(lane == 1, sums, 0.0)) * (1.0 / copies)
    out_ref[0] = squares / (QUERY_HEADS * count)


def objective_of(shares, copies):
    return pl.pallas_call(
        functools.partial(objective_kernel, copies),
        out_shape=f32(1),
        in_specs=[pl.BlockSpec(memory_space=pltpu.VMEM)],
        out_specs=pl.BlockSpec(memory_space=pltpu.SMEM),
        compiler_params=pltpu.CompilerParams(vmem_limit_bytes=4 * 1024 * 1024),
    )(shares).reshape(())


def onward(shard, cores):
    blocks = range(lax.axis_size(SEQ) - 2)
    return lax.ppermute(shard, SEQ, [(i, i + 2) for i in blocks if i % 2 in cores])


def across(shard, pairs):
    return lax.ppermute(shard, "seq_2", pairs)


def f32(*shape):
    return jax.ShapeDtypeStruct(shape, jnp.float32)


def on_device(queries, keys, values, doc_start, hop_counts, loss_mask):
    spot = jnp.stack([lax.axis_index(SEQ) * ROWS, lax.axis_index("seq_2")])
    scalars = [spot, hop_counts, doc_start]
    own = packed(keys, values)
    odd_2 = onward(own, (1,))
    side_1 = across(own, [(0, 1)])
    even_2 = onward(own, (0,))
    state_shapes = [f32(ROWS, HEADS * HEAD_WIDTH), f32(HEADS, ROWS, 128), f32(HEADS, ROWS, 128)]
    *state, first, mark = call(
        first_kernel,
        scalars,
        [doc_start.reshape(TILES, TILE), loss_mask.reshape(TILES, TILE), queries, own],
        state_shapes + [f32(ROWS, 128)] * 2,
        2 * 10**9,
    )
    odd_4 = onward(odd_2, (1,))
    state = call(near_kernel, scalars, [queries, side_1, first, *state], state_shapes, 10**9)
    even_4 = onward(even_2, (0,))
    far_2 = odd_2 + even_2
    side_2 = across(far_2, [(0, 1), (1, 0)])
    out_shape = jax.ShapeDtypeStruct((ROWS, HEADS * HEAD_WIDTH), jnp.bfloat16)
    copy_scratch = [pltpu.VMEM(out_shape.shape, jnp.bfloat16), pltpu.SemaphoreType.DMA((TILES,))]
    *state, done, squares = call(
        far_kernel,
        scalars,
        [queries, far_2, side_2, first, mark, *state],
        state_shapes + [out_shape, f32(8, 128)],
        2 * 10**9,
    )
    side_3 = across(odd_4, [(1, 0)])
    *state, done, squares = call(
        side_kernel,
        scalars,
        [queries, side_2, first, mark, *state, done, squares],
        state_shapes + [out_shape, f32(8, 128)],
        10**9,
        scratch=copy_scratch,
        out_hbm=3,
    )
    devices = lax.axis_size(SEQ_HEAD)
    arrays = [queries, odd_4, even_4, side_3, first, mark, *state, squares, done]
    attention, share = call(
        last_kernel,
        scalars,
        arrays,
        [out_shape, f32(devices, 128)],
        10**9,
        scratch=[
            pltpu.VMEM((TILE, HEADS * HEAD_WIDTH), jnp.float32),
            pltpu.VMEM((HEADS, TILE, 128), jnp.float32),
            pltpu.VMEM((HEADS, TILE, 128), jnp.float32),
            pltpu.VMEM((8, 128), jnp.float32),
            *copy_scratch,
        ],
        in_hbm=1,
        out_hbm=0,
        alias={len(scalars) + len(arrays) - 1: 0},
    )
    shares = lax.all_to_all(share, SEQ_HEAD, 0, 0, tiled=True)
    return (attention, objective_of(shares, lax.axis_size("head")))


def solution(mesh):
    torus = Mesh(
        mesh.devices.reshape(4, 8, 2, mesh.shape["head"]), ("seq_0", "seq_1", "seq_2", "head")
    )
    placed = (P(SEQ, "head"), P(SEQ, "head"), P(SEQ, "head"), P(SEQ), P(SEQ), P(SEQ))

    return jax.shard_map(
        on_device, mesh=torus, in_specs=placed, out_specs=(P(SEQ, "head"), P()), check_vma=False
    )
```

```python
import functools
import math

import jax
import jax.numpy as jnp
from jax import lax
from jax.experimental import pallas as pl
from jax.experimental.pallas import tpu as pltpu
from jax.sharding import Mesh
from jax.sharding import PartitionSpec as P

QUERY_HEADS = 32
KEY_VALUE_HEADS = 8
HEAD_WIDTH = 128
GROUP = QUERY_HEADS // KEY_VALUE_HEADS
SEQ = ("seq_0", "seq_1", "seq_2")
SEQ_HEAD = ("seq_0", "seq_1", "seq_2", "head")
ROWS = 512
TILE = 128
TILES = ROWS // TILE
PART = 32
PAIR = 2 * TILE
LOCAL_KV = 2
HEADS = LOCAL_KV * GROUP
LOWEST = -1e30
EXP2_SCALE = math.log2(math.e) / math.sqrt(HEAD_WIDTH)
NOWHERE = ROWS


def aligned(start, by, size=None):
    return pl.ds(start if isinstance(start, int) else pl.multiple_of(start, by), size or by)


def tile_rows(tile):
    return aligned(tile * TILE, TILE)


def columns(head):
    return slice(head * HEAD_WIDTH, (head + 1) * HEAD_WIDTH)


def dot(a, b, contract_b):
    return lax.dot_general(
        a, b, (((1,), (contract_b,)), ((), ())), preferred_element_type=jnp.float32
    )


def heads_of(kv):
    return range(kv * GROUP, (kv + 1) * GROUP)


def lane_groups(x):
    return [x[:, i : i + 128] for i in range(0, x.shape[1], 128)]


def folded(op, parts):
    while len(parts) > 1:
        parts = [op(*parts[i : i + 2]) if i + 1 < len(parts) else parts[i] for i in range(0, len(parts), 2)]
    return parts[0]


def widened(x, width):
    return jnp.concatenate([x] * (width // 128), axis=1)


def attend(q_ref, block_ref, parts, size):
    steps = [(part, kv) for part in parts for kv in range(LOCAL_KV)]

    def score(step):
        (rows, width, *_), kv = step
        q = jnp.concatenate([q_ref[rows, columns(h)] for h in heads_of(kv)], axis=0)
        return dot(q, block_ref[0, 0:width, columns(kv)], 1)

    def weigh(step, scores):
        (_, width, seen, old, _), kv = step
        rounded, states = [], []
        for g, head in enumerate(heads_of(kv)):
            part = jnp.where(seen, scores[g * size : (g + 1) * size], LOWEST)
            top = jnp.max(folded(jnp.maximum, lane_groups(part)), axis=1, keepdims=True)
            top = jnp.broadcast_to(top, (size, 128))
            before = old(head)
            ratio = None
            if before is not None:
                top = jnp.maximum(before[0], top)
                ratio = jnp.exp2((before[0] - top) * EXP2_SCALE)
            weights = jnp.exp2((part - widened(top, width)) * EXP2_SCALE)
            states.append((top, ratio))
            rounded.append(weights.astype(jnp.bfloat16))
        return jnp.concatenate(rounded, axis=0), states

    def add(step, rounded, states):
        (_, width, _, old, new), kv = step
        v = block_ref[1, 0:width, columns(kv)]
        update = dot(rounded, jnp.concatenate([v, jnp.ones_like(v)], axis=1), 0)
        for g, head in enumerate(heads_of(kv)):
            top, ratio = states[g]
            part = update[g * size : (g + 1) * size]
            sums, total = part[:, 0:HEAD_WIDTH], part[:, HEAD_WIDTH:]
            if ratio is not None:
                _, total_old, sums_old = old(head)
                sums, total = sums_old() * ratio + sums, total_old * ratio + total
            new(head, top, total, sums)

    scores, pending = score(steps[0]), None
    for at, step in enumerate(steps):
        ahead = score(steps[at + 1]) if at + 1 < len(steps) else None
        weighed = weigh(step, scores)
        if pending is not None:
            add(*pending)
        scores, pending = ahead, (step, *weighed)
    add(*pending)


def reader(state, rows):
    acc_ref, top_ref, tot_ref = state
    return lambda head: (
        top_ref[head, rows, :],
        tot_ref[head, rows, :],
        lambda: acc_ref[rows, columns(head)],
    )


def writer(state, rows):
    acc_ref, top_ref, tot_ref = state

    def store(head, top, total, sums):
        top_ref[head, rows, :] = top
        tot_ref[head, rows, :] = total
        acc_ref[rows, columns(head)] = sums

    return store


def attend_earlier(q_ref, block_ref, first_ref, places, size, offset, source, state):
    parts = []
    for rows, rows_in, rows_out in places:
        place = (lax.broadcasted_iota(jnp.int32, (size, ROWS), 1) + offset).astype(jnp.float32)
        seen = place >= widened(first_ref[rows, :], ROWS)
        parts.append((rows, ROWS, seen, reader(source, rows_in), writer(state, rows_out)))
    attend(q_ref, block_ref, parts, size)


def pair_rows(pair):
    return [aligned(pair * PAIR + i, TILE) for i in range(0, PAIR, TILE)]


def same(rows):
    return [(r, r, r) for r in rows]


def reaches(spot_ref, hop_ref, doc_ref, row, offset):
    floor = spot_ref[0] - hop_ref[0] * ROWS
    earliest = jnp.maximum(doc_ref[row], floor) - spot_ref[0]
    return (offset < 0) & (offset + ROWS > earliest)


def first_kernel(
    spot_ref, hop_ref, doc_ref, starts_ref, q_ref, own_ref,
    acc_ref, top_ref, tot_ref, first_ref,
):
    floor = spot_ref[0] - hop_ref[0] * ROWS
    state = (acc_ref, top_ref, tot_ref)
    parts = []
    for tile in range(TILES):
        width = (tile + 1) * TILE
        rows = tile_rows(tile)
        starts = jnp.maximum(starts_ref[tile : tile + 1, :], floor) - spot_ref[0]
        first = jnp.broadcast_to(starts.astype(jnp.float32), (TILE, 128)).T
        first_ref[rows, :] = first
        place = lax.broadcasted_iota(jnp.int32, (TILE, width), 1)
        row = lax.broadcasted_iota(jnp.int32, (TILE, width), 0) + tile * TILE
        seen = (place.astype(jnp.float32) >= widened(first, width)) & (place <= row)
        parts.append((rows, width, seen, lambda head: None, writer(state, rows)))
    attend(q_ref, own_ref, parts, TILE)


def copy_tile(source, target, rows, target_rows):
    for head in range(HEADS):
        top, total, sums = reader(source, rows)(head)
        writer(target, target_rows)(head, top, total, sums())


def finish(state, rows, size, mark_ref, out_ref, squares_ref, places):
    squares = jnp.zeros((size, HEAD_WIDTH), jnp.float32)
    for head in range(HEADS):
        _, total, sums = reader(state, rows)(head)
        attended = sums() * (1.0 / total)
        out_ref[places, columns(head)] = attended.astype(jnp.bfloat16)
        squares += attended * attended
    squares *= mark_ref[places, :]
    squares_ref[...] += jnp.sum(squares.reshape(size // 8, 8, HEAD_WIDTH), axis=0)


def out_copy(from_ref, out_ref, sems, tile):
    rows = tile_rows(tile)
    return pltpu.make_async_copy(from_ref.at[rows, :], out_ref.at[rows, :], sems.at[tile])


def one_block(spot_ref, hop_ref, doc_ref, q_ref, block_ref, first_ref, source, state, offset):
    def step(pair, carry):
        rows = pair_rows(pair)
        needed = reaches(spot_ref, hop_ref, doc_ref, pair * PAIR, offset)

        @pl.when(needed)
        def _():
            attend_earlier(q_ref, block_ref, first_ref, same(rows), TILE, offset, source, state)

        @pl.when(jnp.logical_not(needed))
        def _():
            for part in rows:
                copy_tile(source, state, part, part)

        return carry

    lax.fori_loop(0, ROWS // PAIR, step, 0)


def near_kernel(
    spot_ref, hop_ref, doc_ref, q_ref, near_ref, first_ref, acc_in, top_in, tot_in,
    acc_ref, top_ref, tot_ref,
):
    source, state = (acc_in, top_in, tot_in), (acc_ref, top_ref, tot_ref)
    offset = on_core(spot_ref, 1, 1)
    one_block(spot_ref, hop_ref, doc_ref, q_ref, near_ref, first_ref, source, state, offset)


def on_core(spot_ref, core, distance):
    return jnp.where(spot_ref[1] == core, -distance * ROWS, NOWHERE)


def side_offset(spot_ref):
    return jnp.where(spot_ref[1] == 1, -3 * ROWS, -ROWS)


def far_kernel(
    spot_ref, hop_ref, doc_ref, q_ref, far_ref, first_ref, marks_ref, acc_in, top_in, tot_in,
    acc_ref, top_ref, tot_ref, mark_ref,
):
    source, state = (acc_in, top_in, tot_in), (acc_ref, top_ref, tot_ref)
    for tile in range(TILES):
        marks = marks_ref[tile : tile + 1, :].astype(jnp.float32)
        mark_ref[tile_rows(tile), :] = jnp.broadcast_to(marks, (TILE, 128)).T
    one_block(spot_ref, hop_ref, doc_ref, q_ref, far_ref, first_ref, source, state, -2 * ROWS)


def side_kernel(
    spot_ref, hop_ref, doc_ref, q_ref, side_ref, first_ref, mark_ref, acc_in, top_in, tot_in,
    acc_ref, top_ref, tot_ref, out_ref, squares_ref, done_ref, sems,
):
    source, state = (acc_in, top_in, tot_in), (acc_ref, top_ref, tot_ref)
    offset = side_offset(spot_ref)
    squares_ref[...] = jnp.zeros_like(squares_ref)

    def if_done(tile, act):
        pl.when(jnp.logical_not(late_from(spot_ref, hop_ref, doc_ref, tile * TILE)))(act)

    def moved(tile, act):
        if_done(tile, getattr(out_copy(done_ref, out_ref, sems, tile), act))

    per_pair = PAIR // TILE
    for pair in range(ROWS // PAIR):
        rows = pair_rows(pair)
        needed = reaches(spot_ref, hop_ref, doc_ref, pair * PAIR, offset)

        @pl.when(needed)
        def _():
            attend_earlier(q_ref, side_ref, first_ref, same(rows), TILE, offset, source, state)

        @pl.when(jnp.logical_not(needed))
        def _():
            for part in rows:
                copy_tile(source, state, part, part)

        for i, part in enumerate(rows):

            def act():
                finish(state, part, TILE, mark_ref, done_ref, squares_ref, part)

            if_done(pair * per_pair + i, act)
        if pair:
            for i in range(per_pair):
                moved((pair - 1) * per_pair + i, "start")
    for tile in range(TILES - per_pair, TILES):
        moved(tile, "start")
    for tile in range(TILES):
        moved(tile, "wait")


def late_from(spot_ref, hop_ref, doc_ref, row):
    offset = jnp.where(spot_ref[1] == 1, -4 * ROWS, -3 * ROWS)
    return reaches(spot_ref, hop_ref, doc_ref, row, offset)


def last_kernel(
    spot_ref, hop_ref, doc_ref, q_ref, odd_ref, even_ref, side_ref, first_ref, mark_ref, acc_in,
    top_in, tot_in, squares_in, out_in, out_ref, share_ref, acc_ref, top_ref, tot_ref, squares_ref,
    done_ref, sems,
):
    source, state = (acc_in, top_in, tot_in), (acc_ref, top_ref, tot_ref)
    slots = (
        (odd_ref, on_core(spot_ref, 1, 4)),
        (side_ref, on_core(spot_ref, 0, 3)),
        (even_ref, on_core(spot_ref, 0, 4)),
    )
    late = functools.partial(late_from, spot_ref, hop_ref, doc_ref)
    squares_ref[...] = squares_in[...]

    def absorb(places, size, row):
        here = slice(0, size)
        copy_tile(source, state, places, here)
        for block_ref, offset in slots:

            @pl.when(reaches(spot_ref, hop_ref, doc_ref, row, offset))
            def _():
                attend_earlier(
                    q_ref, block_ref, first_ref, [(places, here, here)], size, offset, state, state
                )

        finish(state, here, size, mark_ref, done_ref, squares_ref, places)

    def step(tile, carry):
        @pl.when(late(tile * TILE))
        def _():
            whole = late(tile * TILE + PART)

            @pl.when(whole)
            def _():
                absorb(tile_rows(tile), TILE, tile * TILE)

            @pl.when(jnp.logical_not(whole))
            def _():
                absorb(aligned(tile * TILE, PART), PART, tile * TILE)
                rest = aligned(tile * TILE + PART, PART, TILE - PART)
                finish(source, rest, TILE - PART, mark_ref, done_ref, squares_ref, rest)

        return carry

    lax.fori_loop(0, TILES, step, 0)
    squares = jnp.sum(squares_ref[...])
    count = jnp.sum(jnp.sum(mark_ref[...].reshape(ROWS // 8, 8, 128), axis=0)) * (1.0 / 128)
    lane = lax.broadcasted_iota(jnp.int32, share_ref.shape, 1)
    share_ref[...] = jnp.where(lane == 0, squares, jnp.where(lane == 1, count, 0.0))
    for ended in (False, True):
        for tile in range(TILES):

            @pl.when(late(tile * TILE))
            def _():
                copy = out_copy(done_ref, out_ref, sems, tile)
                copy.wait() if ended else copy.start()


def call(
    kernel, scalars, arrays, out_shapes, flops, scratch=(), in_hbm=0, out_hbm=None, alias=None
):
    smem, vmem, hbm = [
        pl.BlockSpec(memory_space=space) for space in (pltpu.SMEM, pltpu.VMEM, pltpu.HBM)
    ]
    return pl.pallas_call(
        kernel,
        out_shape=out_shapes,
        in_specs=[smem] * len(scalars) + [vmem] * (len(arrays) - in_hbm) + [hbm] * in_hbm,
        out_specs=[hbm if i == out_hbm else vmem for i in range(len(out_shapes))],
        scratch_shapes=list(scratch),
        input_output_aliases=alias or {},
        compiler_params=pltpu.CompilerParams(vmem_limit_bytes=8 * 1024 * 1024),
        cost_estimate=pl.CostEstimate(flops=flops, bytes_accessed=2**20, transcendentals=2**21),
    )(*scalars, *arrays)


def packed(keys, values):
    pads = ((0, 0), (0, 0))
    return jnp.pad(keys[None], ((0, 1), *pads)) + jnp.pad(values[None], ((1, 0), *pads))


def objective_kernel(copies, shares_ref, out_ref):
    sums = jnp.sum(shares_ref[...], axis=0, keepdims=True)
    lane = lax.broadcasted_iota(jnp.int32, sums.shape, 1)
    squares = jnp.sum(jnp.where(lane == 0, sums, 0.0))
    count = jnp.sum(jnp.where(lane == 1, sums, 0.0)) * (1.0 / copies)
    out_ref[0] = squares / (QUERY_HEADS * count)


def objective_of(shares, copies):
    return pl.pallas_call(
        functools.partial(objective_kernel, copies),
        out_shape=f32(1),
        in_specs=[pl.BlockSpec(memory_space=pltpu.VMEM)],
        out_specs=pl.BlockSpec(memory_space=pltpu.SMEM),
        compiler_params=pltpu.CompilerParams(vmem_limit_bytes=4 * 1024 * 1024),
    )(shares).reshape(())


def onward(shard, cores):
    blocks = range(lax.axis_size(SEQ) - 2)
    return lax.ppermute(shard, SEQ, [(i, i + 2) for i in blocks if i % 2 in cores])


def across(shard, pairs):
    return lax.ppermute(shard, "seq_2", pairs)


def f32(*shape):
    return jax.ShapeDtypeStruct(shape, jnp.float32)


def on_device(queries, keys, values, doc_start, hop_counts, loss_mask):
    spot = jnp.stack([lax.axis_index(SEQ) * ROWS, lax.axis_index("seq_2")])
    scalars = [spot, hop_counts, doc_start]
    own = packed(keys, values)
    odd_2 = onward(own, (1,))
    side_1 = across(own, [(0, 1)])
    even_2 = onward(own, (0,))
    state_shapes = [f32(ROWS, HEADS * HEAD_WIDTH), f32(HEADS, ROWS, 128), f32(HEADS, ROWS, 128)]
    *state, first = call(
        first_kernel,
        scalars,
        [doc_start.reshape(TILES, TILE), queries, own],
        state_shapes + [f32(ROWS, 128)],
        2 * 10**9,
    )
    odd_4 = onward(odd_2, (1,))
    state = call(near_kernel, scalars, [queries, side_1, first, *state], state_shapes, 10**9)
    even_4 = onward(even_2, (0,))
    far_2 = odd_2 + even_2
    side_2 = across(far_2, [(0, 1), (1, 0)])
    out_shape = jax.ShapeDtypeStruct((ROWS, HEADS * HEAD_WIDTH), jnp.bfloat16)
    copy_scratch = [pltpu.VMEM(out_shape.shape, jnp.bfloat16), pltpu.SemaphoreType.DMA((TILES,))]
    *state, mark = call(
        far_kernel,
        scalars,
        [queries, far_2, first, loss_mask.reshape(TILES, TILE), *state],
        state_shapes + [f32(ROWS, 128)],
        10**9,
    )
    side_3 = across(odd_4, [(1, 0)])
    *state, done, squares = call(
        side_kernel,
        scalars,
        [queries, side_2, first, mark, *state],
        state_shapes + [out_shape, f32(8, 128)],
        10**9,
        scratch=copy_scratch,
        out_hbm=3,
    )
    devices = lax.axis_size(SEQ_HEAD)
    arrays = [queries, odd_4, even_4, side_3, first, mark, *state, squares, done]
    attention, share = call(
        last_kernel,
        scalars,
        arrays,
        [out_shape, f32(devices, 128)],
        10**9,
        scratch=[
            pltpu.VMEM((TILE, HEADS * HEAD_WIDTH), jnp.float32),
            pltpu.VMEM((HEADS, TILE, 128), jnp.float32),
            pltpu.VMEM((HEADS, TILE, 128), jnp.float32),
            pltpu.VMEM((8, 128), jnp.float32),
            *copy_scratch,
        ],
        in_hbm=1,
        out_hbm=0,
        alias={len(scalars) + len(arrays) - 1: 0},
    )
    shares = lax.all_to_all(share, SEQ_HEAD, 0, 0, tiled=True)
    return (attention, objective_of(shares, lax.axis_size("head")))


def solution(mesh):
    torus = Mesh(
        mesh.devices.reshape(4, 8, 2, mesh.shape["head"]), ("seq_0", "seq_1", "seq_2", "head")
    )
    placed = (P(SEQ, "head"), P(SEQ, "head"), P(SEQ, "head"), P(SEQ), P(SEQ), P(SEQ))

    return jax.shard_map(
        on_device, mesh=torus, in_specs=placed, out_specs=(P(SEQ, "head"), P()), check_vma=False
    )
```

```python
import functools
import math

import jax
import jax.numpy as jnp
from jax import lax
from jax.experimental import pallas as pl
from jax.experimental.pallas import tpu as pltpu
from jax.sharding import Mesh
from jax.sharding import PartitionSpec as P

QUERY_HEADS = 32
KEY_VALUE_HEADS = 8
HEAD_WIDTH = 128
GROUP = QUERY_HEADS // KEY_VALUE_HEADS
SEQ = ("seq_0", "seq_1", "seq_2")
SEQ_HEAD = ("seq_0", "seq_1", "seq_2", "head")
ROWS = 512
TILE = 128
TILES = ROWS // TILE
PART = 32
PAIR = 2 * TILE
LOCAL_KV = 2
HEADS = LOCAL_KV * GROUP
LOWEST = -1e30
EXP2_SCALE = math.log2(math.e) / math.sqrt(HEAD_WIDTH)
NOWHERE = ROWS


def aligned(start, by, size=None):
    return pl.ds(start if isinstance(start, int) else pl.multiple_of(start, by), size or by)


def tile_rows(tile):
    return aligned(tile * TILE, TILE)


def columns(head):
    return slice(head * HEAD_WIDTH, (head + 1) * HEAD_WIDTH)


def dot(a, b, contract_b):
    return lax.dot_general(
        a, b, (((1,), (contract_b,)), ((), ())), preferred_element_type=jnp.float32
    )


def heads_of(kv):
    return range(kv * GROUP, (kv + 1) * GROUP)


def lane_groups(x):
    return [x[:, i : i + 128] for i in range(0, x.shape[1], 128)]


def folded(op, parts):
    while len(parts) > 1:
        parts = [op(*parts[i : i + 2]) if i + 1 < len(parts) else parts[i] for i in range(0, len(parts), 2)]
    return parts[0]


def widened(x, width):
    return jnp.concatenate([x] * (width // 128), axis=1)


def attend(q_ref, block_ref, parts, size):
    steps = [(part, kv) for part in parts for kv in range(LOCAL_KV)]

    def score(step):
        (rows, width, *_), kv = step
        q = jnp.concatenate([q_ref[rows, columns(h)] for h in heads_of(kv)], axis=0)
        return dot(q, block_ref[0, 0:width, columns(kv)], 1)

    def weigh(step, scores):
        (_, width, seen, old, _), kv = step
        rounded, states = [], []
        for g, head in enumerate(heads_of(kv)):
            part = jnp.where(seen, scores[g * size : (g + 1) * size], LOWEST)
            top = jnp.max(folded(jnp.maximum, lane_groups(part)), axis=1, keepdims=True)
            top = jnp.broadcast_to(top, (size, 128))
            before = old(head)
            ratio = None
            if before is not None:
                top = jnp.maximum(before[0], top)
                ratio = jnp.exp2((before[0] - top) * EXP2_SCALE)
            weights = jnp.exp2((part - widened(top, width)) * EXP2_SCALE)
            states.append((top, ratio))
            rounded.append(weights.astype(jnp.bfloat16))
        return jnp.concatenate(rounded, axis=0), states

    def add(step, rounded, states):
        (_, width, _, old, new), kv = step
        v = block_ref[1, 0:width, columns(kv)]
        update = dot(rounded, jnp.concatenate([v, jnp.ones_like(v)], axis=1), 0)
        for g, head in enumerate(heads_of(kv)):
            top, ratio = states[g]
            part = update[g * size : (g + 1) * size]
            sums, total = part[:, 0:HEAD_WIDTH], part[:, HEAD_WIDTH:]
            if ratio is not None:
                _, total_old, sums_old = old(head)
                sums, total = sums_old() * ratio + sums, total_old * ratio + total
            new(head, top, total, sums)

    scores, pending = score(steps[0]), None
    for at, step in enumerate(steps):
        ahead = score(steps[at + 1]) if at + 1 < len(steps) else None
        weighed = weigh(step, scores)
        if pending is not None:
            add(*pending)
        scores, pending = ahead, (step, *weighed)
    add(*pending)


def reader(state, rows):
    acc_ref, top_ref, tot_ref = state
    return lambda head: (
        top_ref[head, rows, :],
        tot_ref[head, rows, :],
        lambda: acc_ref[rows, columns(head)],
    )


def writer(state, rows):
    acc_ref, top_ref, tot_ref = state

    def store(head, top, total, sums):
        top_ref[head, rows, :] = top
        tot_ref[head, rows, :] = total
        acc_ref[rows, columns(head)] = sums

    return store


def attend_earlier(q_ref, block_ref, first_ref, places, size, offset, source, state):
    parts = []
    for rows, rows_in, rows_out in places:
        place = (lax.broadcasted_iota(jnp.int32, (size, ROWS), 1) + offset).astype(jnp.float32)
        seen = place >= widened(first_ref[rows, :], ROWS)
        parts.append((rows, ROWS, seen, reader(source, rows_in), writer(state, rows_out)))
    attend(q_ref, block_ref, parts, size)


def pair_rows(pair):
    return [aligned(pair * PAIR + i, TILE) for i in range(0, PAIR, TILE)]


def same(rows):
    return [(r, r, r) for r in rows]


def reaches(spot_ref, hop_ref, doc_ref, row, offset):
    floor = spot_ref[0] - hop_ref[0] * ROWS
    earliest = jnp.maximum(doc_ref[row], floor) - spot_ref[0]
    return (offset < 0) & (offset + ROWS > earliest)


def first_kernel(
    spot_ref, hop_ref, doc_ref, starts_ref, q_ref, own_ref,
    acc_ref, top_ref, tot_ref, first_ref,
):
    floor = spot_ref[0] - hop_ref[0] * ROWS
    state = (acc_ref, top_ref, tot_ref)
    parts = []
    for tile in range(TILES):
        width = (tile + 1) * TILE
        rows = tile_rows(tile)
        starts = jnp.maximum(starts_ref[tile : tile + 1, :], floor) - spot_ref[0]
        first = jnp.broadcast_to(starts.astype(jnp.float32), (TILE, 128)).T
        first_ref[rows, :] = first
        place = lax.broadcasted_iota(jnp.int32, (TILE, width), 1)
        row = lax.broadcasted_iota(jnp.int32, (TILE, width), 0) + tile * TILE
        seen = (place.astype(jnp.float32) >= widened(first, width)) & (place <= row)
        parts.append((rows, width, seen, lambda head: None, writer(state, rows)))
    attend(q_ref, own_ref, parts, TILE)


def copy_tile(source, target, rows, target_rows):
    for head in range(HEADS):
        top, total, sums = reader(source, rows)(head)
        writer(target, target_rows)(head, top, total, sums())


def finish(state, rows, size, mark_ref, out_ref, squares_ref, places):
    squares = jnp.zeros((size, HEAD_WIDTH), jnp.float32)
    for head in range(HEADS):
        _, total, sums = reader(state, rows)(head)
        attended = sums() * (1.0 / total)
        out_ref[places, columns(head)] = attended.astype(jnp.bfloat16)
        squares += attended * attended
    squares *= mark_ref[places, :]
    squares_ref[...] += jnp.sum(squares.reshape(size // 8, 8, HEAD_WIDTH), axis=0)


def out_copy(from_ref, out_ref, sems, tile):
    rows = tile_rows(tile)
    return pltpu.make_async_copy(from_ref.at[rows, :], out_ref.at[rows, :], sems.at[tile])


def one_block(spot_ref, hop_ref, doc_ref, q_ref, block_ref, first_ref, source, state, offset):
    def step(pair, carry):
        rows = pair_rows(pair)
        needed = reaches(spot_ref, hop_ref, doc_ref, pair * PAIR, offset)

        @pl.when(needed)
        def _():
            attend_earlier(q_ref, block_ref, first_ref, same(rows), TILE, offset, source, state)

        @pl.when(jnp.logical_not(needed))
        def _():
            for part in rows:
                copy_tile(source, state, part, part)

        return carry

    lax.fori_loop(0, ROWS // PAIR, step, 0)


def near_kernel(
    spot_ref, hop_ref, doc_ref, q_ref, near_ref, first_ref, acc_in, top_in, tot_in,
    acc_ref, top_ref, tot_ref,
):
    source, state = (acc_in, top_in, tot_in), (acc_ref, top_ref, tot_ref)
    offset = on_core(spot_ref, 1, 1)
    one_block(spot_ref, hop_ref, doc_ref, q_ref, near_ref, first_ref, source, state, offset)


def on_core(spot_ref, core, distance):
    return jnp.where(spot_ref[1] == core, -distance * ROWS, NOWHERE)


def side_offset(spot_ref):
    return jnp.where(spot_ref[1] == 1, -3 * ROWS, -ROWS)


def far_kernel(
    spot_ref, hop_ref, doc_ref, q_ref, far_ref, first_ref, marks_ref, acc_in, top_in, tot_in,
    acc_ref, top_ref, tot_ref, mark_ref,
):
    source, state = (acc_in, top_in, tot_in), (acc_ref, top_ref, tot_ref)
    for tile in range(TILES):
        marks = marks_ref[tile : tile + 1, :].astype(jnp.float32)
        mark_ref[tile_rows(tile), :] = jnp.broadcast_to(marks, (TILE, 128)).T
    one_block(spot_ref, hop_ref, doc_ref, q_ref, far_ref, first_ref, source, state, -2 * ROWS)


def side_kernel(
    spot_ref, hop_ref, doc_ref, q_ref, side_ref, first_ref, mark_ref, acc_in, top_in, tot_in,
    acc_ref, top_ref, tot_ref, out_ref, squares_ref, done_ref, sems,
):
    source, state = (acc_in, top_in, tot_in), (acc_ref, top_ref, tot_ref)
    offset = side_offset(spot_ref)
    squares_ref[...] = jnp.zeros_like(squares_ref)

    def if_done(tile, act):
        pl.when(jnp.logical_not(late_from(spot_ref, hop_ref, doc_ref, tile * TILE)))(act)

    def moved(tile, act):
        if_done(tile, getattr(out_copy(done_ref, out_ref, sems, tile), act))

    per_pair = PAIR // TILE
    for pair in range(ROWS // PAIR):
        rows = pair_rows(pair)
        needed = reaches(spot_ref, hop_ref, doc_ref, pair * PAIR, offset)

        @pl.when(needed)
        def _():
            attend_earlier(q_ref, side_ref, first_ref, same(rows), TILE, offset, source, state)

        @pl.when(jnp.logical_not(needed))
        def _():
            for part in rows:
                copy_tile(source, state, part, part)

        for i, part in enumerate(rows):

            def act():
                finish(state, part, TILE, mark_ref, done_ref, squares_ref, part)

            if_done(pair * per_pair + i, act)
        if pair:
            for i in range(per_pair):
                moved((pair - 1) * per_pair + i, "start")
    for tile in range(per_pair):
        moved(tile, "wait")


def late_from(spot_ref, hop_ref, doc_ref, row):
    offset = jnp.where(spot_ref[1] == 1, -4 * ROWS, -3 * ROWS)
    return reaches(spot_ref, hop_ref, doc_ref, row, offset)


def last_kernel(
    spot_ref, hop_ref, doc_ref, q_ref, odd_ref, even_ref, side_ref, first_ref, mark_ref, acc_in,
    top_in, tot_in, squares_in, done_in, out_in, out_ref, share_ref, acc_ref, top_ref, tot_ref,
    squares_ref, done_ref, sems,
):
    source, state = (acc_in, top_in, tot_in), (acc_ref, top_ref, tot_ref)
    slots = (
        (odd_ref, on_core(spot_ref, 1, 4)),
        (side_ref, on_core(spot_ref, 0, 3)),
        (even_ref, on_core(spot_ref, 0, 4)),
    )
    late = functools.partial(late_from, spot_ref, hop_ref, doc_ref)

    def moved(tile, act):
        copy = out_copy(done_in, out_ref, sems, tile)
        pl.when(jnp.logical_not(late(tile * TILE)))(getattr(copy, act))

    for tile in range(PAIR // TILE, TILES):
        moved(tile, "start")
    squares_ref[...] = squares_in[...]

    def absorb(places, size, row):
        here = slice(0, size)
        copy_tile(source, state, places, here)
        for block_ref, offset in slots:

            @pl.when(reaches(spot_ref, hop_ref, doc_ref, row, offset))
            def _():
                attend_earlier(
                    q_ref, block_ref, first_ref, [(places, here, here)], size, offset, state, state
                )

        finish(state, here, size, mark_ref, done_ref, squares_ref, places)

    def step(tile, carry):
        @pl.when(late(tile * TILE))
        def _():
            whole = late(tile * TILE + PART)

            @pl.when(whole)
            def _():
                absorb(tile_rows(tile), TILE, tile * TILE)

            @pl.when(jnp.logical_not(whole))
            def _():
                absorb(aligned(tile * TILE, PART), PART, tile * TILE)
                rest = aligned(tile * TILE + PART, PART, TILE - PART)
                finish(source, rest, TILE - PART, mark_ref, done_ref, squares_ref, rest)

        return carry

    lax.fori_loop(0, TILES, step, 0)
    squares = jnp.sum(squares_ref[...])
    count = jnp.sum(jnp.sum(mark_ref[...].reshape(ROWS // 8, 8, 128), axis=0)) * (1.0 / 128)
    lane = lax.broadcasted_iota(jnp.int32, share_ref.shape, 1)
    share_ref[...] = jnp.where(lane == 0, squares, jnp.where(lane == 1, count, 0.0))
    for ended in (False, True):
        for tile in range(TILES):

            @pl.when(late(tile * TILE))
            def _():
                copy = out_copy(done_ref, out_ref, sems, tile)
                copy.wait() if ended else copy.start()
    for tile in range(PAIR // TILE, TILES):
        moved(tile, "wait")


def call(
    kernel, scalars, arrays, out_shapes, flops, scratch=(), in_hbm=0, out_hbm=None, alias=None
):
    smem, vmem, hbm = [
        pl.BlockSpec(memory_space=space) for space in (pltpu.SMEM, pltpu.VMEM, pltpu.HBM)
    ]
    return pl.pallas_call(
        kernel,
        out_shape=out_shapes,
        in_specs=[smem] * len(scalars) + [vmem] * (len(arrays) - in_hbm) + [hbm] * in_hbm,
        out_specs=[hbm if i == out_hbm else vmem for i in range(len(out_shapes))],
        scratch_shapes=list(scratch),
        input_output_aliases=alias or {},
        compiler_params=pltpu.CompilerParams(vmem_limit_bytes=8 * 1024 * 1024),
        cost_estimate=pl.CostEstimate(flops=flops, bytes_accessed=2**20, transcendentals=2**21),
    )(*scalars, *arrays)


def packed(keys, values):
    pads = ((0, 0), (0, 0))
    return jnp.pad(keys[None], ((0, 1), *pads)) + jnp.pad(values[None], ((1, 0), *pads))


def objective_kernel(copies, shares_ref, out_ref):
    sums = jnp.sum(shares_ref[...], axis=0, keepdims=True)
    lane = lax.broadcasted_iota(jnp.int32, sums.shape, 1)
    squares = jnp.sum(jnp.where(lane == 0, sums, 0.0))
    count = jnp.sum(jnp.where(lane == 1, sums, 0.0)) * (1.0 / copies)
    out_ref[0] = squares / (QUERY_HEADS * count)


def objective_of(shares, copies):
    return pl.pallas_call(
        functools.partial(objective_kernel, copies),
        out_shape=f32(1),
        in_specs=[pl.BlockSpec(memory_space=pltpu.VMEM)],
        out_specs=pl.BlockSpec(memory_space=pltpu.SMEM),
        compiler_params=pltpu.CompilerParams(vmem_limit_bytes=4 * 1024 * 1024),
    )(shares).reshape(())


def onward(shard, cores):
    blocks = range(lax.axis_size(SEQ) - 2)
    return lax.ppermute(shard, SEQ, [(i, i + 2) for i in blocks if i % 2 in cores])


def across(shard, pairs):
    return lax.ppermute(shard, "seq_2", pairs)


def f32(*shape):
    return jax.ShapeDtypeStruct(shape, jnp.float32)


def on_device(queries, keys, values, doc_start, hop_counts, loss_mask):
    spot = jnp.stack([lax.axis_index(SEQ) * ROWS, lax.axis_index("seq_2")])
    scalars = [spot, hop_counts, doc_start]
    own = packed(keys, values)
    odd_2 = onward(own, (1,))
    side_1 = across(own, [(0, 1)])
    even_2 = onward(own, (0,))
    state_shapes = [f32(ROWS, HEADS * HEAD_WIDTH), f32(HEADS, ROWS, 128), f32(HEADS, ROWS, 128)]
    *state, first = call(
        first_kernel,
        scalars,
        [doc_start.reshape(TILES, TILE), queries, own],
        state_shapes + [f32(ROWS, 128)],
        2 * 10**9,
    )
    odd_4 = onward(odd_2, (1,))
    state = call(near_kernel, scalars, [queries, side_1, first, *state], state_shapes, 10**9)
    even_4 = onward(even_2, (0,))
    far_2 = odd_2 + even_2
    side_2 = across(far_2, [(0, 1), (1, 0)])
    out_shape = jax.ShapeDtypeStruct((ROWS, HEADS * HEAD_WIDTH), jnp.bfloat16)
    copy_scratch = [pltpu.VMEM(out_shape.shape, jnp.bfloat16), pltpu.SemaphoreType.DMA((TILES,))]
    *state, mark = call(
        far_kernel,
        scalars,
        [queries, far_2, first, loss_mask.reshape(TILES, TILE), *state],
        state_shapes + [f32(ROWS, 128)],
        10**9,
    )
    side_3 = across(odd_4, [(1, 0)])
    *state, out, squares, done = call(
        side_kernel,
        scalars,
        [queries, side_2, first, mark, *state],
        state_shapes + [out_shape, f32(8, 128), out_shape],
        2 * 10**9,
        scratch=[pltpu.SemaphoreType.DMA((TILES,))],
        out_hbm=3,
    )
    devices = lax.axis_size(SEQ_HEAD)
    arrays = [queries, odd_4, even_4, side_3, first, mark, *state, squares, done, out]
    attention, share = call(
        last_kernel,
        scalars,
        arrays,
        [out_shape, f32(devices, 128)],
        10**9,
        scratch=[
            pltpu.VMEM((TILE, HEADS * HEAD_WIDTH), jnp.float32),
            pltpu.VMEM((HEADS, TILE, 128), jnp.float32),
            pltpu.VMEM((HEADS, TILE, 128), jnp.float32),
            pltpu.VMEM((8, 128), jnp.float32),
            *copy_scratch,
        ],
        in_hbm=1,
        out_hbm=0,
        alias={len(scalars) + len(arrays) - 1: 0},
    )
    shares = lax.all_to_all(share, SEQ_HEAD, 0, 0, tiled=True)
    return (attention, objective_of(shares, lax.axis_size("head")))


def solution(mesh):
    torus = Mesh(
        mesh.devices.reshape(4, 8, 2, mesh.shape["head"]), ("seq_0", "seq_1", "seq_2", "head")
    )
    placed = (P(SEQ, "head"), P(SEQ, "head"), P(SEQ, "head"), P(SEQ), P(SEQ), P(SEQ))

    return jax.shard_map(
        on_device, mesh=torus, in_specs=placed, out_specs=(P(SEQ, "head"), P()), check_vma=False
    )
```

```python
import functools
import math

import jax
import jax.numpy as jnp
from jax import lax
from jax.experimental import pallas as pl
from jax.experimental.pallas import tpu as pltpu
from jax.sharding import Mesh
from jax.sharding import PartitionSpec as P

QUERY_HEADS = 32
KEY_VALUE_HEADS = 8
HEAD_WIDTH = 128
GROUP = QUERY_HEADS // KEY_VALUE_HEADS
SEQ = ("seq_0", "seq_1", "seq_2")
SEQ_HEAD = ("seq_0", "seq_1", "seq_2", "head")
ROWS = 512
TILE = 128
TILES = ROWS // TILE
PART = 32
PAIR = 2 * TILE
LOCAL_KV = 2
HEADS = LOCAL_KV * GROUP
LOWEST = -1e30
EXP2_SCALE = math.log2(math.e) / math.sqrt(HEAD_WIDTH)
NOWHERE = ROWS


def aligned(start, by, size=None):
    return pl.ds(start if isinstance(start, int) else pl.multiple_of(start, by), size or by)


def tile_rows(tile):
    return aligned(tile * TILE, TILE)


def columns(head):
    return slice(head * HEAD_WIDTH, (head + 1) * HEAD_WIDTH)


def dot(a, b, contract_b):
    return lax.dot_general(
        a, b, (((1,), (contract_b,)), ((), ())), preferred_element_type=jnp.float32
    )


def heads_of(kv):
    return range(kv * GROUP, (kv + 1) * GROUP)


def lane_groups(x):
    return [x[:, i : i + 128] for i in range(0, x.shape[1], 128)]


def folded(op, parts):
    while len(parts) > 1:
        parts = [op(*parts[i : i + 2]) if i + 1 < len(parts) else parts[i] for i in range(0, len(parts), 2)]
    return parts[0]


def widened(x, width):
    return jnp.concatenate([x] * (width // 128), axis=1)


def attend(q_ref, block_ref, parts, size):
    steps = [(part, kv) for part in parts for kv in range(LOCAL_KV)]

    def score(step):
        (rows, width, *_), kv = step
        q = jnp.concatenate([q_ref[rows, columns(h)] for h in heads_of(kv)], axis=0)
        return dot(q, block_ref[0, 0:width, columns(kv)], 1)

    def weigh(step, scores):
        (_, width, seen, old, _), kv = step
        rounded, states = [], []
        for g, head in enumerate(heads_of(kv)):
            part = jnp.where(seen, scores[g * size : (g + 1) * size], LOWEST)
            top = jnp.max(folded(jnp.maximum, lane_groups(part)), axis=1, keepdims=True)
            top = jnp.broadcast_to(top, (size, 128))
            before = old(head)
            ratio = None
            if before is not None:
                top = jnp.maximum(before[0], top)
                ratio = jnp.exp2((before[0] - top) * EXP2_SCALE)
            weights = jnp.exp2((part - widened(top, width)) * EXP2_SCALE)
            states.append((top, ratio))
            rounded.append(weights.astype(jnp.bfloat16))
        return jnp.concatenate(rounded, axis=0), states

    def add(step, rounded, states):
        (_, width, _, old, new), kv = step
        v = block_ref[1, 0:width, columns(kv)]
        update = dot(rounded, jnp.concatenate([v, jnp.ones_like(v)], axis=1), 0)
        for g, head in enumerate(heads_of(kv)):
            top, ratio = states[g]
            part = update[g * size : (g + 1) * size]
            sums, total = part[:, 0:HEAD_WIDTH], part[:, HEAD_WIDTH:]
            if ratio is not None:
                _, total_old, sums_old = old(head)
                sums, total = sums_old() * ratio + sums, total_old * ratio + total
            new(head, top, total, sums)

    scores, pending = score(steps[0]), None
    for at, step in enumerate(steps):
        ahead = score(steps[at + 1]) if at + 1 < len(steps) else None
        weighed = weigh(step, scores)
        if pending is not None:
            add(*pending)
        scores, pending = ahead, (step, *weighed)
    add(*pending)


def reader(state, rows):
    acc_ref, top_ref, tot_ref = state
    return lambda head: (
        top_ref[head, rows, :],
        tot_ref[head, rows, :],
        lambda: acc_ref[rows, columns(head)],
    )


def writer(state, rows):
    acc_ref, top_ref, tot_ref = state

    def store(head, top, total, sums):
        top_ref[head, rows, :] = top
        tot_ref[head, rows, :] = total
        acc_ref[rows, columns(head)] = sums

    return store


def attend_earlier(q_ref, block_ref, first_ref, places, size, offset, source, state):
    parts = []
    for rows, rows_in, rows_out in places:
        place = (lax.broadcasted_iota(jnp.int32, (size, ROWS), 1) + offset).astype(jnp.float32)
        seen = place >= widened(first_ref[rows, :], ROWS)
        parts.append((rows, ROWS, seen, reader(source, rows_in), writer(state, rows_out)))
    attend(q_ref, block_ref, parts, size)


def pair_rows(pair):
    return [aligned(pair * PAIR + i, TILE) for i in range(0, PAIR, TILE)]


def same(rows):
    return [(r, r, r) for r in rows]


def reaches(spot_ref, hop_ref, doc_ref, row, offset):
    floor = spot_ref[0] - hop_ref[0] * ROWS
    earliest = jnp.maximum(doc_ref[row], floor) - spot_ref[0]
    return (offset < 0) & (offset + ROWS > earliest)


def first_kernel(
    spot_ref, hop_ref, doc_ref, starts_ref, q_ref, own_ref,
    acc_ref, top_ref, tot_ref, first_ref,
):
    floor = spot_ref[0] - hop_ref[0] * ROWS
    state = (acc_ref, top_ref, tot_ref)
    parts = []
    for tile in range(TILES):
        width = (tile + 1) * TILE
        rows = tile_rows(tile)
        starts = jnp.maximum(starts_ref[tile : tile + 1, :], floor) - spot_ref[0]
        first = jnp.broadcast_to(starts.astype(jnp.float32), (TILE, 128)).T
        first_ref[rows, :] = first
        place = lax.broadcasted_iota(jnp.int32, (TILE, width), 1)
        row = lax.broadcasted_iota(jnp.int32, (TILE, width), 0) + tile * TILE
        seen = (place.astype(jnp.float32) >= widened(first, width)) & (place <= row)
        parts.append((rows, width, seen, lambda head: None, writer(state, rows)))
    attend(q_ref, own_ref, parts, TILE)


def copy_tile(source, target, rows, target_rows):
    for head in range(HEADS):
        top, total, sums = reader(source, rows)(head)
        writer(target, target_rows)(head, top, total, sums())


def finish(state, rows, size, mark_ref, out_ref, squares_ref, places):
    squares = jnp.zeros((size, HEAD_WIDTH), jnp.float32)
    for head in range(HEADS):
        _, total, sums = reader(state, rows)(head)
        attended = sums() * (1.0 / total)
        out_ref[places, columns(head)] = attended.astype(jnp.bfloat16)
        squares += attended * attended
    squares *= mark_ref[places, :]
    squares_ref[...] += jnp.sum(squares.reshape(size // 8, 8, HEAD_WIDTH), axis=0)


def out_copy(from_ref, out_ref, sems, tile):
    rows = tile_rows(tile)
    return pltpu.make_async_copy(from_ref.at[rows, :], out_ref.at[rows, :], sems.at[tile])


def one_block(spot_ref, hop_ref, doc_ref, q_ref, block_ref, first_ref, source, state, offset):
    rows = [tile_rows(tile) for tile in range(TILES)]
    needed = reaches(spot_ref, hop_ref, doc_ref, 0, offset)

    @pl.when(needed)
    def _():
        attend_earlier(q_ref, block_ref, first_ref, same(rows), TILE, offset, source, state)

    @pl.when(jnp.logical_not(needed))
    def _():
        for part in rows:
            copy_tile(source, state, part, part)


def near_kernel(
    spot_ref, hop_ref, doc_ref, q_ref, near_ref, first_ref, acc_in, top_in, tot_in,
    acc_ref, top_ref, tot_ref,
):
    source, state = (acc_in, top_in, tot_in), (acc_ref, top_ref, tot_ref)
    offset = on_core(spot_ref, 1, 1)
    one_block(spot_ref, hop_ref, doc_ref, q_ref, near_ref, first_ref, source, state, offset)


def on_core(spot_ref, core, distance):
    return jnp.where(spot_ref[1] == core, -distance * ROWS, NOWHERE)


def side_offset(spot_ref):
    return jnp.where(spot_ref[1] == 1, -3 * ROWS, -ROWS)


def far_kernel(
    spot_ref, hop_ref, doc_ref, q_ref, far_ref, first_ref, marks_ref, acc_in, top_in, tot_in,
    acc_ref, top_ref, tot_ref, mark_ref,
):
    source, state = (acc_in, top_in, tot_in), (acc_ref, top_ref, tot_ref)
    for tile in range(TILES):
        marks = marks_ref[tile : tile + 1, :].astype(jnp.float32)
        mark_ref[tile_rows(tile), :] = jnp.broadcast_to(marks, (TILE, 128)).T
    one_block(spot_ref, hop_ref, doc_ref, q_ref, far_ref, first_ref, source, state, -2 * ROWS)


def side_kernel(
    spot_ref, hop_ref, doc_ref, q_ref, side_ref, first_ref, mark_ref, acc_in, top_in, tot_in,
    acc_ref, top_ref, tot_ref, out_ref, squares_ref, done_ref, sems,
):
    source, state = (acc_in, top_in, tot_in), (acc_ref, top_ref, tot_ref)
    offset = side_offset(spot_ref)
    squares_ref[...] = jnp.zeros_like(squares_ref)

    def if_done(tile, act):
        pl.when(jnp.logical_not(late_from(spot_ref, hop_ref, doc_ref, tile * TILE)))(act)

    def moved(tile, act):
        if_done(tile, getattr(out_copy(done_ref, out_ref, sems, tile), act))

    per_pair = PAIR // TILE
    for pair in range(ROWS // PAIR):
        rows = pair_rows(pair)
        needed = reaches(spot_ref, hop_ref, doc_ref, pair * PAIR, offset)

        @pl.when(needed)
        def _():
            attend_earlier(q_ref, side_ref, first_ref, same(rows), TILE, offset, source, state)

        @pl.when(jnp.logical_not(needed))
        def _():
            for part in rows:
                copy_tile(source, state, part, part)

        for i, part in enumerate(rows):

            def act():
                finish(state, part, TILE, mark_ref, done_ref, squares_ref, part)

            if_done(pair * per_pair + i, act)
        if pair:
            for i in range(per_pair):
                moved((pair - 1) * per_pair + i, "start")
    for tile in range(TILES - per_pair, TILES):
        moved(tile, "start")
    for tile in range(TILES):
        moved(tile, "wait")


def late_from(spot_ref, hop_ref, doc_ref, row):
    offset = jnp.where(spot_ref[1] == 1, -4 * ROWS, -3 * ROWS)
    return reaches(spot_ref, hop_ref, doc_ref, row, offset)


def last_kernel(
    spot_ref, hop_ref, doc_ref, q_ref, odd_ref, even_ref, side_ref, first_ref, mark_ref, acc_in,
    top_in, tot_in, squares_in, out_in, out_ref, share_ref, acc_ref, top_ref, tot_ref, squares_ref,
    done_ref, sems,
):
    source, state = (acc_in, top_in, tot_in), (acc_ref, top_ref, tot_ref)
    slots = (
        (odd_ref, on_core(spot_ref, 1, 4)),
        (side_ref, on_core(spot_ref, 0, 3)),
        (even_ref, on_core(spot_ref, 0, 4)),
    )
    late = functools.partial(late_from, spot_ref, hop_ref, doc_ref)
    squares_ref[...] = squares_in[...]

    def absorb(places, size, row):
        here = slice(0, size)
        copy_tile(source, state, places, here)
        for block_ref, offset in slots:

            @pl.when(reaches(spot_ref, hop_ref, doc_ref, row, offset))
            def _():
                attend_earlier(
                    q_ref, block_ref, first_ref, [(places, here, here)], size, offset, state, state
                )

        finish(state, here, size, mark_ref, done_ref, squares_ref, places)

    def step(tile, carry):
        @pl.when(late(tile * TILE))
        def _():
            whole = late(tile * TILE + PART)

            @pl.when(whole)
            def _():
                absorb(tile_rows(tile), TILE, tile * TILE)

            @pl.when(jnp.logical_not(whole))
            def _():
                absorb(aligned(tile * TILE, PART), PART, tile * TILE)
                rest = aligned(tile * TILE + PART, PART, TILE - PART)
                finish(source, rest, TILE - PART, mark_ref, done_ref, squares_ref, rest)

        return carry

    lax.fori_loop(0, TILES, step, 0)
    squares = jnp.sum(squares_ref[...])
    count = jnp.sum(jnp.sum(mark_ref[...].reshape(ROWS // 8, 8, 128), axis=0)) * (1.0 / 128)
    lane = lax.broadcasted_iota(jnp.int32, share_ref.shape, 1)
    share_ref[...] = jnp.where(lane == 0, squares, jnp.where(lane == 1, count, 0.0))
    for ended in (False, True):
        for tile in range(TILES):

            @pl.when(late(tile * TILE))
            def _():
                copy = out_copy(done_ref, out_ref, sems, tile)
                copy.wait() if ended else copy.start()


def call(
    kernel, scalars, arrays, out_shapes, flops, scratch=(), in_hbm=0, out_hbm=None, alias=None
):
    smem, vmem, hbm = [
        pl.BlockSpec(memory_space=space) for space in (pltpu.SMEM, pltpu.VMEM, pltpu.HBM)
    ]
    return pl.pallas_call(
        kernel,
        out_shape=out_shapes,
        in_specs=[smem] * len(scalars) + [vmem] * (len(arrays) - in_hbm) + [hbm] * in_hbm,
        out_specs=[hbm if i == out_hbm else vmem for i in range(len(out_shapes))],
        scratch_shapes=list(scratch),
        input_output_aliases=alias or {},
        compiler_params=pltpu.CompilerParams(vmem_limit_bytes=8 * 1024 * 1024),
        cost_estimate=pl.CostEstimate(flops=flops, bytes_accessed=2**20, transcendentals=2**21),
    )(*scalars, *arrays)


def packed(keys, values):
    pads = ((0, 0), (0, 0))
    return jnp.pad(keys[None], ((0, 1), *pads)) + jnp.pad(values[None], ((1, 0), *pads))


def objective_kernel(copies, shares_ref, out_ref):
    sums = jnp.sum(shares_ref[...], axis=0, keepdims=True)
    lane = lax.broadcasted_iota(jnp.int32, sums.shape, 1)
    squares = jnp.sum(jnp.where(lane == 0, sums, 0.0))
    count = jnp.sum(jnp.where(lane == 1, sums, 0.0)) * (1.0 / copies)
    out_ref[0] = squares / (QUERY_HEADS * count)


def objective_of(shares, copies):
    return pl.pallas_call(
        functools.partial(objective_kernel, copies),
        out_shape=f32(1),
        in_specs=[pl.BlockSpec(memory_space=pltpu.VMEM)],
        out_specs=pl.BlockSpec(memory_space=pltpu.SMEM),
        compiler_params=pltpu.CompilerParams(vmem_limit_bytes=4 * 1024 * 1024),
    )(shares).reshape(())


def onward(shard, cores):
    blocks = range(lax.axis_size(SEQ) - 2)
    return lax.ppermute(shard, SEQ, [(i, i + 2) for i in blocks if i % 2 in cores])


def across(shard, pairs):
    return lax.ppermute(shard, "seq_2", pairs)


def f32(*shape):
    return jax.ShapeDtypeStruct(shape, jnp.float32)


def on_device(queries, keys, values, doc_start, hop_counts, loss_mask):
    spot = jnp.stack([lax.axis_index(SEQ) * ROWS, lax.axis_index("seq_2")])
    scalars = [spot, hop_counts, doc_start]
    own = packed(keys, values)
    odd_2 = onward(own, (1,))
    side_1 = across(own, [(0, 1)])
    even_2 = onward(own, (0,))
    state_shapes = [f32(ROWS, HEADS * HEAD_WIDTH), f32(HEADS, ROWS, 128), f32(HEADS, ROWS, 128)]
    *state, first = call(
        first_kernel,
        scalars,
        [doc_start.reshape(TILES, TILE), queries, own],
        state_shapes + [f32(ROWS, 128)],
        2 * 10**9,
    )
    odd_4 = onward(odd_2, (1,))
    state = call(near_kernel, scalars, [queries, side_1, first, *state], state_shapes, 10**9)
    even_4 = onward(even_2, (0,))
    far_2 = odd_2 + even_2
    side_2 = across(far_2, [(0, 1), (1, 0)])
    out_shape = jax.ShapeDtypeStruct((ROWS, HEADS * HEAD_WIDTH), jnp.bfloat16)
    copy_scratch = [pltpu.VMEM(out_shape.shape, jnp.bfloat16), pltpu.SemaphoreType.DMA((TILES,))]
    *state, mark = call(
        far_kernel,
        scalars,
        [queries, far_2, first, loss_mask.reshape(TILES, TILE), *state],
        state_shapes + [f32(ROWS, 128)],
        10**9,
    )
    side_3 = across(odd_4, [(1, 0)])
    *state, done, squares = call(
        side_kernel,
        scalars,
        [queries, side_2, first, mark, *state],
        state_shapes + [out_shape, f32(8, 128)],
        10**9,
        scratch=copy_scratch,
        out_hbm=3,
    )
    devices = lax.axis_size(SEQ_HEAD)
    arrays = [queries, odd_4, even_4, side_3, first, mark, *state, squares, done]
    attention, share = call(
        last_kernel,
        scalars,
        arrays,
        [out_shape, f32(devices, 128)],
        10**9,
        scratch=[
            pltpu.VMEM((TILE, HEADS * HEAD_WIDTH), jnp.float32),
            pltpu.VMEM((HEADS, TILE, 128), jnp.float32),
            pltpu.VMEM((HEADS, TILE, 128), jnp.float32),
            pltpu.VMEM((8, 128), jnp.float32),
            *copy_scratch,
        ],
        in_hbm=1,
        out_hbm=0,
        alias={len(scalars) + len(arrays) - 1: 0},
    )
    shares = lax.all_to_all(share, SEQ_HEAD, 0, 0, tiled=True)
    return (attention, objective_of(shares, lax.axis_size("head")))


def solution(mesh):
    torus = Mesh(
        mesh.devices.reshape(4, 8, 2, mesh.shape["head"]), ("seq_0", "seq_1", "seq_2", "head")
    )
    placed = (P(SEQ, "head"), P(SEQ, "head"), P(SEQ, "head"), P(SEQ), P(SEQ), P(SEQ))

    return jax.shard_map(
        on_device, mesh=torus, in_specs=placed, out_specs=(P(SEQ, "head"), P()), check_vma=False
    )
```
